128 devices in a mesh: data: 1, graph: 128 (over z, y, x, core).
Axes of the slice: x: 4, y: 4, z: 4, core: 2. Of those that a mesh axis runs over, the one named last changes fastest.
Arguments:
- x_feat: bfloat16 [65536, 100], P(('data', 'graph'))
- dst_local: int32 [4194304], P(('data', 'graph'))
- src_slot: int32 [4194304], P(('data', 'graph'))
- edge_w: float32 [4194304], P(('data', 'graph'))
- send_idx: int32 [32768], P(('data', 'graph'))
- hub_ids: int32 [256], P('data')
- w_first: bfloat16 [100, 256], replicated
- b_first: float32 [256], replicated
- w_second: bfloat16 [256, 47], replicated
- grad_out: float32 [65536, 47], P(('data', 'graph'))
Outputs:
- output 1: float32 [65536, 100], P(('data', 'graph'))
- output 2: float32 [100, 256], P('data')
- output 3: float32 [256, 47], P('data')
- output 4: float32 [256], P('data')
- output 5: float32 [47], P('data')
All inputs are finite; a program needn't handle non-finite values.
Results may differ from the reference program's by a relative error of at most 0.00112444.
Values are sent between devices in bfloat16 or wider.
A program may use at most 1 GiB of HBM per device.

```python
import jax
import jax.numpy as jnp
from jax import lax

GROUP_SIZE = 128
NODES_DEV = 512
FEAT_IN = 100
FEAT_HID = 256
FEAT_OUT = 47
EDGE_DEG = 64
SEND_ROWS = 2
NUM_HUBS = 256
HUB_DST_PCT = 15
HUB_SRC_PCT = 15
HALO_SRC_PCT = 35

VERTICES = GROUP_SIZE * NODES_DEV
EDGE_CAP = NODES_DEV * EDGE_DEG
HALO_ROWS = GROUP_SIZE * SEND_ROWS


def draw_graph(graph_key):
    key_list = jax.random.split(graph_key, 16)
    edge_shape = (GROUP_SIZE, EDGE_CAP)
    hub_ids = jax.random.permutation(key_list[0], VERTICES)[:NUM_HUBS].astype(jnp.int32)
    shrink = jax.random.randint(key_list[1], (GROUP_SIZE,), 1, 5)
    full_dev = jax.random.randint(key_list[2], (), 0, GROUP_SIZE)
    counts = jnp.where(jnp.arange(GROUP_SIZE) == full_dev, EDGE_CAP, EDGE_CAP // shrink)
    edge_live = jnp.arange(EDGE_CAP)[None, :] < counts[:, None]
    dst_pick = jax.random.randint(key_list[3], edge_shape, 0, 100)
    dst_span = jax.random.randint(key_list[4], edge_shape, 1, NODES_DEV + 1)
    dst_node = jax.random.randint(key_list[5], edge_shape, 0, NODES_DEV) % dst_span
    dst_hub = jax.random.randint(key_list[6], edge_shape, 0, NUM_HUBS)
    dst_local = jnp.where(dst_pick < HUB_DST_PCT, NODES_DEV + dst_hub, dst_node)
    src_pick = jax.random.randint(key_list[7], edge_shape, 0, 100)
    src_span = jax.random.randint(key_list[8], edge_shape, 1, NODES_DEV + 1)
    src_node = jax.random.randint(key_list[9], edge_shape, 0, NODES_DEV) % src_span
    peer_step = jax.random.randint(key_list[10], edge_shape, 1, GROUP_SIZE)
    peer_dev = (jnp.arange(GROUP_SIZE)[:, None] + peer_step) % GROUP_SIZE
    row_span = jax.random.randint(key_list[11], edge_shape, 1, SEND_ROWS + 1)
    halo_row = jax.random.randint(key_list[12], edge_shape, 0, SEND_ROWS) % row_span
    src_hub = jax.random.randint(key_list[13], edge_shape, 0, NUM_HUBS)
    src_slot = jnp.where(
        src_pick < HUB_SRC_PCT,
        NODES_DEV + HALO_ROWS + src_hub,
        jnp.where(src_pick < HUB_SRC_PCT + HALO_SRC_PCT, NODES_DEV + peer_dev * SEND_ROWS + halo_row, src_node),
    )
    send_idx = jax.random.randint(key_list[14], (GROUP_SIZE * GROUP_SIZE * SEND_ROWS,), 0, NODES_DEV)
    dst_local = jnp.where(edge_live, dst_local, 0).reshape(-1).astype(jnp.int32)
    src_slot = jnp.where(edge_live, src_slot, 0).reshape(-1).astype(jnp.int32)
    return dst_local, src_slot, edge_live.reshape(-1), send_idx.astype(jnp.int32), hub_ids


def setup_inputs(seed: int = 0, part: int = 0) -> dict:
    part_key = jax.random.fold_in(jax.random.key(seed), part)
    dst_local, src_slot, edge_live, send_idx, hub_ids = draw_graph(part_key)
    value_keys = jax.random.split(jax.random.fold_in(part_key, 3), 3)
    weight_keys = jax.random.split(jax.random.key(seed + 1), 3)
    x_feat = jax.random.normal(value_keys[0], (VERTICES, FEAT_IN), jnp.float32).astype(jnp.bfloat16)
    edge_scale = jax.random.uniform(value_keys[1], (GROUP_SIZE * EDGE_CAP,), jnp.float32, 0.5, 1.5)
    edge_w = jnp.where(edge_live, edge_scale * EDGE_DEG ** -0.5, 0.0).astype(jnp.float32)
    grad_out = jax.random.normal(value_keys[2], (VERTICES, FEAT_OUT), jnp.float32)
    w_first = (jax.random.normal(weight_keys[0], (FEAT_IN, FEAT_HID), jnp.float32) * FEAT_IN ** -0.5).astype(jnp.bfloat16)
    b_first = 0.5 * jax.random.normal(weight_keys[1], (FEAT_HID,), jnp.float32)
    w_second = (jax.random.normal(weight_keys[2], (FEAT_HID, FEAT_OUT), jnp.float32) * FEAT_HID ** -0.5).astype(jnp.bfloat16)
    return {
        "x_feat": x_feat,
        "dst_local": dst_local,
        "src_slot": src_slot,
        "edge_w": edge_w,
        "send_idx": send_idx,
        "hub_ids": hub_ids,
        "w_first": w_first,
        "b_first": b_first,
        "w_second": w_second,
        "grad_out": grad_out,
    }


def source_ids(src_slot, send_idx, hub_ids):
    slot_ids = src_slot.reshape(GROUP_SIZE, EDGE_CAP)
    device = jnp.arange(GROUP_SIZE)[:, None]
    halo_pos = jnp.clip(slot_ids - NODES_DEV, 0, HALO_ROWS - 1)
    peer_dev = halo_pos // SEND_ROWS
    send_table = send_idx.reshape(GROUP_SIZE, GROUP_SIZE, SEND_ROWS)
    halo_src = peer_dev * NODES_DEV + send_table[peer_dev, device, halo_pos % SEND_ROWS]
    hub_src = hub_ids[jnp.clip(slot_ids - NODES_DEV - HALO_ROWS, 0, NUM_HUBS - 1)]
    return jnp.where(
        slot_ids < NODES_DEV,
        device * NODES_DEV + slot_ids,
        jnp.where(slot_ids < NODES_DEV + HALO_ROWS, halo_src, hub_src),
    )


def aggregate(features, dst_rows, src_ids, edge_rows, hub_ids):
    def one_device(dev_item):
        dst_dev, src_dev, w_dev = dev_item
        gathered = features[src_dev] * w_dev[:, None]
        return jax.ops.segment_sum(gathered, dst_dev, num_segments=NODES_DEV + NUM_HUBS)
    dev_sums = lax.map(one_device, (dst_rows, src_ids, edge_rows))
    local_rows = dev_sums[:, :NODES_DEV].reshape(VERTICES, -1)
    return local_rows.at[hub_ids].add(dev_sums[:, NODES_DEV:].sum(axis=0))


def reference(x_feat, dst_local, src_slot, edge_w, send_idx, hub_ids, w_first, b_first, w_second, grad_out):
    src_ids = source_ids(src_slot, send_idx, hub_ids)
    dst_rows = dst_local.reshape(GROUP_SIZE, EDGE_CAP)
    edge_rows = edge_w.reshape(GROUP_SIZE, EDGE_CAP)

    def layers(x_in, w_in, b_in, w_out):
        z_first = jnp.dot(x_in, w_in, preferred_element_type=jnp.float32).astype(jnp.bfloat16).astype(jnp.float32)
        pre_act = aggregate(z_first, dst_rows, src_ids, edge_rows, hub_ids) + b_in
        act_full = jax.nn.relu(pre_act)
        hidden = act_full + lax.stop_gradient(act_full.astype(jnp.bfloat16).astype(jnp.float32) - act_full)
        z_second = jnp.dot(hidden, w_out, preferred_element_type=jnp.float32).astype(jnp.bfloat16).astype(jnp.float32)
        return aggregate(z_second, dst_rows, src_ids, edge_rows, hub_ids)

    _, pullback = jax.vjp(
        layers,
        x_feat.astype(jnp.float32),
        w_first.astype(jnp.float32),
        b_first,
        w_second.astype(jnp.float32),
    )
    grad_x, grad_w1, grad_b1, grad_w2 = pullback(grad_out)
    return grad_x, grad_w1, grad_w2, grad_b1, grad_out.sum(axis=0)
```

```python
import functools

import jax
import jax.numpy as jnp
from jax import lax
from jax.experimental import pallas as pl
from jax.experimental.pallas import tpu as pltpu
from jax.sharding import PartitionSpec as P

BF16 = jnp.bfloat16
F32 = jnp.float32
HI = lax.Precision.HIGHEST
LANES = 128
MESH = pl.DeviceIdType.MESH


def exchange_kernel(groups, kinds, *refs):
    count = len(kinds)
    ins, outs, sems = refs[:count], refs[count:2 * count], refs[2 * count:]
    send_sems, recv_sems = sems[:count], sems[count:]
    me = lax.axis_index("graph")
    barrier = pltpu.get_barrier_semaphore()

    def greet(i, carry):
        pl.semaphore_signal(barrier, inc=1, device_id=(0, jnp.bitwise_xor(me, i)), device_id_type=MESH)
        return carry

    lax.fori_loop(1, groups, greet, 0)
    pl.semaphore_wait(barrier, groups - 1)

    def send(i, carry):
        peer = jnp.bitwise_xor(me, i)
        for kind, src, dst, send_sem, recv_sem in zip(kinds, ins, outs, send_sems, recv_sems):
            pltpu.make_async_remote_copy(
                src_ref=src.at[peer] if kind == "a" else src,
                dst_ref=dst.at[me],
                send_sem=send_sem,
                recv_sem=recv_sem,
                device_id=(0, peer),
                device_id_type=MESH,
            ).start()
        return carry

    lax.fori_loop(1, groups, send, 0)
    for kind, src, dst, recv_sem in zip(kinds, ins, outs, recv_sems):
        pltpu.make_async_copy(src.at[me] if kind == "a" else src, dst.at[me], recv_sem).start()
    for dst, send_sem, recv_sem in zip(outs, send_sems, recv_sems):
        pltpu.make_async_copy(dst, dst, recv_sem).wait()
        part = dst.at[pl.ds(0, groups - 1)]
        pltpu.make_async_copy(part, part, send_sem).wait()


def exchange(groups, kinds, arrays, collective_id):
    outs = []
    for kind, arr in zip(kinds, arrays):
        shape = arr.shape if kind == "a" else (groups,) + arr.shape
        outs.append(jax.ShapeDtypeStruct(shape, arr.dtype))
    vmem = pl.BlockSpec(memory_space=pltpu.VMEM)
    return pl.pallas_call(
        functools.partial(exchange_kernel, groups, kinds),
        out_shape=outs,
        in_specs=[vmem] * len(arrays),
        out_specs=[vmem] * len(arrays),
        scratch_shapes=[pltpu.SemaphoreType.DMA] * (2 * len(arrays)),
        compiler_params=pltpu.CompilerParams(collective_id=collective_id, has_side_effects=True),
        name=f"exchange_{collective_id}",
    )(*arrays)


def keys_kernel(own, dst_ref, src_ref, tab_ref, key_ref, lane_ref):
    tables = tab_ref.shape[0]
    dst_rows = own // LANES
    slots = own + (tables - 2 * dst_rows) * LANES + 0

    def body(i, carry):
        rows = pl.ds(pl.multiple_of(i * 8, 8), 8)
        dst = dst_ref[rows, :]
        src = src_ref[rows, :]
        dlane = jnp.bitwise_and(dst, LANES - 1)
        slane = jnp.bitwise_and(src, LANES - 1)
        dblk = jnp.right_shift(dst, 7)
        sblk = jnp.right_shift(src, 7)
        for t in range(tables):
            row = jnp.broadcast_to(tab_ref[t:t + 1, :], (8, LANES))
            if t < dst_rows:
                dst = jnp.where(dblk == t, jnp.take_along_axis(row, dlane, axis=1), dst)
            else:
                src = jnp.where(sblk == t - dst_rows, jnp.take_along_axis(row, slane, axis=1), src)
        key_ref[rows, :] = jnp.right_shift(dst, 7) * 1024 + src
        lane_ref[rows, :] = jnp.bitwise_and(dst, LANES - 1)
        return carry

    lax.fori_loop(0, dst_ref.shape[0] // 8, body, 0)


def edge_keys(dst, src, tables, own):
    rows = dst.shape[0] // LANES
    shape = jax.ShapeDtypeStruct((rows, LANES), jnp.int32)
    return pl.pallas_call(
        functools.partial(keys_kernel, own),
        out_shape=(shape, shape),
        name="edge_keys",
    )(dst.reshape(rows, LANES), src.reshape(rows, LANES), tables)


def build_kernel(slots, dsts, key_ref, lane_ref, w_ref, out_ref, *bufs):
    cells = slots * (dsts // LANES)
    chunk = 64

    def clear(i, carry):
        for buf in bufs:
            buf[pl.ds(pl.multiple_of(i * chunk, chunk), chunk), :] = jnp.zeros((chunk, LANES), F32)
        return carry

    lax.fori_loop(0, cells // chunk, clear, 0)
    lane_iota = lax.broadcasted_iota(jnp.int32, (8, LANES), 1)
    pick = lax.broadcasted_iota(jnp.int32, (8, LANES), 0) * 16

    def step(it, carry):
        lanes = jnp.broadcast_to(lane_ref[pl.ds(it, 1), :], (8, LANES))
        weights = jnp.broadcast_to(w_ref[pl.ds(it, 1), :], (8, LANES))
        vals = []
        for j in range(16):
            lane = jnp.take_along_axis(lanes, pick + j, axis=1)
            weight = jnp.take_along_axis(weights, pick + j, axis=1)
            vals.append(jnp.where(lane == lane_iota, weight, 0.0))
        for j in range(16):
            rows = [key_ref[it, s * 16 + j] for s in range(8)]
            sums = [bufs[s][pl.ds(rows[s], 1), :] + vals[j][s:s + 1, :] for s in range(8)]
            for s in range(8):
                bufs[s][pl.ds(rows[s], 1), :] = sums[s]
        return carry

    lax.fori_loop(0, key_ref.shape[0], step, 0)

    for blk in range(dsts // LANES):
        def finish(i, carry):
            rows = pl.ds(pl.multiple_of(blk * slots + i * chunk, chunk), chunk)
            total = bufs[0][rows, :]
            for buf in bufs[1:]:
                total = total + buf[rows, :]
            out_ref[pl.ds(pl.multiple_of(i * chunk, chunk), chunk), blk * LANES:(blk + 1) * LANES] = total
            return carry

        lax.fori_loop(0, slots // chunk, finish, 0)


def build_adjacency(keys, lanes, weights, slots, dsts):
    cells = slots * (dsts // LANES)
    vmem = pl.BlockSpec(memory_space=pltpu.VMEM)
    return pl.pallas_call(
        functools.partial(build_kernel, slots, dsts),
        out_shape=jax.ShapeDtypeStruct((slots, dsts), F32),
        in_specs=[pl.BlockSpec(memory_space=pltpu.SMEM), vmem, vmem],
        out_specs=vmem,
        scratch_shapes=[pltpu.VMEM((cells, LANES), F32)] * 8,
        compiler_params=pltpu.CompilerParams(vmem_limit_bytes=48 * 2 ** 20),
        name="build_adjacency",
    )(keys, lanes, weights.reshape(keys.shape))


def dot(a, b, ca=1, cb=0, precision=None):
    return lax.dot_general(a, b, (((ca,), (cb,)), ((), ())), precision=precision, preferred_element_type=F32)


def pad_cols(a):
    return jnp.pad(a, ((0, 0), (0, LANES - a.shape[1])))


def solution(mesh):
    groups = mesh.shape["graph"]

    def device_step(x, dst, src, w, send, hub_ids, w_first, b_first, w_second, dy):
        own, feat_in = x.shape
        feat_out = dy.shape[1]
        hid = w_first.shape[1]
        halo, hubs = send.shape[0], hub_ids.shape[0]
        slots, dsts = own + halo + hubs, own + hubs
        me = lax.axis_index("graph")
        own_iota = jnp.arange(own, dtype=jnp.int32)
        is_hub = (hub_ids - me * own)[:, None] == own_iota[None, :]
        code = jnp.sum(jnp.where(is_hub, jnp.arange(1, hubs + 1, dtype=jnp.int32)[:, None], 0), axis=0)
        hub_f = is_hub.astype(F32)
        hub_b = is_hub.astype(BF16)
        pick_b = (send[:, None] == own_iota[None, :]).astype(BF16)
        pick_f = pick_b.astype(F32)
        plain = (code == 0)[:, None]

        x_pad = jnp.concatenate([x, code[:, None].astype(BF16), jnp.zeros((own, LANES - feat_in - 1), BF16)], axis=1)
        dy_pad = pad_cols(dy)
        halo_x = dot(pick_b, x_pad).astype(BF16)
        hub_x = dot(hub_b, x_pad).astype(BF16)
        hub_d = dot(hub_f, dy_pad, precision=HI)
        halo_x, hub_x, hub_d = exchange(
            groups, "aaa", [v.reshape(groups, -1, LANES) for v in (halo_x, hub_x, hub_d)], 0)
        halo_x = halo_x.reshape(halo, LANES)
        home_x = hub_x.astype(F32).sum(axis=0).astype(BF16)
        hub_x, hub_d = exchange(groups, "bb", [home_x, hub_d.sum(axis=0)], 1)
        hub_x, hub_d = hub_x.reshape(hubs, LANES), hub_d.reshape(hubs, LANES)

        halo_code = halo_x[:, feat_in].astype(jnp.int32)
        hub_base = own + halo - 1
        tables = jnp.concatenate([
            jnp.where(code > 0, own - 1 + code, own_iota),
            jnp.where(code > 0, hub_base + code, own_iota),
            jnp.where(halo_code > 0, hub_base + halo_code, own + jnp.arange(halo, dtype=jnp.int32)),
        ]).reshape(-1, LANES)
        keys, lanes = edge_keys(dst, src, tables, own)
        adj = build_adjacency(keys, lanes, w, slots, dsts)

        w1_pad = jnp.pad(w_first, ((0, LANES - feat_in), (0, 0)))
        w2_pad = pad_cols(w_second)
        z = dot(jnp.concatenate([x_pad, halo_x, hub_x], axis=0), w1_pad).astype(BF16)
        y = dot(adj, z.astype(F32), 0, 0, precision=HI)
        g2 = dot(adj, jnp.concatenate([dy_pad, hub_d], axis=0), precision=HI)
        msg = jnp.concatenate([
            g2[own:own + halo].reshape(groups, -1, LANES),
            y[own:].reshape(groups, -1, LANES),
            g2[own + halo:].reshape(groups, -1, LANES),
        ], axis=1)
        (got,) = exchange(groups, "a", [msg], 2)
        per = hubs // groups
        back = got[:, :per].reshape(halo, LANES)
        dz2_own = g2[:own] + dot(pick_f, back, 0, 0, precision=HI)
        home = got[:, per:].sum(axis=0)
        y_rows = per * hid // LANES
        pre = jnp.concatenate([y[:own], home[:y_rows].reshape(per, hid)], axis=0) + b_first
        dz2 = jnp.concatenate([dz2_own, home[y_rows:]], axis=0).astype(BF16)
        keep = jnp.concatenate([plain, jnp.ones((per, 1), bool)], axis=0)
        hidden = jnp.where(keep, jax.nn.relu(pre), 0.0).astype(BF16)
        gw2 = dot(hidden, dz2, 0, 0)
        dh1 = dot(dz2, w2_pad, 1, 1)
        dy1 = jnp.where(keep & (pre > 0), dh1, 0.0)
        bias = jnp.concatenate([dy1.sum(axis=0), dy_pad.sum(axis=0)]).reshape(-1, LANES)
        hub_y, gw2, bias = exchange(
            groups, "bab", [dy1[own:].reshape(-1, LANES), gw2.reshape(groups, -1, LANES), bias], 3)
        bias = bias.sum(axis=0)
        g1 = dot(adj, jnp.concatenate([dy1[:own], hub_y.reshape(hubs, hid)], axis=0), precision=HI)
        msg = jnp.concatenate([
            g1[own:own + halo].reshape(groups, -1, LANES), g1[own + halo:].reshape(groups, -1, LANES)], axis=1)
        (got,) = exchange(groups, "a", [msg], 4)
        back = got[:, :y_rows].reshape(halo, hid)
        dz1_own = (g1[:own] + dot(pick_f, back, 0, 0, precision=HI)).astype(BF16)
        dz1_home = got[:, y_rows:].sum(axis=0).reshape(per, hid).astype(BF16)
        dz1 = jnp.concatenate([jnp.where(plain, dz1_own, jnp.zeros((), BF16)), dz1_home], axis=0)
        gw1 = dot(dz1, jnp.concatenate([x_pad, home_x], axis=0), 0, 0)
        dx = dot(dz1, w1_pad, 1, 1)
        gw1, hub_dx, gw2 = exchange(
            groups, "abb", [gw1.reshape(groups, -1, LANES), dx[own:], gw2.sum(axis=0)], 5)
        (gw1,) = exchange(groups, "b", [gw1.sum(axis=0)], 6)
        dx = jnp.where(plain, dx[:own], dot(hub_f, hub_dx.reshape(hubs, LANES), 0, 0, precision=HI))
        return (
            dx[:, :feat_in],
            gw1.reshape(hid, LANES)[:, :feat_in].T,
            gw2.reshape(hid, LANES)[:, :feat_out],
            bias[:hid // LANES].reshape(-1),
            bias[-1, :feat_out],
        )

    rows, flat = P(("data", "graph"), None), P(("data", "graph"))
    return jax.shard_map(
        device_step,
        mesh=mesh,
        in_specs=(rows, flat, flat, flat, flat, P("data"), P(), P(), P(), rows),
        out_specs=(rows, P("data", None), P("data", None), P("data"), P("data")),
        check_vma=False,
    )
```

```python
import functools

import jax
import jax.numpy as jnp
from jax import lax
from jax.experimental import pallas as pl
from jax.experimental.pallas import tpu as pltpu
from jax.sharding import PartitionSpec as P

BF16 = jnp.bfloat16
F32 = jnp.float32
HI = lax.Precision.HIGHEST
LANES = 128
MESH = pl.DeviceIdType.MESH


def dot(a, b, ca=1, cb=0, precision=None):
    return lax.dot_general(a, b, (((ca,), (cb,)), ((), ())), precision=precision, preferred_element_type=F32)


def exchange_kernel(groups, kinds, *refs):
    count = len(kinds)
    ins, outs, sems = refs[:count], refs[count:2 * count], refs[2 * count:]
    send_sems, recv_sems = sems[:count], sems[count:]
    me = lax.axis_index("graph")
    barrier = pltpu.get_barrier_semaphore()

    def greet(i, carry):
        pl.semaphore_signal(barrier, inc=1, device_id=(0, jnp.bitwise_xor(me, i)), device_id_type=MESH)
        return carry

    lax.fori_loop(1, groups, greet, 0)
    pl.semaphore_wait(barrier, groups - 1)

    def send(i, carry):
        peer = jnp.bitwise_xor(me, i)
        for kind, src, dst, send_sem, recv_sem in zip(kinds, ins, outs, send_sems, recv_sems):
            pltpu.make_async_remote_copy(
                src_ref=src.at[peer] if kind == "a" else src,
                dst_ref=dst.at[me],
                send_sem=send_sem,
                recv_sem=recv_sem,
                device_id=(0, peer),
                device_id_type=MESH,
            ).start()
        return carry

    lax.fori_loop(1, groups, send, 0)
    for kind, src, dst, recv_sem in zip(kinds, ins, outs, recv_sems):
        pltpu.make_async_copy(src.at[me] if kind == "a" else src, dst.at[me], recv_sem).start()
    for dst, send_sem, recv_sem in zip(outs, send_sems, recv_sems):
        pltpu.make_async_copy(dst, dst, recv_sem).wait()
        part = dst.at[pl.ds(0, groups - 1)]
        pltpu.make_async_copy(part, part, send_sem).wait()


def exchange(groups, kinds, arrays, collective_id):
    outs = []
    for kind, arr in zip(kinds, arrays):
        shape = arr.shape if kind == "a" else (groups,) + arr.shape
        outs.append(jax.ShapeDtypeStruct(shape, arr.dtype))
    vmem = pl.BlockSpec(memory_space=pltpu.VMEM)
    return pl.pallas_call(
        functools.partial(exchange_kernel, groups, kinds),
        out_shape=outs,
        in_specs=[vmem] * len(arrays),
        out_specs=[vmem] * len(arrays),
        scratch_shapes=[pltpu.SemaphoreType.DMA] * (2 * len(arrays)),
        compiler_params=pltpu.CompilerParams(collective_id=collective_id, has_side_effects=True),
        name=f"exchange_{collective_id}",
    )(*arrays)


def split3(a):
    hi = a.astype(BF16)
    rest = a - hi.astype(F32)
    mid = rest.astype(BF16)
    return hi, mid, (rest - mid.astype(F32)).astype(BF16)


def keys_kernel(own, dst_ref, src_ref, tab_ref, key_ref, lane_ref):
    tables = tab_ref.shape[0]
    dst_rows = own // LANES
    slots = own + (tables - 2 * dst_rows) * LANES + 0

    def body(i, carry):
        rows = pl.ds(pl.multiple_of(i * 8, 8), 8)
        dst = dst_ref[rows, :]
        src = src_ref[rows, :]
        dlane = jnp.bitwise_and(dst, LANES - 1)
        slane = jnp.bitwise_and(src, LANES - 1)
        dblk = jnp.right_shift(dst, 7)
        sblk = jnp.right_shift(src, 7)
        for t in range(tables):
            row = jnp.broadcast_to(tab_ref[t:t + 1, :], (8, LANES))
            if t < dst_rows:
                dst = jnp.where(dblk == t, jnp.take_along_axis(row, dlane, axis=1), dst)
            else:
                src = jnp.where(sblk == t - dst_rows, jnp.take_along_axis(row, slane, axis=1), src)
        key_ref[rows, :] = jnp.right_shift(dst, 7) * 1024 + src
        lane_ref[rows, :] = jnp.bitwise_and(dst, LANES - 1)
        return carry

    lax.fori_loop(0, dst_ref.shape[0] // 8, body, 0)


def edge_keys(dst, src, tables, own):
    rows = dst.shape[0] // LANES
    shape = jax.ShapeDtypeStruct((rows, LANES), jnp.int32)
    return pl.pallas_call(
        functools.partial(keys_kernel, own),
        out_shape=(shape, shape),
        name="edge_keys",
    )(dst.reshape(rows, LANES), src.reshape(rows, LANES), tables)


def build_kernel(slots, dsts, key_ref, lane_ref, w_ref, hi_ref, mid_ref, low_ref, *bufs):
    cells = slots * (dsts // LANES)
    chunk = 64

    def clear(i, carry):
        for buf in bufs:
            buf[pl.ds(pl.multiple_of(i * chunk, chunk), chunk), :] = jnp.zeros((chunk, LANES), F32)
        return carry

    lax.fori_loop(0, cells // chunk, clear, 0)
    lane_iota = lax.broadcasted_iota(jnp.int32, (8, LANES), 1)
    pick = lax.broadcasted_iota(jnp.int32, (8, LANES), 0) * 16

    def step(it, carry):
        lanes = jnp.broadcast_to(lane_ref[pl.ds(it, 1), :], (8, LANES))
        weights = jnp.broadcast_to(w_ref[pl.ds(it, 1), :], (8, LANES))
        vals = []
        for j in range(16):
            lane = jnp.take_along_axis(lanes, pick + j, axis=1)
            weight = jnp.take_along_axis(weights, pick + j, axis=1)
            vals.append(jnp.where(lane == lane_iota, weight, 0.0))
        for j in range(16):
            rows = [key_ref[it, s * 16 + j] for s in range(8)]
            sums = [bufs[s][pl.ds(rows[s], 1), :] + vals[j][s:s + 1, :] for s in range(8)]
            for s in range(8):
                bufs[s][pl.ds(rows[s], 1), :] = sums[s]
        return carry

    lax.fori_loop(0, key_ref.shape[0], step, 0)

    for blk in range(dsts // LANES):
        def finish(i, carry):
            rows = pl.ds(pl.multiple_of(blk * slots + i * chunk, chunk), chunk)
            total = bufs[0][rows, :]
            for buf in bufs[1:]:
                total = total + buf[rows, :]
            for ref, piece in zip((hi_ref, mid_ref, low_ref), split3(total)):
                ref[pl.ds(pl.multiple_of(i * chunk, chunk), chunk), blk * LANES:(blk + 1) * LANES] = piece
            return carry

        lax.fori_loop(0, slots // chunk, finish, 0)


def build_adjacency(keys, lanes, weights, slots, dsts):
    cells = slots * (dsts // LANES)
    vmem = pl.BlockSpec(memory_space=pltpu.VMEM)
    return pl.pallas_call(
        functools.partial(build_kernel, slots, dsts),
        out_shape=[jax.ShapeDtypeStruct((slots, dsts), BF16)] * 3,
        in_specs=[pl.BlockSpec(memory_space=pltpu.SMEM), vmem, vmem],
        out_specs=[vmem] * 3,
        scratch_shapes=[pltpu.VMEM((cells, LANES), F32)] * 8,
        compiler_params=pltpu.CompilerParams(vmem_limit_bytes=48 * 2 ** 20),
        name="build_adjacency",
    )(keys, lanes, weights.reshape(keys.shape))


def exact3(sel, pieces, ca=1):
    return dot(sel, pieces[2], ca) + dot(sel, pieces[1], ca) + dot(sel, pieces[0], ca)


def full6(a, b):
    low = dot(a[0], b[2]) + dot(a[2], b[0]) + dot(a[1], b[1])
    return low + (dot(a[0], b[1]) + dot(a[1], b[0])) + dot(a[0], b[0])


def wait_all(groups, buf, sem, whole):
    part = buf if whole else buf.at[pl.ds(0, groups - 1)]
    pltpu.make_async_copy(part, part, sem).wait()


def send_all(groups, me, items):
    def send(i, carry):
        peer = jnp.bitwise_xor(me, i)
        for kind, src, dst, send_sem, recv_sem in items:
            pltpu.make_async_remote_copy(
                src_ref=src.at[peer] if kind == "a" else src,
                dst_ref=dst.at[me],
                send_sem=send_sem,
                recv_sem=recv_sem,
                device_id=(0, peer),
                device_id_type=MESH,
            ).start()
        return carry

    lax.fori_loop(1, groups, send, 0)
    for kind, src, dst, _, recv_sem in items:
        pltpu.make_async_copy(src.at[me] if kind == "a" else src, dst.at[me], recv_sem).start()


def main_kernel(groups, own, halo, hubs, hi_ref, mid_ref, low_ref, zt_ref, d_ref, pick_ref, sel_ref, plain_ref, b1_ref,
                w1_ref, w2_ref, x_ref, home_x_ref,
                dx_ref, gw1_ref, gw2_ref, bias_ref,
                s1, s2, s3, s4, s5, s6, s7, s8, r1, r2, r3, r4, r5, r6, r7, pre_ref, g2_ref, g1_ref, dy_ref, *sems):
    snd, rcv = sems[:8], sems[8:]
    adj = (hi_ref, mid_ref, low_ref)
    per = hubs // groups
    hid = b1_ref.shape[1]
    first_hub = own + halo
    me = lax.axis_index("graph")
    barrier = pltpu.get_barrier_semaphore()

    def greet(i, carry):
        pl.semaphore_signal(barrier, inc=1, device_id=(0, jnp.bitwise_xor(me, i)), device_id_type=MESH)
        return carry

    lax.fori_loop(1, groups, greet, 0)
    lane = lax.broadcasted_iota(jnp.int32, (1, LANES), 1)
    half = lane < LANES // 2

    def forward(cols):
        zt = zt_ref[...]
        return dot(zt, low_ref[:, cols]) + dot(zt, mid_ref[:, cols]) + dot(zt, hi_ref[:, cols])

    dh, dm, dl = split3(d_ref[...])
    d_two = (dh.astype(F32) + pltpu.roll(dm.astype(F32), LANES // 2, 1)).astype(BF16)
    d_four = jnp.concatenate([d_two, dl], axis=1)

    def grad_out_sums(rows):
        a = dot(hi_ref[rows, :], d_four)
        t = a[:, :LANES] + a[:, LANES:] + dot(mid_ref[rows, :], d_two) + dot(low_ref[rows, :], dh)
        return jnp.where(half, t + pltpu.roll(t, LANES // 2, 1), 0.0)

    y_hub = forward(slice(own, own + hubs)).T
    s1[:, :, LANES:] = y_hub.reshape(groups, per, hid)
    g2_halo = grad_out_sums(slice(own, first_hub))
    g2_hub = grad_out_sums(slice(first_hub, first_hub + hubs))
    s1[:, :, :LANES] = (g2_halo + pltpu.roll(g2_hub, LANES // 2, 1)).reshape(groups, per, LANES)
    pl.semaphore_wait(barrier, groups - 1)
    send_all(groups, me, [("a", s1, r1, snd[0], rcv[0])])

    b1 = b1_ref[...]
    plain = plain_ref[...] > 0
    pre_ref[...] = forward(slice(0, own)).T + b1
    g2_ref[...] = grad_out_sums(slice(0, own))
    wait_all(groups, r1, rcv[0], True)
    home = r1[...].sum(axis=0)
    pad = jnp.zeros((8 - per, LANES), F32)
    home_g = jnp.where(half, pltpu.roll(jnp.concatenate([home[:, :LANES], pad], axis=0), LANES // 2, 1), 0.0)
    home_pre = jnp.concatenate([home[:, LANES:] + b1, jnp.zeros((8 - per, hid), F32)], axis=0)
    home_dz2 = home_g.astype(BF16)
    w2 = w2_ref[...]
    home_dy = jnp.where(home_pre > 0, dot(home_dz2, w2, 1, 1), 0.0)
    s2[...] = home_dy[:per]
    send_all(groups, me, [("b", s2, r2, snd[1], rcv[1])])

    back = jnp.where(half, r1[:, :, :LANES].reshape(halo, LANES), 0.0)
    dz2 = (g2_ref[...] + exact3(pick_ref[...], split3(back))).astype(BF16)
    pre = pre_ref[...]
    dy1 = jnp.where(plain & (pre > 0), dot(dz2, w2, 1, 1), 0.0)
    hidden = jnp.where(plain, jax.nn.relu(pre), 0.0).astype(BF16)
    home_hidden = jax.nn.relu(home_pre).astype(BF16)
    gw2 = dot(hidden, dz2, 0, 0) + dot(home_hidden, home_dz2, 0, 0)
    s3[...] = gw2.reshape(groups, per, LANES)
    s4[:, :hid] = dy1.sum(axis=0, keepdims=True) + home_dy.sum(axis=0, keepdims=True)
    s4[:, hid:] = d_ref[:own, :].sum(axis=0, keepdims=True)
    send_all(groups, me, [("a", s3, r3, snd[2], rcv[2]), ("b", s4, r4, snd[3], rcv[3])])
    for ref, piece in zip(range(3), split3(dy1)):
        dy_ref[ref, :own, :] = piece
    chunk = 256

    def own_part(i, carry):
        rows = pl.ds(pl.multiple_of(i * chunk, chunk), chunk)
        g1_ref[rows, :] = full6([a[rows, :own] for a in adj], [dy_ref[p, :own, :] for p in range(3)])
        return carry

    lax.fori_loop(0, (first_hub + hubs) // chunk, own_part, 0)
    wait_all(groups, r2, rcv[1], True)
    for ref, piece in zip(range(3), split3(r2[...].reshape(hubs, hid))):
        dy_ref[ref, own:, :] = piece

    def hub_part(rows):
        return g1_ref[rows, :] + full6([a[rows, own:] for a in adj], [dy_ref[p, own:, :] for p in range(3)])

    s5[:, :per, :] = hub_part(slice(own, first_hub)).reshape(groups, per, hid)
    s5[:, per:, :] = hub_part(slice(first_hub, first_hub + hubs)).reshape(groups, per, hid)
    send_all(groups, me, [("a", s5, r5, snd[4], rcv[4])])

    g1_ref[:chunk, :] = hub_part(slice(0, chunk))
    g1_ref[chunk:own, :] = hub_part(slice(chunk, own))
    wait_all(groups, r3, rcv[2], True)
    wait_all(groups, r4, rcv[3], True)
    bias_ref[...] = r4[...].sum(axis=0)
    s7[per:, :] = r3[...].sum(axis=0)
    wait_all(groups, r5, rcv[4], True)
    home_dz1 = jnp.concatenate([r5[:, per:, :].sum(axis=0), jnp.zeros((8 - per, hid), F32)], axis=0).astype(BF16)
    w1 = w1_ref[...]
    s7[:per, :] = dot(home_dz1, w1, 1, 1)[:per]
    back = r5[:, :per, :].reshape(halo, hid)
    dz1 = g1_ref[:own, :] + exact3(pick_ref[...], split3(back))
    dz1 = jnp.where(plain, dz1, 0.0).astype(BF16)
    gw1 = dot(dz1, x_ref[...], 0, 0) + dot(home_dz1, home_x_ref[...], 0, 0)
    s6[...] = gw1.reshape(groups, per, LANES)
    send_all(groups, me, [("a", s6, r6, snd[5], rcv[5]), ("b", s7, r7, snd[6], rcv[6])])

    dx = dot(dz1, w1, 1, 1)
    wait_all(groups, r6, rcv[5], True)
    s8[...] = r6[...].sum(axis=0)
    send_all(groups, me, [("b", s8, gw1_ref, snd[7], rcv[7])])

    wait_all(groups, r7, rcv[6], True)
    gw2_ref[...] = r7[:, per:, :]
    dx_ref[...] = dx + exact3(sel_ref[...], split3(r7[:, :per, :].reshape(hubs, LANES)))
    for buf, sem in zip((r1, r2, r3, r4, r5, r6, r7, gw1_ref), snd):
        wait_all(groups, buf, sem, False)
    wait_all(groups, gw1_ref, rcv[7], True)


def main_call(groups, own, halo, hubs, *args):
    hid = args[8].shape[1]
    per = hubs // groups
    vmem = pl.BlockSpec(memory_space=pltpu.VMEM)
    blocks = [(per, LANES + hid), (per, hid), (per, LANES), (1, hid + LANES), (2 * per, hid), (per, LANES), (2 * per, LANES), (per, LANES)]
    kinds = "ababaabb"
    sends = [pltpu.VMEM(((groups,) if k == "a" else ()) + b, F32) for k, b in zip(kinds, blocks)]
    recvs = [pltpu.VMEM((groups,) + b, F32) for b in blocks[:-1]]
    return pl.pallas_call(
        functools.partial(main_kernel, groups, own, halo, hubs),
        out_shape=[
            jax.ShapeDtypeStruct((own, LANES), F32),
            jax.ShapeDtypeStruct((groups, per, LANES), F32),
            jax.ShapeDtypeStruct((groups, per, LANES), F32),
            jax.ShapeDtypeStruct((1, hid + LANES), F32),
        ],
        in_specs=[vmem] * len(args),
        out_specs=[vmem] * 4,
        scratch_shapes=sends + recvs + [
            pltpu.VMEM((own, hid), F32),
            pltpu.VMEM((own, LANES), F32),
            pltpu.VMEM((own + halo + hubs, hid), F32),
            pltpu.VMEM((3, own + hubs, hid), BF16),
        ] + [pltpu.SemaphoreType.DMA] * 16,
        compiler_params=pltpu.CompilerParams(collective_id=2, has_side_effects=True, vmem_limit_bytes=56 * 2 ** 20),
        name="main_exchange",
    )(*args)


def pad_cols(a):
    return jnp.pad(a, ((0, 0), (0, LANES - a.shape[1])))


def solution(mesh):
    groups = mesh.shape["graph"]

    def device_step(x, dst, src, w, send, hub_ids, w_first, b_first, w_second, dy):
        own, feat_in = x.shape
        feat_out = dy.shape[1]
        hid = w_first.shape[1]
        halo, hubs = send.shape[0], hub_ids.shape[0]
        slots, dsts = own + halo + hubs, own + hubs
        me = lax.axis_index("graph")
        own_iota = jnp.arange(own, dtype=jnp.int32)
        is_hub = (hub_ids - me * own)[:, None] == own_iota[None, :]
        code = jnp.sum(jnp.where(is_hub, jnp.arange(1, hubs + 1, dtype=jnp.int32)[:, None], 0), axis=0)
        hub_f = is_hub.astype(F32)
        hub_b = is_hub.astype(BF16)
        pick_b = (send[:, None] == own_iota[None, :]).astype(BF16)
        plain = (code == 0)[:, None]

        x_pad = jnp.concatenate([x, code[:, None].astype(BF16), jnp.zeros((own, LANES - feat_in - 1), BF16)], axis=1)
        dy_pad = pad_cols(dy)
        halo_x = dot(pick_b, x_pad).astype(BF16)
        hub_x = dot(hub_b, x_pad).astype(BF16)
        hub_d = dot(hub_f, dy_pad, precision=HI)
        halo_x, hub_x, hub_d = exchange(
            groups, "aaa", [v.reshape(groups, -1, LANES) for v in (halo_x, hub_x, hub_d)], 0)
        halo_x = halo_x.reshape(halo, LANES)
        home_x = hub_x.astype(F32).sum(axis=0).astype(BF16)
        hub_x, hub_d = exchange(groups, "bb", [home_x, hub_d.sum(axis=0)], 1)
        hub_x, hub_d = hub_x.reshape(hubs, LANES), hub_d.reshape(hubs, LANES)

        halo_code = halo_x[:, feat_in].astype(jnp.int32)
        hub_base = own + halo - 1
        tables = jnp.concatenate([
            jnp.where(code > 0, own - 1 + code, own_iota),
            jnp.where(code > 0, hub_base + code, own_iota),
            jnp.where(halo_code > 0, hub_base + halo_code, own + jnp.arange(halo, dtype=jnp.int32)),
        ]).reshape(-1, LANES)
        keys, lanes = edge_keys(dst, src, tables, own)
        adj = build_adjacency(keys, lanes, w, slots, dsts)

        w1_pad = jnp.pad(w_first, ((0, LANES - feat_in), (0, 0)))
        w2_pad = pad_cols(w_second)
        zt = dot(w1_pad, jnp.concatenate([x_pad, halo_x, hub_x], axis=0), 0, 1).astype(BF16)
        d_ext = jnp.concatenate([dy_pad, hub_d], axis=0)
        pick_t = (own_iota[:, None] == send[None, :]).astype(BF16)
        sel_t = (own_iota[:, None] == (hub_ids - me * own)[None, :]).astype(BF16)
        dx, gw1, gw2, bias = main_call(
            groups, own, halo, hubs, *adj, zt, d_ext, pick_t, sel_t, plain.astype(jnp.int32), b_first[None, :],
            w1_pad, w2_pad, x_pad, jnp.pad(home_x, ((0, 8 - home_x.shape[0]), (0, 0))))
        return (
            dx[:, :feat_in],
            gw1.reshape(hid, LANES)[:, :feat_in].T,
            gw2.reshape(hid, LANES)[:, :feat_out],
            bias[0, :hid],
            bias[0, hid:hid + feat_out],
        )

    rows, flat = P(("data", "graph"), None), P(("data", "graph"))
    return jax.shard_map(
        device_step,
        mesh=mesh,
        in_specs=(rows, flat, flat, flat, flat, P("data"), P(), P(), P(), rows),
        out_specs=(rows, P("data", None), P("data", None), P("data"), P("data")),
        check_vma=False,
    )
```

```python
import functools

import jax
import jax.numpy as jnp
from jax import lax
from jax.experimental import pallas as pl
from jax.experimental.pallas import tpu as pltpu
from jax.sharding import PartitionSpec as P

BF16 = jnp.bfloat16
F32 = jnp.float32
HI = lax.Precision.HIGHEST
LANES = 128
MESH = pl.DeviceIdType.MESH


def dot(a, b, ca=1, cb=0, precision=None):
    return lax.dot_general(a, b, (((ca,), (cb,)), ((), ())), precision=precision, preferred_element_type=F32)


def split3(a):
    hi = a.astype(BF16)
    rest = a - hi.astype(F32)
    mid = rest.astype(BF16)
    return hi, mid, (rest - mid.astype(F32)).astype(BF16)


def exact3(sel, pieces, ca=1):
    return dot(sel, pieces[2], ca) + dot(sel, pieces[1], ca) + dot(sel, pieces[0], ca)


def full6(a, b):
    low = dot(a[0], b[2]) + dot(a[2], b[0]) + dot(a[1], b[1])
    return low + (dot(a[0], b[1]) + dot(a[1], b[0])) + dot(a[0], b[0])


def wait_all(groups, buf, sem, whole):
    part = buf if whole else buf.at[pl.ds(0, groups - 1)]
    pltpu.make_async_copy(part, part, sem).wait()


def send_all(groups, me, items):
    def send(i, carry):
        peer = jnp.bitwise_xor(me, i)
        for kind, src, dst, send_sem, recv_sem in items:
            pltpu.make_async_remote_copy(
                src_ref=src.at[peer] if kind == "a" else src,
                dst_ref=dst.at[me],
                send_sem=send_sem,
                recv_sem=recv_sem,
                device_id=(0, peer),
                device_id_type=MESH,
            ).start()
        return carry

    lax.fori_loop(1, groups, send, 0)
    for kind, src, dst, _, recv_sem in items:
        pltpu.make_async_copy(src.at[me] if kind == "a" else src, dst.at[me], recv_sem).start()


def greet_all(groups, me):
    barrier = pltpu.get_barrier_semaphore()

    def greet(i, carry):
        pl.semaphore_signal(barrier, inc=1, device_id=(0, jnp.bitwise_xor(me, i)), device_id_type=MESH)
        return carry

    lax.fori_loop(1, groups, greet, 0)
    return barrier


def padded(ref, rows, cols):
    a = ref[...]
    if cols > a.shape[1]:
        a = jnp.concatenate([a, jnp.zeros((a.shape[0], cols - a.shape[1]), a.dtype)], axis=1)
    if rows > a.shape[0]:
        a = jnp.concatenate([a, jnp.zeros((rows - a.shape[0], cols), a.dtype)], axis=0)
    return a


def rows_to_blocks(a, groups):
    return a.reshape(groups, a.shape[0] // groups, a.shape[1])


SRC_BLOCK, DST_BLOCK = 128, 256
BUCKET = SRC_BLOCK * DST_BLOCK


def first_kernel(groups, own, halo, hubs, x_ref, dy_ref, send_ref, hub_ref, w1_ref, dst_ref, src_ref,
                 key_ref, bound_ref, zt_ref, d_ref, xp_ref, home_ref,
                 sx, sd, hx, hd, rx, rd, gx, gd, *sems):
    snd, rcv = sems[:4], sems[4:]
    per = hubs // groups
    feat_in = x_ref.shape[1]
    me = lax.axis_index("graph")
    barrier = greet_all(groups, me)
    lane = lax.broadcasted_iota(jnp.int32, (1, LANES), 1)
    own_row = lax.broadcasted_iota(jnp.int32, (own, 1), 0)
    pick_t = (own_row == send_ref[...]).astype(F32).astype(BF16)
    is_hub = own_row == hub_ref[...] - me * own
    sel_t = is_hub.astype(F32).astype(BF16)
    number = lax.broadcasted_iota(jnp.int32, (1, hubs), 1) + 1
    code = jnp.sum(jnp.where(is_hub, number, 0).astype(F32), axis=1, keepdims=True)
    x = padded(x_ref, own, LANES)
    x = jnp.where(lane == feat_in, code, x.astype(F32)).astype(BF16)
    xp_ref[...] = x
    dy = padded(dy_ref, own, LANES)
    d_ref[:own, :] = dy
    picked = dot(jnp.concatenate([pick_t, sel_t], axis=1), jnp.concatenate((x,) + split3(dy), axis=1), 0, 0)
    hub_d = picked[halo:, 3 * LANES:] + picked[halo:, 2 * LANES:3 * LANES] + picked[halo:, LANES:2 * LANES]
    sx[:, :per, :] = rows_to_blocks(picked[:halo, :LANES], groups).astype(BF16)
    sx[:, per:, :] = rows_to_blocks(picked[halo:, :LANES], groups).astype(BF16)
    sd[...] = rows_to_blocks(hub_d, groups)
    pl.semaphore_wait(barrier, groups - 1)
    send_all(groups, me, [("a", sx, rx, snd[0], rcv[0]), ("a", sd, rd, snd[1], rcv[1])])

    numbers = jnp.broadcast_to(number.astype(F32), (8, hubs)).astype(BF16)
    code_row = dot(numbers, sel_t, 1, 1)[:1].astype(jnp.int32)
    w1_t = padded(w1_ref, LANES, w1_ref.shape[1]).T
    zt_ref[:, :own] = dot(w1_t, x, 1, 1).astype(BF16)
    wait_all(groups, rx, rcv[0], True)
    wait_all(groups, rd, rcv[1], True)
    got = rx[...].astype(F32)
    home_x = got[:, per:, :].sum(axis=0)
    hx[...] = home_x.astype(BF16)
    hd[...] = rd[...].sum(axis=0)
    send_all(groups, me, [("b", hx, gx, snd[2], rcv[2]), ("b", hd, gd, snd[3], rcv[3])])

    home_ref[...] = jnp.concatenate([home_x, jnp.zeros((8 - per, LANES), F32)], axis=0).astype(BF16)
    halo_x = got[:, :per, :].reshape(halo, LANES).astype(BF16)
    zt_ref[:, own:own + halo] = dot(w1_t, halo_x, 1, 1).astype(BF16)
    column = jnp.broadcast_to(jnp.where(lane == feat_in, 1.0, 0.0), (8, LANES)).astype(BF16)
    halo_code = dot(column, halo_x, 1, 1)[:1].astype(jnp.int32)
    hub_base = own + halo - 1
    own_ids = lax.broadcasted_iota(jnp.int32, (1, own), 1)
    halo_ids = lax.broadcasted_iota(jnp.int32, (1, halo), 1) + own
    dst_table = jnp.where(code_row > 0, own - 1 + code_row, own_ids)
    src_table = jnp.concatenate([
        jnp.where(code_row > 0, hub_base + code_row, own_ids),
        jnp.where(halo_code > 0, hub_base + halo_code, halo_ids)], axis=1)
    block = 32
    steps = dst_ref.shape[0] // block
    tops = (own + hubs) // DST_BLOCK
    buckets = (own + halo + hubs) // SRC_BLOCK * tops

    def rename(ids, table):
        at = jnp.bitwise_and(ids, LANES - 1)
        top = jnp.right_shift(ids, 7)
        out = ids
        for t in range(table.shape[1] // LANES):
            row = jnp.broadcast_to(table[:, t * LANES:(t + 1) * LANES], ids.shape)
            out = jnp.where(top == t, jnp.take_along_axis(row, at, axis=1), out)
        return out

    def keys(i, carry):
        rows = pl.ds(pl.multiple_of(i * block, block), block)
        dst = rename(dst_ref[rows, :], dst_table)
        src = rename(src_ref[rows, :], src_table)
        bucket = jnp.right_shift(src, 7) * tops + jnp.right_shift(dst, 8)
        key = bucket * BUCKET + jnp.bitwise_and(src, SRC_BLOCK - 1) * DST_BLOCK + jnp.bitwise_and(dst, DST_BLOCK - 1)
        key_ref[rows, :] = key
        return tuple(
            c + jnp.sum(jnp.where(bucket < b, 1, 0).reshape(block // 8, 8, LANES), axis=0) for b, c in enumerate(carry))

    counts = lax.fori_loop(0, steps, keys, tuple(jnp.zeros((8, LANES), jnp.int32) for _ in range(buckets + 1)))
    bounds = jnp.zeros((8, LANES), F32)
    for b, c in enumerate(counts):
        total = jnp.sum(jnp.sum(c.astype(F32), axis=0, keepdims=True), axis=1, keepdims=True)
        bounds = jnp.where(lane == b, total, bounds)
    bound_ref[...] = bounds.astype(jnp.int32)
    wait_all(groups, gx, rcv[2], True)
    wait_all(groups, gd, rcv[3], True)
    hub_x = gx[...].astype(F32).reshape(hubs, LANES).astype(BF16)
    zt_ref[:, own + halo:] = dot(w1_t, hub_x, 1, 1).astype(BF16)
    d_ref[own:, :] = gd[...].reshape(hubs, LANES)
    for buf, sem in zip((rx, rd, gx, gd), snd):
        wait_all(groups, buf, sem, False)


def first_call(groups, own, halo, hubs, hid, *args):
    per = hubs // groups
    edge_rows = args[-1].shape[0]
    vmem = pl.BlockSpec(memory_space=pltpu.VMEM)
    shape = jax.ShapeDtypeStruct
    return pl.pallas_call(
        functools.partial(first_kernel, groups, own, halo, hubs),
        out_shape=[
            shape((edge_rows, LANES), jnp.int32),
            shape((8, LANES), jnp.int32),
            shape((hid, own + halo + hubs), BF16),
            shape((own + hubs, LANES), F32),
            shape((own, LANES), BF16),
            shape((8, LANES), BF16),
        ],
        in_specs=[vmem] * len(args),
        out_specs=[vmem] * 6,
        scratch_shapes=[
            pltpu.VMEM((groups, 2 * per, LANES), BF16),
            pltpu.VMEM((groups, per, LANES), F32),
            pltpu.VMEM((per, LANES), BF16),
            pltpu.VMEM((per, LANES), F32),
            pltpu.VMEM((groups, 2 * per, LANES), BF16),
            pltpu.VMEM((groups, per, LANES), F32),
            pltpu.VMEM((groups, per, LANES), BF16),
            pltpu.VMEM((groups, per, LANES), F32),
        ] + [pltpu.SemaphoreType.DMA] * 8,
        compiler_params=pltpu.CompilerParams(collective_id=0, has_side_effects=True),
        name="first_exchange",
    )(*args)


CHUNK_ROWS, UNROLL = 2, 8


def adjacency_kernel(slots, dsts, bound_ref, key_ref, w_ref, hi_ref, mid_ref, low_ref, acc_ref, pair_ref):
    tops = dsts // DST_BLOCK
    buckets = slots // SRC_BLOCK * tops
    size = CHUNK_ROWS * LANES
    src_ids = lax.broadcasted_iota(jnp.int32, (SRC_BLOCK, LANES), 0).astype(F32).astype(BF16)
    dst_ids = lax.broadcasted_iota(jnp.int32, (DST_BLOCK, LANES), 0).astype(F32).astype(BF16)
    one, zero = jnp.ones((), BF16), jnp.zeros((), BF16)

    def clear(i, carry):
        acc_ref[pl.ds(pl.multiple_of(i * SRC_BLOCK, SRC_BLOCK), SRC_BLOCK), :] = jnp.zeros((SRC_BLOCK, DST_BLOCK), F32)
        return carry

    lax.fori_loop(0, buckets, clear, 0)

    def list_pairs(b, at):
        low, high = bound_ref[0, b], bound_ref[0, b + 1]
        start = low // size
        count = jnp.where(high > low, (high + size - 1) // size - start, 0)

        def put(i, carry):
            pair_ref[at + i] = b * 1024 + start + i
            return carry

        lax.fori_loop(0, count, put, 0)
        return at + count

    total = lax.fori_loop(0, buckets, list_pairs, 0)
    for i in range(UNROLL - 1):
        pair_ref[total + i] = buckets * 1024

    def step(it, carry):
        work = []
        for u in range(UNROLL):
            pair = pair_ref[it * UNROLL + u]
            b, c = jnp.right_shift(pair, 10), jnp.bitwise_and(pair, 1023)
            lhs, rhs = [], []
            for r in range(CHUNK_ROWS):
                rel = key_ref[pl.ds(c * CHUNK_ROWS + r, 1), :] - b * BUCKET
                weight = w_ref[pl.ds(c * CHUNK_ROWS + r, 1), :]
                src = jnp.right_shift(rel, 8)
                src = jnp.where((src >= 0) & (src < SRC_BLOCK), src, 512).astype(F32).astype(BF16)
                dst = jnp.bitwise_and(rel, DST_BLOCK - 1).astype(F32).astype(BF16)
                hit = src_ids == jnp.broadcast_to(src, src_ids.shape)
                lhs.append(jnp.concatenate(
                    [jnp.where(hit, jnp.broadcast_to(p, src_ids.shape), zero) for p in split3(weight)], axis=0))
                rhs.append(jnp.where(dst_ids == jnp.broadcast_to(dst, dst_ids.shape), one, zero))
            work.append((b, jnp.concatenate(lhs, axis=1), jnp.concatenate(rhs, axis=1)))
        outs = [dot(lhs, rhs, 1, 1) for _, lhs, rhs in work]
        for (b, _, _), out in zip(work, outs):
            rows = pl.ds(pl.multiple_of(b * SRC_BLOCK, SRC_BLOCK), SRC_BLOCK)
            acc_ref[rows, :] += out[2 * SRC_BLOCK:] + out[SRC_BLOCK:2 * SRC_BLOCK] + out[:SRC_BLOCK]
        return carry

    lax.fori_loop(0, (total + UNROLL - 1) // UNROLL, step, 0)
    for b in range(buckets):
        rows = slice(b // tops * SRC_BLOCK, (b // tops + 1) * SRC_BLOCK)
        cols = slice(b % tops * DST_BLOCK, (b % tops + 1) * DST_BLOCK)
        for ref, piece in zip((hi_ref, mid_ref, low_ref), split3(acc_ref[b * SRC_BLOCK:(b + 1) * SRC_BLOCK, :])):
            ref[rows, cols] = piece


def adjacency(bounds, keys, weights, slots, dsts):
    edges = weights.shape[0]
    buckets = slots // SRC_BLOCK * (dsts // DST_BLOCK)
    vmem = pl.BlockSpec(memory_space=pltpu.VMEM)
    return pl.pallas_call(
        functools.partial(adjacency_kernel, slots, dsts),
        out_shape=[jax.ShapeDtypeStruct((slots, dsts), BF16)] * 3,
        in_specs=[pl.BlockSpec(memory_space=pltpu.SMEM), vmem, vmem],
        out_specs=[vmem] * 3,
        scratch_shapes=[
            pltpu.VMEM(((buckets + 1) * SRC_BLOCK, DST_BLOCK), F32),
            pltpu.SMEM((edges // (CHUNK_ROWS * LANES) + buckets + UNROLL,), jnp.int32),
        ],
        name="adjacency",
    )(bounds, keys.reshape(-1, LANES), weights.reshape(-1, LANES))


def main_kernel(groups, own, halo, hubs, hi_ref, mid_ref, low_ref, zt_ref, d_ref, send_ref, hub_ref, b1_ref,
                w1_ref, w2_ref, x_ref, home_x_ref,
                dx_ref, gw1_ref, gw2_ref, bias_ref,
                s1, s2, s3, s4, s5, s6, s7, s8, r1, r2, r3, r4, r5, r6, r7, pre_ref, g2_ref, g1_ref, dy_ref, *sems):
    snd, rcv = sems[:8], sems[8:]
    adj = (hi_ref, mid_ref, low_ref)
    per = hubs // groups
    hid = b1_ref.shape[1]
    first_hub = own + halo
    me = lax.axis_index("graph")
    barrier = greet_all(groups, me)
    lane = lax.broadcasted_iota(jnp.int32, (1, LANES), 1)
    half = lane < LANES // 2

    def forward(cols):
        zt = zt_ref[...]
        return dot(zt, low_ref[:, cols]) + dot(zt, mid_ref[:, cols]) + dot(zt, hi_ref[:, cols])

    dh, dm, dl = split3(d_ref[...])
    d_two = (dh.astype(F32) + pltpu.roll(dm.astype(F32), LANES // 2, 1)).astype(BF16)
    d_four = jnp.concatenate([d_two, dl], axis=1)

    def grad_out_sums(rows):
        a = dot(hi_ref[rows, :], d_four)
        t = a[:, :LANES] + a[:, LANES:] + dot(mid_ref[rows, :], d_two) + dot(low_ref[rows, :], dh)
        return jnp.where(half, t + pltpu.roll(t, LANES // 2, 1), 0.0)

    y_hub = forward(slice(own, own + hubs)).T
    s1[:, :, LANES:] = y_hub.reshape(groups, per, hid)
    g2_halo = grad_out_sums(slice(own, first_hub))
    g2_hub = grad_out_sums(slice(first_hub, first_hub + hubs))
    s1[:, :, :LANES] = (g2_halo + pltpu.roll(g2_hub, LANES // 2, 1)).reshape(groups, per, LANES)
    pl.semaphore_wait(barrier, groups - 1)
    send_all(groups, me, [("a", s1, r1, snd[0], rcv[0])])

    b1 = b1_ref[...]
    own_row = lax.broadcasted_iota(jnp.int32, (own, 1), 0)
    pick_t = (own_row == send_ref[...]).astype(F32).astype(BF16)
    sel_f = (own_row == hub_ref[...] - me * own).astype(F32)
    sel_t = sel_f.astype(BF16)
    plain = jnp.sum(sel_f, axis=1, keepdims=True) == 0
    pre_ref[...] = forward(slice(0, own)).T + b1
    g2_ref[...] = grad_out_sums(slice(0, own))
    wait_all(groups, r1, rcv[0], True)
    home = r1[...].sum(axis=0)
    pad = jnp.zeros((8 - per, LANES), F32)
    home_g = jnp.where(half, pltpu.roll(jnp.concatenate([home[:, :LANES], pad], axis=0), LANES // 2, 1), 0.0)
    home_pre = jnp.concatenate([home[:, LANES:] + b1, jnp.zeros((8 - per, hid), F32)], axis=0)
    home_dz2 = home_g.astype(BF16)
    w2 = padded(w2_ref, hid, LANES)
    home_dy = jnp.where(home_pre > 0, dot(home_dz2, w2, 1, 1), 0.0)
    s2[...] = home_dy[:per]
    send_all(groups, me, [("b", s2, r2, snd[1], rcv[1])])

    back = jnp.where(half, r1[:, :, :LANES].reshape(halo, LANES), 0.0)
    dz2 = (g2_ref[...] + exact3(pick_t, split3(back))).astype(BF16)
    pre = pre_ref[...]
    dy1 = jnp.where(plain & (pre > 0), dot(dz2, w2, 1, 1), 0.0)
    hidden = jnp.where(plain, jax.nn.relu(pre), 0.0).astype(BF16)
    home_hidden = jax.nn.relu(home_pre).astype(BF16)
    gw2 = dot(hidden, dz2, 0, 0) + dot(home_hidden, home_dz2, 0, 0)
    s3[...] = gw2.reshape(groups, per, LANES)
    s4[:, :hid] = dy1.sum(axis=0, keepdims=True) + home_dy.sum(axis=0, keepdims=True)
    s4[:, hid:] = d_ref[:own, :].sum(axis=0, keepdims=True)
    send_all(groups, me, [("a", s3, r3, snd[2], rcv[2]), ("b", s4, r4, snd[3], rcv[3])])
    for ref, piece in zip(range(3), split3(dy1)):
        dy_ref[ref, :own, :] = piece
    chunk = 256

    def own_part(i, carry):
        rows = pl.ds(pl.multiple_of(i * chunk, chunk), chunk)
        g1_ref[rows, :] = full6([a[rows, :own] for a in adj], [dy_ref[p, :own, :] for p in range(3)])
        return carry

    lax.fori_loop(0, (first_hub + hubs) // chunk, own_part, 0)
    wait_all(groups, r2, rcv[1], True)
    for ref, piece in zip(range(3), split3(r2[...].reshape(hubs, hid))):
        dy_ref[ref, own:, :] = piece

    def hub_part(rows):
        return g1_ref[rows, :] + full6([a[rows, own:] for a in adj], [dy_ref[p, own:, :] for p in range(3)])

    s5[:, :per, :] = hub_part(slice(own, first_hub)).reshape(groups, per, hid)
    s5[:, per:, :] = hub_part(slice(first_hub, first_hub + hubs)).reshape(groups, per, hid)
    send_all(groups, me, [("a", s5, r5, snd[4], rcv[4])])

    g1_ref[:chunk, :] = hub_part(slice(0, chunk))
    g1_ref[chunk:own, :] = hub_part(slice(chunk, own))
    wait_all(groups, r3, rcv[2], True)
    wait_all(groups, r4, rcv[3], True)
    bias_ref[...] = r4[...].sum(axis=0)
    s7[per:, :] = r3[...].sum(axis=0)
    wait_all(groups, r5, rcv[4], True)
    home_dz1 = jnp.concatenate([r5[:, per:, :].sum(axis=0), jnp.zeros((8 - per, hid), F32)], axis=0).astype(BF16)
    w1 = padded(w1_ref, LANES, hid)
    s7[:per, :] = dot(home_dz1, w1, 1, 1)[:per]
    back = r5[:, :per, :].reshape(halo, hid)
    dz1 = g1_ref[:own, :] + exact3(pick_t, split3(back))
    dz1 = jnp.where(plain, dz1, 0.0).astype(BF16)
    gw1 = dot(dz1, x_ref[...], 0, 0) + dot(home_dz1, home_x_ref[...], 0, 0)
    s6[...] = gw1.reshape(groups, per, LANES)
    send_all(groups, me, [("a", s6, r6, snd[5], rcv[5]), ("b", s7, r7, snd[6], rcv[6])])

    dx = dot(dz1, w1, 1, 1)
    wait_all(groups, r6, rcv[5], True)
    s8[...] = r6[...].sum(axis=0)
    send_all(groups, me, [("b", s8, gw1_ref, snd[7], rcv[7])])

    wait_all(groups, r7, rcv[6], True)
    gw2_ref[...] = r7[:, per:, :]
    dx_ref[...] = dx + exact3(sel_t, split3(r7[:, :per, :].reshape(hubs, LANES)))
    for buf, sem in zip((r1, r2, r3, r4, r5, r6, r7, gw1_ref), snd):
        wait_all(groups, buf, sem, False)
    wait_all(groups, gw1_ref, rcv[7], True)


def main_call(groups, own, halo, hubs, *args):
    hid = args[7].shape[1]
    per = hubs // groups
    vmem = pl.BlockSpec(memory_space=pltpu.VMEM)
    blocks = [(per, LANES + hid), (per, hid), (per, LANES), (1, hid + LANES), (2 * per, hid), (per, LANES), (2 * per, LANES), (per, LANES)]
    kinds = "ababaabb"
    sends = [pltpu.VMEM(((groups,) if k == "a" else ()) + b, F32) for k, b in zip(kinds, blocks)]
    recvs = [pltpu.VMEM((groups,) + b, F32) for b in blocks[:-1]]
    return pl.pallas_call(
        functools.partial(main_kernel, groups, own, halo, hubs),
        out_shape=[
            jax.ShapeDtypeStruct((own, LANES), F32),
            jax.ShapeDtypeStruct((groups, per, LANES), F32),
            jax.ShapeDtypeStruct((groups, per, LANES), F32),
            jax.ShapeDtypeStruct((1, hid + LANES), F32),
        ],
        in_specs=[vmem] * len(args),
        out_specs=[vmem] * 4,
        scratch_shapes=sends + recvs + [
            pltpu.VMEM((own, hid), F32),
            pltpu.VMEM((own, LANES), F32),
            pltpu.VMEM((own + halo + hubs, hid), F32),
            pltpu.VMEM((3, own + hubs, hid), BF16),
        ] + [pltpu.SemaphoreType.DMA] * 16,
        compiler_params=pltpu.CompilerParams(collective_id=2, has_side_effects=True, vmem_limit_bytes=56 * 2 ** 20),
        name="main_exchange",
    )(*args)


def output_kernel(dx_ref, gw1_ref, gw2_ref, bias_ref, dx_out, gw1_out, gw2_out, b1_out, b2_out):
    feat_in, feat_out, hid = dx_out.shape[1], gw2_out.shape[1], gw2_out.shape[0]
    dx_out[...] = dx_ref[:, :feat_in]
    gw1_out[...] = gw1_ref[...].reshape(hid, LANES).T[:feat_in, :]
    gw2_out[...] = gw2_ref[...].reshape(hid, LANES)[:, :feat_out]
    b1_out[...] = bias_ref[:, :hid]
    b2_out[...] = bias_ref[:, hid:hid + feat_out]


def solution(mesh):
    groups = mesh.shape["graph"]

    def device_step(x, dst, src, w, send, hub_ids, w_first, b_first, w_second, dy):
        own, feat_in = x.shape
        feat_out = dy.shape[1]
        hid = w_first.shape[1]
        halo, hubs = send.shape[0], hub_ids.shape[0]
        slots, dsts = own + halo + hubs, own + hubs
        send, hub_ids = send[None, :], hub_ids[None, :]
        keys, bounds, zt, d_ext, x_pad, home_x = first_call(
            groups, own, halo, hubs, hid, x, dy, send, hub_ids, w_first, dst.reshape(-1, LANES), src.reshape(-1, LANES))
        keys, weights = lax.sort((keys.reshape(-1), w), num_keys=1, is_stable=False)
        adj = adjacency(bounds, keys, weights, slots, dsts)
        raw = main_call(
            groups, own, halo, hubs, *adj, zt, d_ext, send, hub_ids, b_first[None, :], w_first, w_second, x_pad, home_x)
        dx, gw1, gw2, gb1, gb2 = pl.pallas_call(
            output_kernel,
            out_shape=[jax.ShapeDtypeStruct(shape, F32) for shape in (
                (own, feat_in), (feat_in, hid), (hid, feat_out), (1, hid), (1, feat_out))],
            name="outputs",
        )(*raw)
        return dx, gw1, gw2, gb1[0], gb2[0]

    rows, flat = P(("data", "graph"), None), P(("data", "graph"))
    return jax.shard_map(
        device_step,
        mesh=mesh,
        in_specs=(rows, flat, flat, flat, flat, P("data"), P(), P(), P(), rows),
        out_specs=(rows, P("data", None), P("data", None), P("data"), P("data")),
        check_vma=False,
    )
```

```python
import functools

import jax
import jax.numpy as jnp
from jax import lax
from jax.experimental import pallas as pl
from jax.experimental.pallas import tpu as pltpu
from jax.sharding import PartitionSpec as P

BF16 = jnp.bfloat16
F32 = jnp.float32
HI = lax.Precision.HIGHEST
LANES = 128
MESH = pl.DeviceIdType.MESH


def dot(a, b, ca=1, cb=0, precision=None):
    return lax.dot_general(a, b, (((ca,), (cb,)), ((), ())), precision=precision, preferred_element_type=F32)


def split3(a):
    hi = a.astype(BF16)
    rest = a - hi.astype(F32)
    mid = rest.astype(BF16)
    return hi, mid, (rest - mid.astype(F32)).astype(BF16)


def exact3(sel, pieces, ca=1):
    return dot(sel, pieces[2], ca) + dot(sel, pieces[1], ca) + dot(sel, pieces[0], ca)


def exact3_right(pieces, sel):
    return dot(pieces[2], sel) + dot(pieces[1], sel) + dot(pieces[0], sel)


def sum3(pieces):
    return pieces[2].astype(F32) + pieces[1].astype(F32) + pieces[0].astype(F32)


def full6(a, b):
    low = dot(a[0], b[2]) + dot(a[2], b[0]) + dot(a[1], b[1])
    return low + (dot(a[0], b[1]) + dot(a[1], b[0])) + dot(a[0], b[0])


def partner(groups, me, i):
    low = sum(2 << k for k in range(0, groups.bit_length() - 2, 2))
    t = jnp.bitwise_xor(i - 1, 2 * low + 1)
    high = jnp.bitwise_and(jnp.right_shift(t, 1), low)
    return jnp.bitwise_xor(me, jnp.bitwise_xor(t, jnp.bitwise_xor(high, low)))


def wait_all(groups, buf, sem, whole):
    part = buf if whole else buf.at[pl.ds(0, groups - 1)]
    pltpu.make_async_copy(part, part, sem).wait()


def send_all(groups, me, items):
    def send(i, carry):
        peer = partner(groups, me, i)
        for kind, src, dst, send_sem, recv_sem in items:
            pltpu.make_async_remote_copy(
                src_ref=src.at[peer] if kind == "a" else src,
                dst_ref=dst.at[me],
                send_sem=send_sem,
                recv_sem=recv_sem,
                device_id=(0, peer),
                device_id_type=MESH,
            ).start()
        return carry

    lax.fori_loop(1, groups, send, 0)
    for kind, src, dst, _, recv_sem in items:
        pltpu.make_async_copy(src.at[me] if kind == "a" else src, dst.at[me], recv_sem).start()


def greet_all(groups, me):
    barrier = pltpu.get_barrier_semaphore()

    def greet(i, carry):
        pl.semaphore_signal(barrier, inc=1, device_id=(0, partner(groups, me, i)), device_id_type=MESH)
        return carry

    lax.fori_loop(1, groups, greet, 0)
    return barrier


def padded(ref, rows, cols):
    a = ref[...]
    if cols > a.shape[1]:
        a = jnp.concatenate([a, jnp.zeros((a.shape[0], cols - a.shape[1]), a.dtype)], axis=1)
    if rows > a.shape[0]:
        a = jnp.concatenate([a, jnp.zeros((rows - a.shape[0], cols), a.dtype)], axis=0)
    return a


SRC_BLOCK, DST_BLOCK = 128, 256
BUCKET = SRC_BLOCK * DST_BLOCK
CHUNK_ROWS, UNROLL = 2, 8


def adjacency_kernel(slots, dsts, key_ref, w_ref, acc_ref, pair_ref, bound_ref):
    tops = dsts // DST_BLOCK
    buckets = slots // SRC_BLOCK * tops
    size = CHUNK_ROWS * LANES
    src_ids = lax.broadcasted_iota(jnp.int32, (SRC_BLOCK, LANES), 0).astype(F32).astype(BF16)
    dst_ids = lax.broadcasted_iota(jnp.int32, (DST_BLOCK, LANES), 0).astype(F32).astype(BF16)
    one, zero = jnp.ones((), BF16), jnp.zeros((), BF16)

    def clear(i, carry):
        acc_ref[pl.ds(pl.multiple_of(i * SRC_BLOCK, SRC_BLOCK), SRC_BLOCK), :] = jnp.zeros((SRC_BLOCK, DST_BLOCK), F32)
        return carry

    lax.fori_loop(0, buckets, clear, 0)

    def count(i, carry):
        bucket = jnp.right_shift(key_ref[pl.ds(pl.multiple_of(i * 8, 8), 8), :], BUCKET.bit_length() - 1)
        return tuple(c + jnp.where(bucket < b + 1, 1, 0) for b, c in enumerate(carry))

    zeros = jnp.zeros((8, LANES), jnp.int32)
    counts = lax.fori_loop(0, key_ref.shape[0] // 8, count, (zeros,) * buckets)
    bound_ref[0] = 0
    for b, c in enumerate(counts):
        bound_ref[b + 1] = jnp.sum(c.astype(F32)).astype(jnp.int32)

    def list_pairs(b, at):
        low, high = bound_ref[b], bound_ref[b + 1]
        start = low // size
        count = jnp.where(high > low, (high + size - 1) // size - start, 0)

        def put(i, carry):
            pair_ref[at + i] = b * 1024 + start + i
            return carry

        lax.fori_loop(0, count, put, 0)
        return at + count

    total = lax.fori_loop(0, buckets, list_pairs, 0)
    for i in range(UNROLL - 1):
        pair_ref[total + i] = buckets * 1024

    def step(it, carry):
        work = []
        for u in range(UNROLL):
            pair = pair_ref[it * UNROLL + u]
            b, c = jnp.right_shift(pair, 10), jnp.bitwise_and(pair, 1023)
            lhs, rhs = [], []
            for r in range(CHUNK_ROWS):
                rel = key_ref[pl.ds(c * CHUNK_ROWS + r, 1), :] - b * BUCKET
                weight = w_ref[pl.ds(c * CHUNK_ROWS + r, 1), :]
                src = jnp.right_shift(rel, 8)
                src = jnp.where((src >= 0) & (src < SRC_BLOCK), src, 512).astype(F32).astype(BF16)
                dst = jnp.bitwise_and(rel, DST_BLOCK - 1).astype(F32).astype(BF16)
                hit = src_ids == jnp.broadcast_to(src, src_ids.shape)
                lhs.append(jnp.concatenate(
                    [jnp.where(hit, jnp.broadcast_to(p, src_ids.shape), zero) for p in split3(weight)], axis=0))
                rhs.append(jnp.where(dst_ids == jnp.broadcast_to(dst, dst_ids.shape), one, zero))
            work.append((b, jnp.concatenate(lhs, axis=1), jnp.concatenate(rhs, axis=1)))
        outs = [dot(lhs, rhs, 1, 1) for _, lhs, rhs in work]
        for (b, _, _), out in zip(work, outs):
            rows = pl.ds(pl.multiple_of(b * SRC_BLOCK, SRC_BLOCK), SRC_BLOCK)
            acc_ref[rows, :] += out[2 * SRC_BLOCK:] + out[SRC_BLOCK:2 * SRC_BLOCK] + out[:SRC_BLOCK]
        return carry

    lax.fori_loop(0, (total + UNROLL - 1) // UNROLL, step, 0)


def adjacency(keys, weights, slots, dsts):
    edges = weights.shape[0]
    buckets = slots // SRC_BLOCK * (dsts // DST_BLOCK)
    vmem = pl.BlockSpec(memory_space=pltpu.VMEM)
    return pl.pallas_call(
        functools.partial(adjacency_kernel, slots, dsts),
        out_shape=jax.ShapeDtypeStruct(((buckets + 1) * SRC_BLOCK, DST_BLOCK), F32),
        in_specs=[vmem, vmem],
        out_specs=vmem,
        scratch_shapes=[
            pltpu.SMEM((edges // (CHUNK_ROWS * LANES) + buckets + UNROLL,), jnp.int32),
            pltpu.SMEM((buckets + 1,), jnp.int32),
        ],
        name="adjacency",
    )(keys.reshape(-1, LANES), weights.reshape(-1, LANES))


def rows_to_blocks(a, groups):
    return a.reshape(groups, a.shape[0] // groups, a.shape[1])


def main_kernel(groups, own, halo, hubs, cells_ref, xt_ref, dyt_ref, send_ref, hub_ref, b1_ref, w1_ref, w2t_ref,
                dxt_ref, gw_ref, bias_ref,
                sx, sd, hx, hd, s1, s2, s3, s4, s5, s6, s7, s8,
                rx, rd, gx, gd, r1, r2, r3, r4, r5, r6, r7,
                raw_ref, hi_ref, mid_ref, low_ref, hubrow_ref, pt_ref, g2_ref, g1_ref, dy_ref, zt_ref, load_sem, *sems):
    count = len(sems) // 2
    snd, rcv = sems[:count], sems[count:]
    adj = (hi_ref, mid_ref, low_ref)
    per = hubs // groups
    hid = b1_ref.shape[1]
    feat_in = xt_ref.shape[0]
    first_hub = own + halo
    slots, dsts = own + halo + hubs, own + hubs
    tops = dsts // DST_BLOCK
    me = lax.axis_index("graph")
    barrier = greet_all(groups, me)
    load = pltpu.make_async_copy(cells_ref.at[pl.ds(0, raw_ref.shape[0])], raw_ref, load_sem)
    load.start()

    lane = lax.broadcasted_iota(jnp.int32, (1, LANES), 1)
    half = lane < LANES // 2
    own_row = lax.broadcasted_iota(jnp.int32, (own, 1), 0)
    pick_t = (own_row == send_ref[...]).astype(F32).astype(BF16)
    sel_f = (own_row == hub_ref[...] - me * own).astype(F32)
    sel_t = sel_f.astype(BF16)
    plain = jnp.sum(sel_f, axis=1, keepdims=True) == 0
    number = lax.broadcasted_iota(jnp.int32, (1, hubs), 1) + 1
    numbers = jnp.broadcast_to(number.astype(F32), (8, hubs)).astype(BF16)
    code_row = dot(numbers, sel_t, 1, 1)[:1]
    plain_row = code_row == 0
    xt = padded(xt_ref, LANES, own)
    feature = lax.broadcasted_iota(jnp.int32, (LANES, 1), 0)
    xt = jnp.where(feature == feat_in, code_row, xt.astype(F32)).astype(BF16)
    dyt = padded(dyt_ref, LANES, own)
    picked = dot(jnp.concatenate((xt,) + split3(dyt), axis=0), jnp.concatenate([pick_t, sel_t], axis=1))
    hub_dt = picked[3 * LANES:, halo:] + picked[2 * LANES:3 * LANES, halo:] + picked[LANES:2 * LANES, halo:]
    sx[:, :per, :] = rows_to_blocks(picked[:LANES, :halo].T, groups).astype(BF16)
    sx[:, per:, :] = rows_to_blocks(picked[:LANES, halo:].T, groups).astype(BF16)
    sd[...] = rows_to_blocks(hub_dt.T, groups)
    pl.semaphore_wait(barrier, groups - 1)
    send_all(groups, me, [("a", sx, rx, snd[0], rcv[0]), ("a", sd, rd, snd[1], rcv[1])])

    w1 = padded(w1_ref, LANES, hid)
    w1_t = w1.astype(F32).T.astype(BF16)
    zt_ref[:, :own] = dot(w1_t, xt).astype(BF16)
    dy = dyt.T
    load.wait()

    def rename(i, carry):
        cell = [raw_ref[pl.ds(pl.multiple_of((i * tops + j) * SRC_BLOCK, SRC_BLOCK), SRC_BLOCK), :] for j in range(tops)]
        mine = jnp.concatenate(cell[:own // DST_BLOCK], axis=1)
        hub = jnp.concatenate(cell[own // DST_BLOCK:], axis=1) + exact3_right(split3(mine), sel_t)
        rows = pl.ds(pl.multiple_of(i * SRC_BLOCK, SRC_BLOCK), SRC_BLOCK)
        new = jnp.concatenate([jnp.where(plain_row, mine, 0.0), hub], axis=1)
        for ref, piece in zip(adj, split3(new)):
            ref[rows, :] = piece
        return carry

    lax.fori_loop(0, slots // SRC_BLOCK, rename, 0)
    sel = sel_f.T.astype(BF16)
    for j in range(tops):
        cols = slice(j * DST_BLOCK, (j + 1) * DST_BLOCK)
        base = first_hub // SRC_BLOCK
        old = jnp.concatenate(
            [sum3([a[(base + k) * SRC_BLOCK:(base + k + 1) * SRC_BLOCK, cols] for a in adj])
             for k in range(hubs // SRC_BLOCK)], axis=0)
        hubrow_ref[:, cols] = old + exact3(sel, [a[:own, cols] for a in adj])
    for a in adj:
        a[:own, :] = jnp.where(plain, a[:own, :].astype(F32), 0.0).astype(BF16)
    wait_all(groups, rx, rcv[0], True)
    wait_all(groups, rd, rcv[1], True)
    got = rx[...].astype(F32)
    home_x = got[:, per:, :].sum(axis=0)
    hx[...] = home_x.astype(BF16)
    hd[...] = rd[...].sum(axis=0)
    send_all(groups, me, [("b", hx, gx, snd[2], rcv[2]), ("b", hd, gd, snd[3], rcv[3])])

    home_x = jnp.concatenate([home_x, jnp.zeros((8 - per, LANES), F32)], axis=0).astype(BF16)
    halo_x = got[:, :per, :].reshape(halo, LANES)
    halo_code = halo_x[:, feat_in:feat_in + 1]
    halo_x = halo_x.astype(BF16)
    zt_ref[:, own:first_hub] = dot(w1_t, halo_x, 1, 1).astype(BF16)
    column = jnp.broadcast_to(jnp.where(lane == feat_in, 1.0, 0.0), (8, LANES)).astype(BF16)
    halo_row = dot(column, halo_x, 1, 1)[:1].astype(jnp.int32)
    halo_sel = (lax.broadcasted_iota(jnp.int32, (hubs, 1), 0) + 1 == halo_row).astype(F32).astype(BF16)
    for j in range(tops):
        cols = slice(j * DST_BLOCK, (j + 1) * DST_BLOCK)
        new = hubrow_ref[:, cols] + exact3(halo_sel, [a[own:first_hub, cols] for a in adj])
        for a, piece in zip(adj, split3(new)):
            a[first_hub:, cols] = piece
    for a in adj:
        a[own:first_hub, :] = jnp.where(halo_code == 0, a[own:first_hub, :].astype(F32), 0.0).astype(BF16)

    def forward(rows, cols):
        zt = zt_ref[:, rows]
        return dot(zt, low_ref[rows, cols]) + dot(zt, mid_ref[rows, cols]) + dot(zt, hi_ref[rows, cols])

    def pack(d):
        dh, dm, dl = split3(d)
        d_two = (dh.astype(F32) + pltpu.roll(dm.astype(F32), LANES // 2, 1)).astype(BF16)
        return jnp.concatenate([d_two, dl], axis=1), d_two, dh

    def grad_out_sums(rows, cols, packed):
        a = dot(hi_ref[rows, cols], packed[0])
        t = a[:, :LANES] + a[:, LANES:] + dot(mid_ref[rows, cols], packed[1]) + dot(low_ref[rows, cols], packed[2])
        return jnp.where(half, t + pltpu.roll(t, LANES // 2, 1), 0.0)

    own_cols, hub_cols = slice(0, own), slice(own, dsts)
    pt_ref[...] = forward(slice(0, first_hub), slice(0, dsts))
    d_own = pack(dy)
    g2_ref[...] = grad_out_sums(slice(0, slots), own_cols, d_own)
    wait_all(groups, gx, rcv[2], True)
    wait_all(groups, gd, rcv[3], True)
    hub_x = gx[...].astype(F32).reshape(hubs, LANES).astype(BF16)
    zt_ref[:, first_hub:] = dot(w1_t, hub_x, 1, 1).astype(BF16)
    d_hub = pack(gd[...].reshape(hubs, LANES))
    hub_slots = slice(first_hub, slots)
    y_hub = (pt_ref[:, own:] + forward(hub_slots, hub_cols)).T
    s1[:, :, LANES:] = rows_to_blocks(y_hub, groups)
    g2_halo = g2_ref[own:first_hub, :] + grad_out_sums(slice(own, first_hub), hub_cols, d_hub)
    g2_hub = g2_ref[first_hub:, :] + grad_out_sums(hub_slots, hub_cols, d_hub)
    s1[:, :, :LANES] = rows_to_blocks(g2_halo + pltpu.roll(g2_hub, LANES // 2, 1), groups)
    send_all(groups, me, [("a", s1, r1, snd[4], rcv[4])])

    b1 = b1_ref[...]
    w2t = padded(w2t_ref, LANES, hid)
    pre = (pt_ref[:, :own] + forward(hub_slots, own_cols)).T + b1
    g2_own = g2_ref[:own, :] + grad_out_sums(slice(0, own), hub_cols, d_hub)
    hidden = jnp.where(plain, jax.nn.relu(pre), 0.0).astype(BF16)
    live = plain & (pre > 0)
    wait_all(groups, r1, rcv[4], True)
    home = r1[...].sum(axis=0)
    pad = jnp.zeros((8 - per, LANES), F32)
    home_g = jnp.where(half, pltpu.roll(jnp.concatenate([home[:, :LANES], pad], axis=0), LANES // 2, 1), 0.0)
    home_pre = jnp.concatenate([home[:, LANES:] + b1, jnp.zeros((8 - per, hid), F32)], axis=0)
    home_dz2 = home_g.astype(BF16)
    home_dy = jnp.where(home_pre > 0, dot(home_dz2, w2t), 0.0)
    s2[...] = home_dy[:per]
    send_all(groups, me, [("b", s2, r2, snd[5], rcv[5])])

    back = jnp.where(half, r1[:, :, :LANES].reshape(halo, LANES), 0.0)
    dz2 = (g2_own + exact3(pick_t, split3(back))).astype(BF16)
    dy1 = jnp.where(live, dot(dz2, w2t), 0.0)
    home_hidden = jax.nn.relu(home_pre).astype(BF16)
    gw2 = dot(dz2, hidden, 0, 0) + dot(home_dz2, home_hidden, 0, 0)
    s3[...] = rows_to_blocks(gw2, groups)
    s4[:, :hid] = dy1.sum(axis=0, keepdims=True) + home_dy.sum(axis=0, keepdims=True)
    s4[:, hid:] = dy.sum(axis=0, keepdims=True)
    send_all(groups, me, [("a", s3, r3, snd[6], rcv[6]), ("b", s4, r4, snd[7], rcv[7])])
    for p, piece in enumerate(split3(dy1)):
        dy_ref[p, :own, :] = piece
    chunk = 256

    def own_part(i, carry):
        rows = pl.ds(pl.multiple_of(i * chunk, chunk), chunk)
        g1_ref[rows, :] = full6([a[rows, :own] for a in adj], [dy_ref[p, :own, :] for p in range(3)])
        return carry

    lax.fori_loop(0, slots // chunk, own_part, 0)
    wait_all(groups, r2, rcv[5], True)
    for p, piece in enumerate(split3(r2[...].reshape(hubs, hid))):
        dy_ref[p, own:, :] = piece

    def hub_part(rows):
        return g1_ref[rows, :] + full6([a[rows, own:] for a in adj], [dy_ref[p, own:, :] for p in range(3)])

    s5[:, :per, :] = rows_to_blocks(hub_part(slice(own, first_hub)), groups)
    s5[:, per:, :] = rows_to_blocks(hub_part(hub_slots), groups)
    send_all(groups, me, [("a", s5, r5, snd[8], rcv[8])])

    g1_ref[:chunk, :] = hub_part(slice(0, chunk))
    g1_ref[chunk:own, :] = hub_part(slice(chunk, own))
    wait_all(groups, r3, rcv[6], True)
    wait_all(groups, r4, rcv[7], True)
    bias_ref[...] = r4[...].sum(axis=0)
    s8[:, hid:] = r3[...].sum(axis=0)
    wait_all(groups, r5, rcv[8], True)
    home_dz1 = jnp.concatenate([r5[:, per:, :].sum(axis=0), jnp.zeros((8 - per, hid), F32)], axis=0).astype(BF16)
    back = r5[:, :per, :].reshape(halo, hid)
    dz1 = g1_ref[:own, :] + exact3(pick_t, split3(back))
    dz1 = jnp.where(plain, dz1, 0.0).astype(BF16)
    gw1 = dot(xt, dz1) + dot(home_x, home_dz1, 0, 0)
    s6[...] = rows_to_blocks(gw1, groups)
    s7[...] = dot(home_dz1, w1, 1, 1)[:per]
    send_all(groups, me, [("a", s6, r6, snd[9], rcv[9]), ("b", s7, r7, snd[10], rcv[10])])

    dxt = dot(w1, dz1, 1, 1)
    wait_all(groups, r6, rcv[9], True)
    s8[:, :hid] = r6[...].sum(axis=0)
    send_all(groups, me, [("b", s8, gw_ref, snd[11], rcv[11])])

    wait_all(groups, r7, rcv[10], True)
    hub_dx = r7[...].reshape(hubs, LANES).T
    dxt_ref[...] = dxt + exact3_right(split3(hub_dx), sel)
    for buf, sem in zip((rx, rd, gx, gd, r1, r2, r3, r4, r5, r6, r7, gw_ref), snd):
        wait_all(groups, buf, sem, False)
    wait_all(groups, gw_ref, rcv[11], True)


def main_call(groups, own, halo, hubs, *args):
    hid = args[5].shape[1]
    per = hubs // groups
    slots, dsts = own + halo + hubs, own + hubs
    cells = slots * dsts // DST_BLOCK
    vmem = pl.BlockSpec(memory_space=pltpu.VMEM)
    blocks = [
        ("a", (2 * per, LANES), BF16), ("a", (per, LANES), F32), ("b", (per, LANES), BF16), ("b", (per, LANES), F32),
        ("a", (per, LANES + hid), F32), ("b", (per, hid), F32), ("a", (1, hid), F32), ("b", (1, hid + LANES), F32),
        ("a", (2 * per, hid), F32), ("a", (1, hid), F32), ("b", (per, LANES), F32), ("b", (1, 2 * hid), F32)]
    sends = [pltpu.VMEM(((groups,) if k == "a" else ()) + b, t) for k, b, t in blocks]
    recvs = [pltpu.VMEM((groups,) + b, t) for _, b, t in blocks[:-1]]
    shape = jax.ShapeDtypeStruct
    return pl.pallas_call(
        functools.partial(main_kernel, groups, own, halo, hubs),
        out_shape=[shape((LANES, own), F32), shape((groups, 1, 2 * hid), F32), shape((1, hid + LANES), F32)],
        in_specs=[pl.BlockSpec(memory_space=pl.ANY)] + [vmem] * (len(args) - 1),
        out_specs=[vmem] * 3,
        scratch_shapes=sends + recvs + [
            pltpu.VMEM((cells, DST_BLOCK), F32),
            pltpu.VMEM((slots, dsts), BF16),
            pltpu.VMEM((slots, dsts), BF16),
            pltpu.VMEM((slots, dsts), BF16),
            pltpu.VMEM((hubs, dsts), F32),
            pltpu.VMEM((hid, dsts), F32),
            pltpu.VMEM((slots, LANES), F32),
            pltpu.VMEM((slots, hid), F32),
            pltpu.VMEM((3, dsts, hid), BF16),
            pltpu.VMEM((hid, slots), BF16),
        ] + [pltpu.SemaphoreType.DMA] * (1 + 2 * len(blocks)),
        compiler_params=pltpu.CompilerParams(collective_id=0, has_side_effects=True, vmem_limit_bytes=56 * 2 ** 20),
        name="main_exchange",
    )(*args)


def output_kernel(dxt_ref, gw_ref, bias_ref, dx_out, gw1_out, gw2_out, b1_out, b2_out):
    feat_in, feat_out, hid = dx_out.shape[0], gw2_out.shape[0], gw2_out.shape[1]
    dx_out[...] = dxt_ref[:feat_in, :]
    gw = gw_ref[...].reshape(gw_ref.shape[0], 2 * hid)
    gw1_out[...] = gw[:feat_in, :hid]
    gw2_out[...] = gw[:feat_out, hid:]
    b1_out[...] = bias_ref[:, :hid]
    b2_out[...] = bias_ref[:, hid:hid + feat_out]


def solution(mesh):
    groups = mesh.shape["graph"]

    def device_step(x, dst, src, w, send, hub_ids, w_first, b_first, w_second, dy):
        own, feat_in = x.shape
        feat_out = dy.shape[1]
        hid = w_first.shape[1]
        halo, hubs = send.shape[0], hub_ids.shape[0]
        slots, dsts = own + halo + hubs, own + hubs
        bucket = jnp.right_shift(src, SRC_BLOCK.bit_length() - 1) * (dsts // DST_BLOCK)
        bucket = bucket + jnp.right_shift(dst, DST_BLOCK.bit_length() - 1)
        keys = bucket * BUCKET + jnp.bitwise_and(src, SRC_BLOCK - 1) * DST_BLOCK + jnp.bitwise_and(dst, DST_BLOCK - 1)
        keys, weights = lax.sort((keys, w), num_keys=1, is_stable=False)
        cells = adjacency(keys, weights, slots, dsts)
        raw = main_call(
            groups, own, halo, hubs, cells, x.T, dy.T, send[None, :], hub_ids[None, :], b_first[None, :],
            w_first, w_second.T)
        dx, gw1, gw2, gb1, gb2 = pl.pallas_call(
            output_kernel,
            out_shape=[jax.ShapeDtypeStruct(shape, F32) for shape in (
                (feat_in, own), (feat_in, hid), (feat_out, hid), (1, hid), (1, feat_out))],
            name="outputs",
        )(*raw)
        return dx.T, gw1, gw2.T, gb1[0], gb2[0]

    rows, flat = P(("data", "graph"), None), P(("data", "graph"))
    return jax.shard_map(
        device_step,
        mesh=mesh,
        in_specs=(rows, flat, flat, flat, flat, P("data"), P(), P(), P(), rows),
        out_specs=(rows, P("data", None), P("data", None), P("data"), P("data")),
        check_vma=False,
    )
```

```python
import functools

import jax
import jax.numpy as jnp
from jax import lax
from jax.experimental import pallas as pl
from jax.experimental.pallas import tpu as pltpu
from jax.sharding import PartitionSpec as P

BF16 = jnp.bfloat16
F32 = jnp.float32
HI = lax.Precision.HIGHEST
LANES = 128
MESH = pl.DeviceIdType.MESH


def dot(a, b, ca=1, cb=0, precision=None):
    return lax.dot_general(a, b, (((ca,), (cb,)), ((), ())), precision=precision, preferred_element_type=F32)


def split3(a):
    hi = a.astype(BF16)
    rest = a - hi.astype(F32)
    mid = rest.astype(BF16)
    return hi, mid, (rest - mid.astype(F32)).astype(BF16)


def exact3(sel, pieces, ca=1):
    return dot(sel, pieces[2], ca) + dot(sel, pieces[1], ca) + dot(sel, pieces[0], ca)


def exact3_right(pieces, sel):
    return dot(pieces[2], sel) + dot(pieces[1], sel) + dot(pieces[0], sel)


def sum3(pieces):
    return pieces[2].astype(F32) + pieces[1].astype(F32) + pieces[0].astype(F32)


def full6(a, b):
    low = dot(a[0], b[2]) + dot(a[2], b[0]) + dot(a[1], b[1])
    return low + (dot(a[0], b[1]) + dot(a[1], b[0])) + dot(a[0], b[0])


def partner(groups, me, i):
    low = sum(2 << k for k in range(0, groups.bit_length() - 2, 2))
    t = jnp.bitwise_xor(i - 1, 2 * low + 1)
    high = jnp.bitwise_and(jnp.right_shift(t, 1), low)
    return jnp.bitwise_xor(me, jnp.bitwise_xor(t, jnp.bitwise_xor(high, low)))


def wait_all(groups, buf, sem, whole):
    part = buf if whole else buf.at[pl.ds(0, groups - 1)]
    pltpu.make_async_copy(part, part, sem).wait()


def send_all(groups, me, items):
    def send(i, carry):
        peer = partner(groups, me, i)
        for kind, src, dst, send_sem, recv_sem in items:
            pltpu.make_async_remote_copy(
                src_ref=src.at[peer] if kind == "a" else src,
                dst_ref=dst.at[me],
                send_sem=send_sem,
                recv_sem=recv_sem,
                device_id=(0, peer),
                device_id_type=MESH,
            ).start()
        return carry

    lax.fori_loop(1, groups, send, 0)
    for kind, src, dst, _, recv_sem in items:
        pltpu.make_async_copy(src.at[me] if kind == "a" else src, dst.at[me], recv_sem).start()


def greet_all(groups, me):
    barrier = pltpu.get_barrier_semaphore()

    def greet(i, carry):
        pl.semaphore_signal(barrier, inc=1, device_id=(0, partner(groups, me, i)), device_id_type=MESH)
        return carry

    lax.fori_loop(1, groups, greet, 0)
    return barrier


def padded(ref, rows, cols):
    a = ref[...]
    if cols > a.shape[1]:
        a = jnp.concatenate([a, jnp.zeros((a.shape[0], cols - a.shape[1]), a.dtype)], axis=1)
    if rows > a.shape[0]:
        a = jnp.concatenate([a, jnp.zeros((rows - a.shape[0], cols), a.dtype)], axis=0)
    return a


SRC_BLOCK, DST_BLOCK = 128, 256
BUCKET = SRC_BLOCK * DST_BLOCK
CHUNK_ROWS, UNROLL = 2, 8
STEPS_BEFORE, STEPS_MIDDLE = 3, 10


def plan_kernel(buckets, key_ref, plan_ref, bound_ref):
    size = CHUNK_ROWS * LANES

    def count(i, carry):
        bucket = jnp.right_shift(key_ref[pl.ds(pl.multiple_of(i * 8, 8), 8), :], BUCKET.bit_length() - 1)
        return tuple(c + jnp.where(bucket < b + 1, 1, 0) for b, c in enumerate(carry))

    zeros = jnp.zeros((8, LANES), jnp.int32)
    counts = lax.fori_loop(0, key_ref.shape[0] // 8, count, (zeros,) * buckets)
    bound_ref[0] = 0
    for b, c in enumerate(counts):
        bound_ref[b + 1] = jnp.sum(c.astype(F32)).astype(jnp.int32)

    def put(at, bucket, chunk, same):
        plan_ref[0, at] = bucket
        plan_ref[1, at] = chunk
        plan_ref[2, at] = same

    def list_pairs(b, at):
        low, high = bound_ref[b], bound_ref[b + 1]
        start = low // size
        pairs = jnp.where(high > low, (high + size - 1) // size - start, 0)
        plan_ref[3, b] = jnp.where(pairs > 0, at + pairs, 0)

        def pair(i, carry):
            put(at + i, b, start + i, jnp.where(i > 0, 1, 0))
            return carry

        lax.fori_loop(0, pairs, pair, 0)
        return at + pairs

    def rest(i, carry):
        put(i, buckets, 0, 0)
        return carry

    lax.fori_loop(lax.fori_loop(0, buckets, list_pairs, 0), key_ref.shape[0] // CHUNK_ROWS + buckets, rest, 0)


def edge_plan(keys, buckets):
    return pl.pallas_call(
        functools.partial(plan_kernel, buckets),
        out_shape=jax.ShapeDtypeStruct((4, 256), jnp.int32),
        in_specs=[pl.BlockSpec(memory_space=pltpu.VMEM)],
        out_specs=pl.BlockSpec(memory_space=pltpu.SMEM),
        scratch_shapes=[pltpu.SMEM((buckets + 1,), jnp.int32)],
        name="edge_plan",
    )(keys)


def add_pairs(plan_ref, key_ref, w_ref, cum_ref, low, high):
    src_ids = lax.broadcasted_iota(jnp.int32, (SRC_BLOCK, LANES), 0).astype(F32).astype(BF16)
    dst_ids = lax.broadcasted_iota(jnp.int32, (DST_BLOCK, LANES), 0).astype(F32).astype(BF16)
    one, zero = jnp.ones((), BF16), jnp.zeros((), BF16)

    def step(it, carry):
        work = []
        for u in range(UNROLL):
            b, c = plan_ref[0, it * UNROLL + u], plan_ref[1, it * UNROLL + u]
            lhs, rhs = [], []
            for r in range(CHUNK_ROWS):
                rel = key_ref[pl.ds(c * CHUNK_ROWS + r, 1), :] - b * BUCKET
                weight = w_ref[pl.ds(c * CHUNK_ROWS + r, 1), :]
                src = jnp.right_shift(rel, 8)
                src = jnp.where((src >= 0) & (src < SRC_BLOCK), src, 512).astype(F32).astype(BF16)
                dst = jnp.bitwise_and(rel, DST_BLOCK - 1).astype(F32).astype(BF16)
                hit = src_ids == jnp.broadcast_to(src, src_ids.shape)
                lhs.append(jnp.concatenate(
                    [jnp.where(hit, jnp.broadcast_to(p, src_ids.shape), zero) for p in split3(weight)], axis=0))
                rhs.append(jnp.where(dst_ids == jnp.broadcast_to(dst, dst_ids.shape), one, zero))
            work.append((jnp.concatenate(lhs, axis=1), jnp.concatenate(rhs, axis=1)))
        outs = [dot(lhs, rhs, 1, 1) for lhs, rhs in work]
        total = cum_ref[it * UNROLL]
        for u, out in enumerate(outs):
            same = jnp.broadcast_to(plan_ref[2, it * UNROLL + u], (1, DST_BLOCK)) > 0
            out = out[2 * SRC_BLOCK:] + out[SRC_BLOCK:2 * SRC_BLOCK] + out[:SRC_BLOCK]
            total = out + jnp.where(same, total, 0.0)
            cum_ref[it * UNROLL + u + 1] = total
        return carry

    lax.fori_loop(low, high, step, 0)


def rows_to_blocks(a, groups):
    return a.reshape(groups, a.shape[0] // groups, a.shape[1])


def main_kernel(groups, own, halo, hubs, plan_ref, key_ref, w_ref, xt_ref, dyt_ref, send_ref, hub_ref, b1_ref, w1_ref, w2t_ref,
                dxt_ref, gw_ref, bias_ref,
                sx, sd, hx, hd, s1, s2, s3, s4, s5, s6, s7, s8,
                rx, rd, gx, gd, r1, r2, r3, r4, r5, r6, r7,
                cum_ref, hi_ref, mid_ref, low_ref, hubrow_ref, pt_ref, g2_ref, g1_ref, dy_ref, zt_ref, *sems):
    count = len(sems) // 2
    snd, rcv = sems[:count], sems[count:]
    adj = (hi_ref, mid_ref, low_ref)
    per = hubs // groups
    hid = b1_ref.shape[1]
    feat_in = xt_ref.shape[0]
    first_hub = own + halo
    slots, dsts = own + halo + hubs, own + hubs
    tops = dsts // DST_BLOCK
    me = lax.axis_index("graph")
    barrier = greet_all(groups, me)
    steps = (cum_ref.shape[0] - 1) // UNROLL
    before, middle = steps * STEPS_BEFORE // 19, steps * STEPS_MIDDLE // 19
    cum_ref[0] = jnp.zeros((SRC_BLOCK, DST_BLOCK), F32)

    lane = lax.broadcasted_iota(jnp.int32, (1, LANES), 1)
    half = lane < LANES // 2
    own_row = lax.broadcasted_iota(jnp.int32, (own, 1), 0)
    pick_t = (own_row == send_ref[...]).astype(F32).astype(BF16)
    sel_f = (own_row == hub_ref[...] - me * own).astype(F32)
    sel_t = sel_f.astype(BF16)
    plain = jnp.sum(sel_f, axis=1, keepdims=True) == 0
    number = lax.broadcasted_iota(jnp.int32, (1, hubs), 1) + 1
    numbers = jnp.broadcast_to(number.astype(F32), (8, hubs)).astype(BF16)
    code_row = dot(numbers, sel_t, 1, 1)[:1]
    plain_row = code_row == 0
    xt = padded(xt_ref, LANES, own)
    feature = lax.broadcasted_iota(jnp.int32, (LANES, 1), 0)
    xt = jnp.where(feature == feat_in, code_row, xt.astype(F32)).astype(BF16)
    dyt = padded(dyt_ref, LANES, own)
    picked = dot(jnp.concatenate((xt,) + split3(dyt), axis=0), jnp.concatenate([pick_t, sel_t], axis=1))
    hub_dt = picked[3 * LANES:, halo:] + picked[2 * LANES:3 * LANES, halo:] + picked[LANES:2 * LANES, halo:]
    sx[:, :per, :] = rows_to_blocks(picked[:LANES, :halo].T, groups).astype(BF16)
    sx[:, per:, :] = rows_to_blocks(picked[:LANES, halo:].T, groups).astype(BF16)
    sd[...] = rows_to_blocks(hub_dt.T, groups)
    add_pairs(plan_ref, key_ref, w_ref, cum_ref, 0, before)
    pl.semaphore_wait(barrier, groups - 1)
    send_all(groups, me, [("a", sx, rx, snd[0], rcv[0]), ("a", sd, rd, snd[1], rcv[1])])

    w1 = padded(w1_ref, LANES, hid)
    w1_t = w1.astype(F32).T.astype(BF16)
    zt_ref[:, :own] = dot(w1_t, xt).astype(BF16)
    dy = dyt.T
    add_pairs(plan_ref, key_ref, w_ref, cum_ref, before, middle)
    wait_all(groups, rx, rcv[0], True)
    wait_all(groups, rd, rcv[1], True)
    got = rx[...].astype(F32)
    home_x = got[:, per:, :].sum(axis=0)
    hx[...] = home_x.astype(BF16)
    hd[...] = rd[...].sum(axis=0)
    send_all(groups, me, [("b", hx, gx, snd[2], rcv[2]), ("b", hd, gd, snd[3], rcv[3])])

    home_x = jnp.concatenate([home_x, jnp.zeros((8 - per, LANES), F32)], axis=0).astype(BF16)
    halo_x = got[:, :per, :].reshape(halo, LANES)
    halo_code = halo_x[:, feat_in:feat_in + 1]
    halo_x = halo_x.astype(BF16)
    zt_ref[:, own:first_hub] = dot(w1_t, halo_x, 1, 1).astype(BF16)
    column = jnp.broadcast_to(jnp.where(lane == feat_in, 1.0, 0.0), (8, LANES)).astype(BF16)
    halo_row = dot(column, halo_x, 1, 1)[:1].astype(jnp.int32)
    halo_sel = (lax.broadcasted_iota(jnp.int32, (hubs, 1), 0) + 1 == halo_row).astype(F32).astype(BF16)
    add_pairs(plan_ref, key_ref, w_ref, cum_ref, middle, steps)

    def rename(i, carry):
        cell = [cum_ref[plan_ref[3, i * tops + j]] for j in range(tops)]
        mine = jnp.concatenate(cell[:own // DST_BLOCK], axis=1)
        hub = jnp.concatenate(cell[own // DST_BLOCK:], axis=1) + exact3_right(split3(mine), sel_t)
        rows = pl.ds(pl.multiple_of(i * SRC_BLOCK, SRC_BLOCK), SRC_BLOCK)
        new = jnp.concatenate([jnp.where(plain_row, mine, 0.0), hub], axis=1)
        for ref, piece in zip(adj, split3(new)):
            ref[rows, :] = piece
        return carry

    lax.fori_loop(0, slots // SRC_BLOCK, rename, 0)
    sel = sel_f.T.astype(BF16)
    for j in range(tops):
        cols = slice(j * DST_BLOCK, (j + 1) * DST_BLOCK)
        base = first_hub // SRC_BLOCK
        old = jnp.concatenate(
            [sum3([a[(base + k) * SRC_BLOCK:(base + k + 1) * SRC_BLOCK, cols] for a in adj])
             for k in range(hubs // SRC_BLOCK)], axis=0)
        hubrow_ref[:, cols] = old + exact3(sel, [a[:own, cols] for a in adj])
    for a in adj:
        a[:own, :] = jnp.where(plain, a[:own, :].astype(F32), 0.0).astype(BF16)
    for j in range(tops):
        cols = slice(j * DST_BLOCK, (j + 1) * DST_BLOCK)
        new = hubrow_ref[:, cols] + exact3(halo_sel, [a[own:first_hub, cols] for a in adj])
        for a, piece in zip(adj, split3(new)):
            a[first_hub:, cols] = piece
    for a in adj:
        a[own:first_hub, :] = jnp.where(halo_code == 0, a[own:first_hub, :].astype(F32), 0.0).astype(BF16)

    def forward(rows, cols):
        zt = zt_ref[:, rows]
        return dot(zt, low_ref[rows, cols]) + dot(zt, mid_ref[rows, cols]) + dot(zt, hi_ref[rows, cols])

    def pack(d):
        dh, dm, dl = split3(d)
        d_two = (dh.astype(F32) + pltpu.roll(dm.astype(F32), LANES // 2, 1)).astype(BF16)
        return jnp.concatenate([d_two, dl], axis=1), d_two, dh

    def grad_out_sums(rows, cols, packed):
        a = dot(hi_ref[rows, cols], packed[0])
        t = a[:, :LANES] + a[:, LANES:] + dot(mid_ref[rows, cols], packed[1]) + dot(low_ref[rows, cols], packed[2])
        return jnp.where(half, t + pltpu.roll(t, LANES // 2, 1), 0.0)

    own_cols, hub_cols = slice(0, own), slice(own, dsts)
    pt_ref[...] = forward(slice(0, first_hub), slice(0, dsts))
    d_own = pack(dy)
    g2_ref[...] = grad_out_sums(slice(0, slots), own_cols, d_own)
    wait_all(groups, gx, rcv[2], True)
    wait_all(groups, gd, rcv[3], True)
    hub_x = gx[...].astype(F32).reshape(hubs, LANES).astype(BF16)
    zt_ref[:, first_hub:] = dot(w1_t, hub_x, 1, 1).astype(BF16)
    d_hub = pack(gd[...].reshape(hubs, LANES))
    hub_slots = slice(first_hub, slots)
    y_hub = (pt_ref[:, own:] + forward(hub_slots, hub_cols)).T
    s1[:, :, LANES:] = rows_to_blocks(y_hub, groups)
    g2_halo = g2_ref[own:first_hub, :] + grad_out_sums(slice(own, first_hub), hub_cols, d_hub)
    g2_hub = g2_ref[first_hub:, :] + grad_out_sums(hub_slots, hub_cols, d_hub)
    s1[:, :, :LANES] = rows_to_blocks(g2_halo + pltpu.roll(g2_hub, LANES // 2, 1), groups)
    send_all(groups, me, [("a", s1, r1, snd[4], rcv[4])])

    b1 = b1_ref[...]
    w2t = padded(w2t_ref, LANES, hid)
    pre = (pt_ref[:, :own] + forward(hub_slots, own_cols)).T + b1
    g2_own = g2_ref[:own, :] + grad_out_sums(slice(0, own), hub_cols, d_hub)
    hidden = jnp.where(plain, jax.nn.relu(pre), 0.0).astype(BF16)
    live = plain & (pre > 0)
    wait_all(groups, r1, rcv[4], True)
    home = r1[...].sum(axis=0)
    pad = jnp.zeros((8 - per, LANES), F32)
    home_g = jnp.where(half, pltpu.roll(jnp.concatenate([home[:, :LANES], pad], axis=0), LANES // 2, 1), 0.0)
    home_pre = jnp.concatenate([home[:, LANES:] + b1, jnp.zeros((8 - per, hid), F32)], axis=0)
    home_dz2 = home_g.astype(BF16)
    home_dy = jnp.where(home_pre > 0, dot(home_dz2, w2t), 0.0)
    s2[...] = home_dy[:per]
    send_all(groups, me, [("b", s2, r2, snd[5], rcv[5])])

    back = jnp.where(half, r1[:, :, :LANES].reshape(halo, LANES), 0.0)
    dz2 = (g2_own + exact3(pick_t, split3(back))).astype(BF16)
    dy1 = jnp.where(live, dot(dz2, w2t), 0.0)
    home_hidden = jax.nn.relu(home_pre).astype(BF16)
    gw2 = dot(dz2, hidden, 0, 0) + dot(home_dz2, home_hidden, 0, 0)
    s3[...] = rows_to_blocks(gw2, groups)
    s4[:, :hid] = dy1.sum(axis=0, keepdims=True) + home_dy.sum(axis=0, keepdims=True)
    s4[:, hid:] = dy.sum(axis=0, keepdims=True)
    send_all(groups, me, [("a", s3, r3, snd[6], rcv[6]), ("b", s4, r4, snd[7], rcv[7])])
    for p, piece in enumerate(split3(dy1)):
        dy_ref[p, :own, :] = piece
    chunk = 256

    def own_part(i, carry):
        rows = pl.ds(pl.multiple_of(i * chunk, chunk), chunk)
        g1_ref[rows, :] = full6([a[rows, :own] for a in adj], [dy_ref[p, :own, :] for p in range(3)])
        return carry

    lax.fori_loop(0, slots // chunk, own_part, 0)
    wait_all(groups, r2, rcv[5], True)
    for p, piece in enumerate(split3(r2[...].reshape(hubs, hid))):
        dy_ref[p, own:, :] = piece

    def hub_part(rows):
        return g1_ref[rows, :] + full6([a[rows, own:] for a in adj], [dy_ref[p, own:, :] for p in range(3)])

    s5[:, :per, :] = rows_to_blocks(hub_part(slice(own, first_hub)), groups)
    s5[:, per:, :] = rows_to_blocks(hub_part(hub_slots), groups)
    send_all(groups, me, [("a", s5, r5, snd[8], rcv[8])])

    g1_ref[:chunk, :] = hub_part(slice(0, chunk))
    g1_ref[chunk:own, :] = hub_part(slice(chunk, own))
    wait_all(groups, r3, rcv[6], True)
    wait_all(groups, r4, rcv[7], True)
    bias_ref[...] = r4[...].sum(axis=0)
    s8[:, hid:] = r3[...].sum(axis=0)
    wait_all(groups, r5, rcv[8], True)
    home_dz1 = jnp.concatenate([r5[:, per:, :].sum(axis=0), jnp.zeros((8 - per, hid), F32)], axis=0).astype(BF16)
    back = r5[:, :per, :].reshape(halo, hid)
    dz1 = g1_ref[:own, :] + exact3(pick_t, split3(back))
    dz1 = jnp.where(plain, dz1, 0.0).astype(BF16)
    gw1 = dot(xt, dz1) + dot(home_x, home_dz1, 0, 0)
    s6[...] = rows_to_blocks(gw1, groups)
    s7[...] = dot(home_dz1, w1, 1, 1)[:per]
    send_all(groups, me, [("a", s6, r6, snd[9], rcv[9]), ("b", s7, r7, snd[10], rcv[10])])

    dxt = dot(w1, dz1, 1, 1)
    wait_all(groups, r6, rcv[9], True)
    s8[:, :hid] = r6[...].sum(axis=0)
    send_all(groups, me, [("b", s8, gw_ref, snd[11], rcv[11])])

    wait_all(groups, r7, rcv[10], True)
    hub_dx = r7[...].reshape(hubs, LANES).T
    dxt_ref[...] = dxt + exact3_right(split3(hub_dx), sel)
    for buf, sem in zip((rx, rd, gx, gd, r1, r2, r3, r4, r5, r6, r7, gw_ref), snd):
        wait_all(groups, buf, sem, False)
    wait_all(groups, gw_ref, rcv[11], True)


def main_call(groups, own, halo, hubs, *args):
    hid = args[7].shape[1]
    per = hubs // groups
    slots, dsts = own + halo + hubs, own + hubs
    pairs = args[1].shape[0] // CHUNK_ROWS + slots // SRC_BLOCK * (dsts // DST_BLOCK)
    vmem = pl.BlockSpec(memory_space=pltpu.VMEM)
    blocks = [
        ("a", (2 * per, LANES), BF16), ("a", (per, LANES), F32), ("b", (per, LANES), BF16), ("b", (per, LANES), F32),
        ("a", (per, LANES + hid), F32), ("b", (per, hid), F32), ("a", (1, hid), F32), ("b", (1, hid + LANES), F32),
        ("a", (2 * per, hid), F32), ("a", (1, hid), F32), ("b", (per, LANES), F32), ("b", (1, 2 * hid), F32)]
    sends = [pltpu.VMEM(((groups,) if k == "a" else ()) + b, t) for k, b, t in blocks]
    recvs = [pltpu.VMEM((groups,) + b, t) for _, b, t in blocks[:-1]]
    shape = jax.ShapeDtypeStruct
    return pl.pallas_call(
        functools.partial(main_kernel, groups, own, halo, hubs),
        out_shape=[shape((LANES, own), F32), shape((groups, 1, 2 * hid), F32), shape((1, hid + LANES), F32)],
        in_specs=[pl.BlockSpec(memory_space=pltpu.SMEM)] + [vmem] * (len(args) - 1),
        out_specs=[vmem] * 3,
        scratch_shapes=sends + recvs + [
            pltpu.VMEM((pairs + 1, SRC_BLOCK, DST_BLOCK), F32),
            pltpu.VMEM((slots, dsts), BF16),
            pltpu.VMEM((slots, dsts), BF16),
            pltpu.VMEM((slots, dsts), BF16),
            pltpu.VMEM((hubs, dsts), F32),
            pltpu.VMEM((hid, dsts), F32),
            pltpu.VMEM((slots, LANES), F32),
            pltpu.VMEM((slots, hid), F32),
            pltpu.VMEM((3, dsts, hid), BF16),
            pltpu.VMEM((hid, slots), BF16),
        ] + [pltpu.SemaphoreType.DMA] * (2 * len(blocks)),
        compiler_params=pltpu.CompilerParams(collective_id=0, has_side_effects=True, vmem_limit_bytes=56 * 2 ** 20),
        name="main_exchange",
    )(*args)


def output_kernel(dxt_ref, gw_ref, bias_ref, dx_out, gw1_out, gw2_out, b1_out, b2_out):
    feat_in, feat_out, hid = dx_out.shape[0], gw2_out.shape[0], gw2_out.shape[1]
    dx_out[...] = dxt_ref[:feat_in, :]
    gw = gw_ref[...].reshape(gw_ref.shape[0], 2 * hid)
    gw1_out[...] = gw[:feat_in, :hid]
    gw2_out[...] = gw[:feat_out, hid:]
    b1_out[...] = bias_ref[:, :hid]
    b2_out[...] = bias_ref[:, hid:hid + feat_out]


def solution(mesh):
    groups = mesh.shape["graph"]

    def device_step(x, dst, src, w, send, hub_ids, w_first, b_first, w_second, dy):
        own, feat_in = x.shape
        feat_out = dy.shape[1]
        hid = w_first.shape[1]
        halo, hubs = send.shape[0], hub_ids.shape[0]
        slots, dsts = own + halo + hubs, own + hubs
        bucket = jnp.right_shift(src, SRC_BLOCK.bit_length() - 1) * (dsts // DST_BLOCK)
        bucket = bucket + jnp.right_shift(dst, DST_BLOCK.bit_length() - 1)
        keys = bucket * BUCKET + jnp.bitwise_and(src, SRC_BLOCK - 1) * DST_BLOCK + jnp.bitwise_and(dst, DST_BLOCK - 1)
        keys, weights = lax.sort((keys, w), num_keys=1, is_stable=False)
        keys, weights = keys.reshape(-1, LANES), weights.reshape(-1, LANES)
        plan = edge_plan(keys, slots // SRC_BLOCK * (dsts // DST_BLOCK))
        raw = main_call(
            groups, own, halo, hubs, plan, keys, weights, x.T, dy.T, send[None, :], hub_ids[None, :], b_first[None, :],
            w_first, w_second.T)
        dx, gw1, gw2, gb1, gb2 = pl.pallas_call(
            output_kernel,
            out_shape=[jax.ShapeDtypeStruct(shape, F32) for shape in (
                (feat_in, own), (feat_in, hid), (feat_out, hid), (1, hid), (1, feat_out))],
            name="outputs",
        )(*raw)
        return dx.T, gw1, gw2.T, gb1[0], gb2[0]

    rows, flat = P(("data", "graph"), None), P(("data", "graph"))
    return jax.shard_map(
        device_step,
        mesh=mesh,
        in_specs=(rows, flat, flat, flat, flat, P("data"), P(), P(), P(), rows),
        out_specs=(rows, P("data", None), P("data", None), P("data"), P("data")),
        check_vma=False,
    )
```

```python
import functools

import jax
import jax.numpy as jnp
from jax import lax
from jax.experimental import pallas as pl
from jax.experimental.pallas import tpu as pltpu
from jax.sharding import PartitionSpec as P

BF16 = jnp.bfloat16
F32 = jnp.float32
HI = lax.Precision.HIGHEST
LANES = 128
MESH = pl.DeviceIdType.MESH


def dot(a, b, ca=1, cb=0, precision=None):
    return lax.dot_general(a, b, (((ca,), (cb,)), ((), ())), precision=precision, preferred_element_type=F32)


def split3(a):
    hi = a.astype(BF16)
    rest = a - hi.astype(F32)
    mid = rest.astype(BF16)
    return hi, mid, (rest - mid.astype(F32)).astype(BF16)


def exact3(sel, pieces, ca=1):
    return dot(sel, pieces[2], ca) + dot(sel, pieces[1], ca) + dot(sel, pieces[0], ca)


def exact3_right(pieces, sel):
    return dot(pieces[2], sel) + dot(pieces[1], sel) + dot(pieces[0], sel)


def full6(a, b):
    low = dot(a[0], b[2]) + dot(a[2], b[0]) + dot(a[1], b[1])
    return low + (dot(a[0], b[1]) + dot(a[1], b[0])) + dot(a[0], b[0])


def partner(groups, me, i):
    low = sum(2 << k for k in range(0, groups.bit_length() - 2, 2))
    t = jnp.bitwise_xor(i - 1, 2 * low + 1)
    high = jnp.bitwise_and(jnp.right_shift(t, 1), low)
    return jnp.bitwise_xor(me, jnp.bitwise_xor(t, jnp.bitwise_xor(high, low)))


def wait_all(groups, buf, sem, whole):
    part = buf if whole else buf.at[pl.ds(0, groups - 1)]
    pltpu.make_async_copy(part, part, sem).wait()


def send_all(groups, me, items):
    def send(i, carry):
        peer = partner(groups, me, i)
        for kind, src, dst, send_sem, recv_sem in items:
            pltpu.make_async_remote_copy(
                src_ref=src.at[peer] if kind == "a" else src,
                dst_ref=dst.at[me],
                send_sem=send_sem,
                recv_sem=recv_sem,
                device_id=(0, peer),
                device_id_type=MESH,
            ).start()
        return carry

    lax.fori_loop(1, groups, send, 0)
    for kind, src, dst, _, recv_sem in items:
        pltpu.make_async_copy(src.at[me] if kind == "a" else src, dst.at[me], recv_sem).start()


def greet_all(groups, me):
    barrier = pltpu.get_barrier_semaphore()

    def greet(i, carry):
        pl.semaphore_signal(barrier, inc=1, device_id=(0, partner(groups, me, i)), device_id_type=MESH)
        return carry

    lax.fori_loop(1, groups, greet, 0)
    return barrier


def padded(ref, rows, cols):
    a = ref[...]
    if cols > a.shape[1]:
        a = jnp.concatenate([a, jnp.zeros((a.shape[0], cols - a.shape[1]), a.dtype)], axis=1)
    if rows > a.shape[0]:
        a = jnp.concatenate([a, jnp.zeros((rows - a.shape[0], cols), a.dtype)], axis=0)
    return a


SRC_BLOCK, DST_BLOCK = 128, 256
BUCKET = SRC_BLOCK * DST_BLOCK
CHUNK_ROWS, UNROLL = 2, 19


def plan_kernel(buckets, key_ref, plan_ref, bound_ref):
    size = CHUNK_ROWS * LANES

    def count(i, carry):
        bucket = jnp.right_shift(key_ref[pl.ds(pl.multiple_of(i * 8, 8), 8), :], BUCKET.bit_length() - 1)
        return tuple(c + jnp.where(bucket < b + 1, 1, 0) for b, c in enumerate(carry))

    zeros = jnp.zeros((8, LANES), jnp.int32)
    counts = lax.fori_loop(0, key_ref.shape[0] // 8, count, (zeros,) * buckets)
    bound_ref[0] = 0
    for b, c in enumerate(counts):
        bound_ref[b + 1] = jnp.sum(c.astype(F32)).astype(jnp.int32)

    def put(at, bucket, chunk, same):
        plan_ref[0, at] = bucket
        plan_ref[1, at] = chunk
        plan_ref[2, at] = same

    def list_pairs(b, at):
        low, high = bound_ref[b], bound_ref[b + 1]
        start = low // size
        pairs = jnp.where(high > low, (high + size - 1) // size - start, 0)
        plan_ref[3, b] = jnp.where(pairs > 0, at + pairs, 0)

        def pair(i, carry):
            put(at + i, b, start + i, jnp.where(i > 0, 1, 0))
            return carry

        lax.fori_loop(0, pairs, pair, 0)
        return at + pairs

    def rest(i, carry):
        put(i, buckets, 0, 0)
        return carry

    lax.fori_loop(lax.fori_loop(0, buckets, list_pairs, 0), key_ref.shape[0] // CHUNK_ROWS + buckets, rest, 0)


def edge_plan(keys, buckets):
    return pl.pallas_call(
        functools.partial(plan_kernel, buckets),
        out_shape=jax.ShapeDtypeStruct((4, 256), jnp.int32),
        in_specs=[pl.BlockSpec(memory_space=pltpu.VMEM)],
        out_specs=pl.BlockSpec(memory_space=pltpu.SMEM),
        scratch_shapes=[pltpu.SMEM((buckets + 1,), jnp.int32)],
        name="edge_plan",
    )(keys)


def add_pairs(plan_ref, key_ref, w_ref, cum_ref, low, high):
    src_ids = lax.broadcasted_iota(jnp.int32, (SRC_BLOCK, LANES), 0).astype(F32).astype(BF16)
    dst_ids = lax.broadcasted_iota(jnp.int32, (DST_BLOCK, LANES), 0).astype(F32).astype(BF16)
    one, zero = jnp.ones((), BF16), jnp.zeros((), BF16)

    def step(it, carry):
        work = []
        for u in range(UNROLL):
            b, c = plan_ref[0, it * UNROLL + u], plan_ref[1, it * UNROLL + u]
            lhs, rhs = [], []
            for r in range(CHUNK_ROWS):
                rel = key_ref[pl.ds(c * CHUNK_ROWS + r, 1), :] - b * BUCKET
                weight = w_ref[pl.ds(c * CHUNK_ROWS + r, 1), :]
                src = jnp.right_shift(rel, 8)
                src = jnp.where((src >= 0) & (src < SRC_BLOCK), src, 512).astype(F32).astype(BF16)
                dst = jnp.bitwise_and(rel, DST_BLOCK - 1).astype(F32).astype(BF16)
                hit = src_ids == jnp.broadcast_to(src, src_ids.shape)
                lhs.append(jnp.concatenate(
                    [jnp.where(hit, jnp.broadcast_to(p, src_ids.shape), zero) for p in split3(weight)], axis=0))
                rhs.append(jnp.where(dst_ids == jnp.broadcast_to(dst, dst_ids.shape), one, zero))
            work.append((jnp.concatenate(lhs, axis=1), jnp.concatenate(rhs, axis=1)))
        outs = [dot(lhs, rhs, 1, 1) for lhs, rhs in work]
        total = cum_ref[it * UNROLL]
        for u, out in enumerate(outs):
            same = jnp.broadcast_to(plan_ref[2, it * UNROLL + u], (1, DST_BLOCK)) > 0
            out = out[2 * SRC_BLOCK:] + out[SRC_BLOCK:2 * SRC_BLOCK] + out[:SRC_BLOCK]
            total = out + jnp.where(same, total, 0.0)
            cum_ref[it * UNROLL + u + 1] = total
        return carry

    lax.fori_loop(low, high, step, 0)


def rows_to_blocks(a, groups):
    return a.reshape(groups, a.shape[0] // groups, a.shape[1])


def main_kernel(groups, own, halo, hubs, plan_ref, key_ref, w_ref, xt_ref, dyt_ref, send_ref, hub_ref, b1_ref, w1_ref, w2t_ref,
                dxt_ref, gw_ref, bias_ref,
                sx, sd, hx, hd, s1, s2, s3, s4, s5, s6, s7, s8,
                rx, rd, gx, gd, r1, r2, r3, r4, r5, r6, r7,
                cum_ref, hi_ref, mid_ref, low_ref, hubrow_ref, pt_ref, g2_ref, g1_ref, dy_ref, zt_ref, *sems):
    count = len(sems) // 2
    snd, rcv = sems[:count], sems[count:]
    adj = (hi_ref, mid_ref, low_ref)
    per = hubs // groups
    hid = b1_ref.shape[1]
    feat_in = xt_ref.shape[0]
    first_hub = own + halo
    slots, dsts = own + halo + hubs, own + hubs
    tops = dsts // DST_BLOCK
    me = lax.axis_index("graph")
    barrier = greet_all(groups, me)
    steps = (cum_ref.shape[0] - 1) // UNROLL
    before, middle = steps // 4, steps * 7 // 8
    cum_ref[0] = jnp.zeros((SRC_BLOCK, DST_BLOCK), F32)

    lane = lax.broadcasted_iota(jnp.int32, (1, LANES), 1)
    half = lane < LANES // 2
    own_row = lax.broadcasted_iota(jnp.int32, (own, 1), 0)
    pick_t = (own_row == send_ref[...]).astype(F32).astype(BF16)
    sel_f = (own_row == hub_ref[...] - me * own).astype(F32)
    sel_t = sel_f.astype(BF16)
    plain = jnp.sum(sel_f, axis=1, keepdims=True) == 0
    number = lax.broadcasted_iota(jnp.int32, (1, hubs), 1) + 1
    numbers = jnp.broadcast_to(number.astype(F32), (8, hubs)).astype(BF16)
    code_row = dot(numbers, sel_t, 1, 1)[:1]
    plain_row = code_row == 0
    xt = padded(xt_ref, LANES, own)
    feature = lax.broadcasted_iota(jnp.int32, (LANES, 1), 0)
    xt = jnp.where(feature == feat_in, code_row, xt.astype(F32)).astype(BF16)
    dyt = padded(dyt_ref, LANES, own)
    picked = dot(jnp.concatenate((xt,) + split3(dyt), axis=0), jnp.concatenate([pick_t, sel_t], axis=1))
    hub_dt = picked[3 * LANES:, halo:] + picked[2 * LANES:3 * LANES, halo:] + picked[LANES:2 * LANES, halo:]
    sx[:, :per, :] = rows_to_blocks(picked[:LANES, :halo].T, groups).astype(BF16)
    sx[:, per:, :] = rows_to_blocks(picked[:LANES, halo:].T, groups).astype(BF16)
    sd[...] = rows_to_blocks(hub_dt.T, groups)
    add_pairs(plan_ref, key_ref, w_ref, cum_ref, 0, before)
    pl.semaphore_wait(barrier, groups - 1)
    send_all(groups, me, [("a", sx, rx, snd[0], rcv[0]), ("a", sd, rd, snd[1], rcv[1])])

    w1 = padded(w1_ref, LANES, hid)
    w1_t = w1.astype(F32).T.astype(BF16)
    zt_ref[:, :own] = jnp.where(plain_row, dot(w1_t, xt), 0.0).astype(BF16)
    dy = dyt.T
    add_pairs(plan_ref, key_ref, w_ref, cum_ref, before, middle)
    wait_all(groups, rx, rcv[0], True)
    wait_all(groups, rd, rcv[1], True)
    got = rx[...].astype(F32)
    home_x = got[:, per:, :].sum(axis=0)
    hx[...] = home_x.astype(BF16)
    hd[...] = rd[...].sum(axis=0)
    send_all(groups, me, [("b", hx, gx, snd[2], rcv[2]), ("b", hd, gd, snd[3], rcv[3])])

    home_x = jnp.concatenate([home_x, jnp.zeros((8 - per, LANES), F32)], axis=0).astype(BF16)
    add_pairs(plan_ref, key_ref, w_ref, cum_ref, middle, steps)

    def renamed(i):
        cell = [cum_ref[plan_ref[3, i * tops + j]] for j in range(tops)]
        mine = jnp.concatenate(cell[:own // DST_BLOCK], axis=1)
        pieces = split3(mine)
        return mine, pieces, jnp.concatenate(cell[own // DST_BLOCK:], axis=1) + exact3_right(pieces, sel_t)

    def rename(i, carry):
        _, pieces, hub = renamed(i)
        rows = pl.ds(pl.multiple_of(i * SRC_BLOCK, SRC_BLOCK), SRC_BLOCK)
        for ref, left, right in zip(adj, pieces, split3(hub)):
            ref[rows, :own] = left
            ref[rows, own:] = right
        return carry

    def rename_hub(i, carry):
        mine, _, hub = renamed(first_hub // SRC_BLOCK + i)
        rows = pl.ds(pl.multiple_of(i * SRC_BLOCK, SRC_BLOCK), SRC_BLOCK)
        hubrow_ref[rows, :own] = mine
        hubrow_ref[rows, own:] = hub
        return carry

    lax.fori_loop(0, first_hub // SRC_BLOCK, rename, 0)
    lax.fori_loop(0, hubs // SRC_BLOCK, rename_hub, 0)
    halo_x = got[:, :per, :].reshape(halo, LANES).astype(BF16)
    column = jnp.broadcast_to(jnp.where(lane == feat_in, 1.0, 0.0), (8, LANES)).astype(BF16)
    halo_row = dot(column, halo_x, 1, 1)[:1].astype(jnp.int32)
    zt_ref[:, own:first_hub] = jnp.where(halo_row == 0, dot(w1_t, halo_x, 1, 1), 0.0).astype(BF16)
    halo_sel = (lax.broadcasted_iota(jnp.int32, (hubs, 1), 0) + 1 == halo_row).astype(F32)
    moved = jnp.concatenate([sel_f.T, halo_sel], axis=1).astype(BF16)
    for j in range(tops):
        cols = slice(j * DST_BLOCK, (j + 1) * DST_BLOCK)
        new = hubrow_ref[:, cols] + exact3(moved, [a[:first_hub, cols] for a in adj])
        for a, piece in zip(adj, split3(new)):
            a[first_hub:, cols] = piece

    def forward(rows, cols):
        zt = zt_ref[:, rows]
        return dot(zt, low_ref[rows, cols]) + dot(zt, mid_ref[rows, cols]) + dot(zt, hi_ref[rows, cols])

    def pack(d):
        dh, dm, dl = split3(d)
        d_two = (dh.astype(F32) + pltpu.roll(dm.astype(F32), LANES // 2, 1)).astype(BF16)
        return jnp.concatenate([d_two, dl], axis=1), d_two, dh

    def grad_out_sums(rows, cols, packed):
        a = dot(hi_ref[rows, cols], packed[0])
        t = a[:, :LANES] + a[:, LANES:] + dot(mid_ref[rows, cols], packed[1]) + dot(low_ref[rows, cols], packed[2])
        return jnp.where(half, t + pltpu.roll(t, LANES // 2, 1), 0.0)

    own_cols, hub_cols = slice(0, own), slice(own, dsts)
    pt_ref[...] = forward(slice(0, first_hub), hub_cols)
    d_own = pack(jnp.where(plain, dy, 0.0))
    g2_ref[...] = grad_out_sums(slice(own, slots), own_cols, d_own)
    wait_all(groups, gx, rcv[2], True)
    wait_all(groups, gd, rcv[3], True)
    hub_x = gx[...].astype(F32).reshape(hubs, LANES).astype(BF16)
    zt_ref[:, first_hub:] = dot(w1_t, hub_x, 1, 1).astype(BF16)
    d_hub = pack(gd[...].reshape(hubs, LANES))
    hub_slots = slice(first_hub, slots)
    y_hub = (pt_ref[...] + forward(hub_slots, hub_cols)).T
    s1[:, :, LANES:] = rows_to_blocks(y_hub, groups)
    g2_halo = g2_ref[:halo, :] + grad_out_sums(slice(own, first_hub), hub_cols, d_hub)
    g2_hub = g2_ref[halo:, :] + grad_out_sums(hub_slots, hub_cols, d_hub)
    s1[:, :, :LANES] = rows_to_blocks(g2_halo + pltpu.roll(g2_hub, LANES // 2, 1), groups)
    send_all(groups, me, [("a", s1, r1, snd[4], rcv[4])])

    b1 = b1_ref[...]
    w2t = padded(w2t_ref, LANES, hid)
    pre = forward(slice(0, slots), own_cols).T + b1
    g2_own = grad_out_sums(slice(0, own), own_cols, d_own) + grad_out_sums(slice(0, own), hub_cols, d_hub)
    hidden = jnp.where(plain, jax.nn.relu(pre), 0.0).astype(BF16)
    live = plain & (pre > 0)
    wait_all(groups, r1, rcv[4], True)
    home = r1[...].sum(axis=0)
    pad = jnp.zeros((8 - per, LANES), F32)
    home_g = jnp.where(half, pltpu.roll(jnp.concatenate([home[:, :LANES], pad], axis=0), LANES // 2, 1), 0.0)
    home_pre = jnp.concatenate([home[:, LANES:] + b1, jnp.zeros((8 - per, hid), F32)], axis=0)
    home_dz2 = home_g.astype(BF16)
    home_dy = jnp.where(home_pre > 0, dot(home_dz2, w2t), 0.0)
    s2[...] = home_dy[:per]
    send_all(groups, me, [("b", s2, r2, snd[5], rcv[5])])

    back = jnp.where(half, r1[:, :, :LANES].reshape(halo, LANES), 0.0)
    dz2 = jnp.where(plain, g2_own + exact3(pick_t, split3(back)), 0.0).astype(BF16)
    dy1 = jnp.where(live, dot(dz2, w2t), 0.0)
    home_hidden = jax.nn.relu(home_pre).astype(BF16)
    gw2 = dot(dz2, hidden, 0, 0) + dot(home_dz2, home_hidden, 0, 0)
    s3[...] = rows_to_blocks(gw2, groups)
    s4[:, :hid] = dy1.sum(axis=0, keepdims=True) + home_dy.sum(axis=0, keepdims=True)
    s4[:, hid:] = dy.sum(axis=0, keepdims=True)
    send_all(groups, me, [("a", s3, r3, snd[6], rcv[6]), ("b", s4, r4, snd[7], rcv[7])])
    for p, piece in enumerate(split3(dy1)):
        dy_ref[p, :own, :] = piece
    chunk = 256

    def own_part(i, carry):
        rows = pl.ds(pl.multiple_of(i * chunk, chunk), chunk)
        g1_ref[rows, :] = full6([a[rows, :own] for a in adj], [dy_ref[p, :own, :] for p in range(3)])
        return carry

    lax.fori_loop(0, slots // chunk, own_part, 0)
    wait_all(groups, r2, rcv[5], True)
    for p, piece in enumerate(split3(r2[...].reshape(hubs, hid))):
        dy_ref[p, own:, :] = piece

    def hub_part(rows):
        return g1_ref[rows, :] + full6([a[rows, own:] for a in adj], [dy_ref[p, own:, :] for p in range(3)])

    s5[:, :per, :] = rows_to_blocks(hub_part(slice(own, first_hub)), groups)
    s5[:, per:, :] = rows_to_blocks(hub_part(hub_slots), groups)
    send_all(groups, me, [("a", s5, r5, snd[8], rcv[8])])

    g1_ref[:chunk, :] = hub_part(slice(0, chunk))
    g1_ref[chunk:own, :] = hub_part(slice(chunk, own))
    wait_all(groups, r3, rcv[6], True)
    wait_all(groups, r4, rcv[7], True)
    bias_ref[...] = r4[...].sum(axis=0)
    s8[:, hid:] = r3[...].sum(axis=0)
    wait_all(groups, r5, rcv[8], True)
    home_dz1 = jnp.concatenate([r5[:, per:, :].sum(axis=0), jnp.zeros((8 - per, hid), F32)], axis=0).astype(BF16)
    back = r5[:, :per, :].reshape(halo, hid)
    dz1 = g1_ref[:own, :] + exact3(pick_t, split3(back))
    dz1 = jnp.where(plain, dz1, 0.0).astype(BF16)
    gw1 = dot(xt, dz1) + dot(home_x, home_dz1, 0, 0)
    s6[...] = rows_to_blocks(gw1, groups)
    s7[...] = dot(home_dz1, w1, 1, 1)[:per]
    send_all(groups, me, [("a", s6, r6, snd[9], rcv[9]), ("b", s7, r7, snd[10], rcv[10])])

    dxt = dot(w1, dz1, 1, 1)
    wait_all(groups, r6, rcv[9], True)
    s8[:, :hid] = r6[...].sum(axis=0)
    send_all(groups, me, [("b", s8, gw_ref, snd[11], rcv[11])])

    wait_all(groups, r7, rcv[10], True)
    hub_dx = r7[...].reshape(hubs, LANES).T
    dxt_ref[...] = dxt + exact3_right(split3(hub_dx), sel_f.T.astype(BF16))
    for buf, sem in zip((rx, rd, gx, gd, r1, r2, r3, r4, r5, r6, r7, gw_ref), snd):
        wait_all(groups, buf, sem, False)
    wait_all(groups, gw_ref, rcv[11], True)


def main_call(groups, own, halo, hubs, *args):
    hid = args[7].shape[1]
    per = hubs // groups
    slots, dsts = own + halo + hubs, own + hubs
    pairs = args[1].shape[0] // CHUNK_ROWS + slots // SRC_BLOCK * (dsts // DST_BLOCK)
    vmem = pl.BlockSpec(memory_space=pltpu.VMEM)
    blocks = [
        ("a", (2 * per, LANES), BF16), ("a", (per, LANES), F32), ("b", (per, LANES), BF16), ("b", (per, LANES), F32),
        ("a", (per, LANES + hid), F32), ("b", (per, hid), F32), ("a", (1, hid), F32), ("b", (1, hid + LANES), F32),
        ("a", (2 * per, hid), F32), ("a", (1, hid), F32), ("b", (per, LANES), F32), ("b", (1, 2 * hid), F32)]
    sends = [pltpu.VMEM(((groups,) if k == "a" else ()) + b, t) for k, b, t in blocks]
    recvs = [pltpu.VMEM((groups,) + b, t) for _, b, t in blocks[:-1]]
    shape = jax.ShapeDtypeStruct
    return pl.pallas_call(
        functools.partial(main_kernel, groups, own, halo, hubs),
        out_shape=[shape((LANES, own), F32), shape((groups, 1, 2 * hid), F32), shape((1, hid + LANES), F32)],
        in_specs=[pl.BlockSpec(memory_space=pltpu.SMEM)] + [vmem] * (len(args) - 1),
        out_specs=[vmem] * 3,
        scratch_shapes=sends + recvs + [
            pltpu.VMEM((pairs + 1, SRC_BLOCK, DST_BLOCK), F32),
            pltpu.VMEM((slots, dsts), BF16),
            pltpu.VMEM((slots, dsts), BF16),
            pltpu.VMEM((slots, dsts), BF16),
            pltpu.VMEM((hubs, dsts), F32),
            pltpu.VMEM((hid, hubs), F32),
            pltpu.VMEM((slots - own, LANES), F32),
            pltpu.VMEM((slots, hid), F32),
            pltpu.VMEM((3, dsts, hid), BF16),
            pltpu.VMEM((hid, slots), BF16),
        ] + [pltpu.SemaphoreType.DMA] * (2 * len(blocks)),
        compiler_params=pltpu.CompilerParams(collective_id=0, has_side_effects=True, vmem_limit_bytes=56 * 2 ** 20),
        name="main_exchange",
    )(*args)


def output_kernel(dxt_ref, gw_ref, bias_ref, dx_out, gw1_out, gw2_out, b1_out, b2_out):
    feat_in, feat_out, hid = dx_out.shape[0], gw2_out.shape[0], gw2_out.shape[1]
    dx_out[...] = dxt_ref[:feat_in, :]
    gw = gw_ref[...].reshape(gw_ref.shape[0], 2 * hid)
    gw1_out[...] = gw[:feat_in, :hid]
    gw2_out[...] = gw[:feat_out, hid:]
    b1_out[...] = bias_ref[:, :hid]
    b2_out[...] = bias_ref[:, hid:hid + feat_out]


def solution(mesh):
    groups = mesh.shape["graph"]

    def device_step(x, dst, src, w, send, hub_ids, w_first, b_first, w_second, dy):
        own, feat_in = x.shape
        feat_out = dy.shape[1]
        hid = w_first.shape[1]
        halo, hubs = send.shape[0], hub_ids.shape[0]
        slots, dsts = own + halo + hubs, own + hubs
        bucket = jnp.right_shift(src, SRC_BLOCK.bit_length() - 1) * (dsts // DST_BLOCK)
        bucket = bucket + jnp.right_shift(dst, DST_BLOCK.bit_length() - 1)
        keys = bucket * BUCKET + jnp.bitwise_and(src, SRC_BLOCK - 1) * DST_BLOCK + jnp.bitwise_and(dst, DST_BLOCK - 1)
        keys, weights = lax.sort((keys, w), num_keys=1, is_stable=False)
        keys, weights = keys.reshape(-1, LANES), weights.reshape(-1, LANES)
        plan = edge_plan(keys, slots // SRC_BLOCK * (dsts // DST_BLOCK))
        raw = main_call(
            groups, own, halo, hubs, plan, keys, weights, x.T, dy.T, send[None, :], hub_ids[None, :], b_first[None, :],
            w_first, w_second.T)
        dx, gw1, gw2, gb1, gb2 = pl.pallas_call(
            output_kernel,
            out_shape=[jax.ShapeDtypeStruct(shape, F32) for shape in (
                (feat_in, own), (feat_in, hid), (feat_out, hid), (1, hid), (1, feat_out))],
            name="outputs",
        )(*raw)
        return dx.T, gw1, gw2.T, gb1[0], gb2[0]

    rows, flat = P(("data", "graph"), None), P(("data", "graph"))
    return jax.shard_map(
        device_step,
        mesh=mesh,
        in_specs=(rows, flat, flat, flat, flat, P("data"), P(), P(), P(), rows),
        out_specs=(rows, P("data", None), P("data", None), P("data"), P("data")),
        check_vma=False,
    )
```

```python
import functools

import jax
import jax.numpy as jnp
from jax import lax
from jax.experimental import pallas as pl
from jax.experimental.pallas import tpu as pltpu
from jax.sharding import PartitionSpec as P

BF16 = jnp.bfloat16
F32 = jnp.float32
HI = lax.Precision.HIGHEST
LANES = 128
MESH = pl.DeviceIdType.MESH


def dot(a, b, ca=1, cb=0, precision=None):
    return lax.dot_general(a, b, (((ca,), (cb,)), ((), ())), precision=precision, preferred_element_type=F32)


def split3(a):
    hi = a.astype(BF16)
    rest = a - hi.astype(F32)
    mid = rest.astype(BF16)
    return hi, mid, (rest - mid.astype(F32)).astype(BF16)


def exact3(sel, pieces, ca=1):
    return dot(sel, pieces[2], ca) + dot(sel, pieces[1], ca) + dot(sel, pieces[0], ca)


def exact3_right(pieces, sel):
    return dot(pieces[2], sel) + dot(pieces[1], sel) + dot(pieces[0], sel)


def full6(a, b):
    low = dot(a[0], b[2]) + dot(a[2], b[0]) + dot(a[1], b[1])
    return low + (dot(a[0], b[1]) + dot(a[1], b[0])) + dot(a[0], b[0])


def partner(groups, me, i):
    low = sum(2 << k for k in range(0, groups.bit_length() - 2, 2))
    t = jnp.bitwise_xor(i - 1, 2 * low + 1)
    high = jnp.bitwise_and(jnp.right_shift(t, 1), low)
    return jnp.bitwise_xor(me, jnp.bitwise_xor(t, jnp.bitwise_xor(high, low)))


def wait_all(groups, buf, sem, whole):
    part = buf if whole else buf.at[pl.ds(0, groups - 1)]
    pltpu.make_async_copy(part, part, sem).wait()


def send_all(groups, me, items):
    def send(i, carry):
        peer = partner(groups, me, i)
        for kind, src, dst, send_sem, recv_sem in items:
            pltpu.make_async_remote_copy(
                src_ref=src.at[peer] if kind == "a" else src,
                dst_ref=dst.at[me],
                send_sem=send_sem,
                recv_sem=recv_sem,
                device_id=(0, peer),
                device_id_type=MESH,
            ).start()
        return carry

    lax.fori_loop(1, groups, send, 0)
    for kind, src, dst, _, recv_sem in items:
        pltpu.make_async_copy(src.at[me] if kind == "a" else src, dst.at[me], recv_sem).start()


def greet_all(groups, me):
    barrier = pltpu.get_barrier_semaphore()

    def greet(i, carry):
        pl.semaphore_signal(barrier, inc=1, device_id=(0, partner(groups, me, i)), device_id_type=MESH)
        return carry

    lax.fori_loop(1, groups, greet, 0)
    return barrier


def padded(ref, rows, cols):
    a = ref[...]
    if cols > a.shape[1]:
        a = jnp.concatenate([a, jnp.zeros((a.shape[0], cols - a.shape[1]), a.dtype)], axis=1)
    if rows > a.shape[0]:
        a = jnp.concatenate([a, jnp.zeros((rows - a.shape[0], cols), a.dtype)], axis=0)
    return a


SRC_BLOCK, DST_BLOCK = 128, 256
BUCKET = SRC_BLOCK * DST_BLOCK
CHUNK_ROWS, UNROLL = 2, 19


def ring_sum(a, axis):
    step = a.shape[axis] // 2
    while step:
        a = a + pltpu.roll(a, step, axis)
        step //= 2
    return a


def list_pairs(buckets, key_ref, plan_ref):
    size = CHUNK_ROWS * LANES
    shift = size.bit_length() - 1
    total = 1 << buckets.bit_length()

    def count(i, carry):
        bucket = jnp.right_shift(key_ref[pl.ds(pl.multiple_of(i * 8, 8), 8), :], BUCKET.bit_length() - 1)
        return tuple(c + jnp.where(bucket <= b, 1, 0) for b, c in enumerate(carry))

    counts = lax.fori_loop(0, key_ref.shape[0] // 8, count, (jnp.zeros((8, LANES), jnp.int32),) * buckets)
    counts = [ring_sum(c, 0)[:1] for c in counts]
    none = jnp.zeros((1, LANES), jnp.int32)
    counts = [none] + counts + [counts[-1]] * (total - buckets)
    low = ring_sum(jnp.concatenate(counts[:total], axis=0), 1)
    high = ring_sum(jnp.concatenate(counts[1:], axis=0), 1)
    start = jnp.right_shift(low, shift)
    pairs = jnp.where(high > low, jnp.right_shift(high + size - 1, shift) - start, 0)
    row = lax.broadcasted_iota(jnp.int32, (total, LANES), 0)
    last, step = pairs, 1
    while step < total:
        last = last + jnp.where(row >= step, pltpu.roll(last, step, 0), 0)
        step *= 2
    first = last - pairs
    for half in range(plan_ref.shape[1] // LANES):
        at = lax.broadcasted_iota(jnp.int32, (total, LANES), 1) + half * LANES
        inside = (first <= at) & (at < last)
        rows = [
            jnp.where(last <= at, 1, 0), jnp.where(inside, start + at - first, 0), jnp.where(inside & (at > first), 1, 0),
            jnp.where((row == at) & (pairs > 0), last, 0)]
        rows = [ring_sum(r, 0)[:1] for r in rows] + [none] * 4
        plan_ref[:, half * LANES:(half + 1) * LANES] = jnp.concatenate(rows, axis=0)


def add_pairs(plan_ref, key_ref, w_ref, cum_ref, low, high):
    src_ids = lax.broadcasted_iota(jnp.int32, (SRC_BLOCK, LANES), 0).astype(F32).astype(BF16)
    dst_ids = lax.broadcasted_iota(jnp.int32, (DST_BLOCK, LANES), 0).astype(F32).astype(BF16)
    one, zero = jnp.ones((), BF16), jnp.zeros((), BF16)

    def step(it, carry):
        work = []
        for u in range(UNROLL):
            b, c = plan_ref[0, it * UNROLL + u], plan_ref[1, it * UNROLL + u]
            lhs, rhs = [], []
            for r in range(CHUNK_ROWS):
                rel = key_ref[pl.ds(c * CHUNK_ROWS + r, 1), :] - b * BUCKET
                weight = w_ref[pl.ds(c * CHUNK_ROWS + r, 1), :]
                src = jnp.right_shift(rel, 8)
                src = jnp.where((src >= 0) & (src < SRC_BLOCK), src, 512).astype(F32).astype(BF16)
                dst = jnp.bitwise_and(rel, DST_BLOCK - 1).astype(F32).astype(BF16)
                hit = src_ids == jnp.broadcast_to(src, src_ids.shape)
                lhs.append(jnp.concatenate(
                    [jnp.where(hit, jnp.broadcast_to(p, src_ids.shape), zero) for p in split3(weight)], axis=0))
                rhs.append(jnp.where(dst_ids == jnp.broadcast_to(dst, dst_ids.shape), one, zero))
            work.append((jnp.concatenate(lhs, axis=1), jnp.concatenate(rhs, axis=1)))
        outs = [dot(lhs, rhs, 1, 1) for lhs, rhs in work]
        total = cum_ref[it * UNROLL]
        for u, out in enumerate(outs):
            same = jnp.broadcast_to(plan_ref[2, it * UNROLL + u], (1, DST_BLOCK)) > 0
            out = out[2 * SRC_BLOCK:] + out[SRC_BLOCK:2 * SRC_BLOCK] + out[:SRC_BLOCK]
            total = out + jnp.where(same, total, 0.0)
            cum_ref[it * UNROLL + u + 1] = total
        return carry

    lax.fori_loop(low, high, step, 0)


def rows_to_blocks(a, groups):
    return a.reshape(groups, a.shape[0] // groups, a.shape[1])


def main_kernel(groups, own, halo, hubs, key_ref, w_ref, xt_ref, dyt_ref, send_ref, hub_ref, b1_ref, w1_ref, w2t_ref,
                dxt_ref, gw_ref, bias_ref,
                sx, sd, hx, hd, s1, s2, s3, s4, s5, s6, s7, s8,
                rx, rd, gx, gd, r1, r2, r3, r4, r5, r6, r7,
                list_ref, plan_ref, cum_ref, hi_ref, mid_ref, low_ref, hubrow_ref, pt_ref, g2_ref, g1_ref, dy_ref, zt_ref, plan_sem, *sems):
    count = len(sems) // 2
    snd, rcv = sems[:count], sems[count:]
    adj = (hi_ref, mid_ref, low_ref)
    per = hubs // groups
    hid = b1_ref.shape[1]
    feat_in = xt_ref.shape[0]
    first_hub = own + halo
    slots, dsts = own + halo + hubs, own + hubs
    tops = dsts // DST_BLOCK
    me = lax.axis_index("graph")
    barrier = greet_all(groups, me)
    steps = (cum_ref.shape[0] - 1) // UNROLL
    before, middle = steps // 4, steps * 7 // 8
    cum_ref[0] = jnp.zeros((SRC_BLOCK, DST_BLOCK), F32)
    list_pairs(slots // SRC_BLOCK * tops, key_ref, list_ref)
    plan = pltpu.make_async_copy(list_ref, plan_ref, plan_sem)
    plan.start()

    lane = lax.broadcasted_iota(jnp.int32, (1, LANES), 1)
    half = lane < LANES // 2
    own_row = lax.broadcasted_iota(jnp.int32, (own, 1), 0)
    pick_t = (own_row == send_ref[...]).astype(F32).astype(BF16)
    sel_f = (own_row == hub_ref[...] - me * own).astype(F32)
    sel_t = sel_f.astype(BF16)
    plain = jnp.sum(sel_f, axis=1, keepdims=True) == 0
    number = lax.broadcasted_iota(jnp.int32, (1, hubs), 1) + 1
    numbers = jnp.broadcast_to(number.astype(F32), (8, hubs)).astype(BF16)
    code_row = dot(numbers, sel_t, 1, 1)[:1]
    plain_row = code_row == 0
    xt = padded(xt_ref, LANES, own)
    feature = lax.broadcasted_iota(jnp.int32, (LANES, 1), 0)
    xt = jnp.where(feature == feat_in, code_row, xt.astype(F32)).astype(BF16)
    dyt = padded(dyt_ref, LANES, own)
    picked = dot(jnp.concatenate((xt,) + split3(dyt), axis=0), jnp.concatenate([pick_t, sel_t], axis=1))
    hub_dt = picked[3 * LANES:, halo:] + picked[2 * LANES:3 * LANES, halo:] + picked[LANES:2 * LANES, halo:]
    sx[:, :per, :] = rows_to_blocks(picked[:LANES, :halo].T, groups).astype(BF16)
    sx[:, per:, :] = rows_to_blocks(picked[:LANES, halo:].T, groups).astype(BF16)
    sd[...] = rows_to_blocks(hub_dt.T, groups)
    plan.wait()
    add_pairs(plan_ref, key_ref, w_ref, cum_ref, 0, before)
    pl.semaphore_wait(barrier, groups - 1)
    send_all(groups, me, [("a", sx, rx, snd[0], rcv[0]), ("a", sd, rd, snd[1], rcv[1])])

    w1 = padded(w1_ref, LANES, hid)
    w1_t = w1.astype(F32).T.astype(BF16)
    zt_ref[:, :own] = jnp.where(plain_row, dot(w1_t, xt), 0.0).astype(BF16)
    dy = dyt.T
    add_pairs(plan_ref, key_ref, w_ref, cum_ref, before, middle)
    wait_all(groups, rx, rcv[0], True)
    wait_all(groups, rd, rcv[1], True)
    got = rx[...].astype(F32)
    home_x = got[:, per:, :].sum(axis=0)
    hx[...] = home_x.astype(BF16)
    hd[...] = rd[...].sum(axis=0)
    send_all(groups, me, [("b", hx, gx, snd[2], rcv[2]), ("b", hd, gd, snd[3], rcv[3])])

    home_x = jnp.concatenate([home_x, jnp.zeros((8 - per, LANES), F32)], axis=0).astype(BF16)
    add_pairs(plan_ref, key_ref, w_ref, cum_ref, middle, steps)

    def renamed(i):
        cell = [cum_ref[plan_ref[3, i * tops + j]] for j in range(tops)]
        mine = jnp.concatenate(cell[:own // DST_BLOCK], axis=1)
        pieces = split3(mine)
        return mine, pieces, jnp.concatenate(cell[own // DST_BLOCK:], axis=1) + exact3_right(pieces, sel_t)

    def rename(i, carry):
        _, pieces, hub = renamed(i)
        rows = pl.ds(pl.multiple_of(i * SRC_BLOCK, SRC_BLOCK), SRC_BLOCK)
        for ref, left, right in zip(adj, pieces, split3(hub)):
            ref[rows, :own] = left
            ref[rows, own:] = right
        return carry

    def rename_hub(i, carry):
        mine, _, hub = renamed(first_hub // SRC_BLOCK + i)
        rows = pl.ds(pl.multiple_of(i * SRC_BLOCK, SRC_BLOCK), SRC_BLOCK)
        hubrow_ref[rows, :own] = mine
        hubrow_ref[rows, own:] = hub
        return carry

    lax.fori_loop(0, first_hub // SRC_BLOCK, rename, 0)
    lax.fori_loop(0, hubs // SRC_BLOCK, rename_hub, 0)
    halo_x = got[:, :per, :].reshape(halo, LANES).astype(BF16)
    column = jnp.broadcast_to(jnp.where(lane == feat_in, 1.0, 0.0), (8, LANES)).astype(BF16)
    halo_row = dot(column, halo_x, 1, 1)[:1].astype(jnp.int32)
    zt_ref[:, own:first_hub] = jnp.where(halo_row == 0, dot(w1_t, halo_x, 1, 1), 0.0).astype(BF16)
    halo_sel = (lax.broadcasted_iota(jnp.int32, (hubs, 1), 0) + 1 == halo_row).astype(F32)
    moved = jnp.concatenate([sel_f.T, halo_sel], axis=1).astype(BF16)
    for j in range(tops):
        cols = slice(j * DST_BLOCK, (j + 1) * DST_BLOCK)
        new = hubrow_ref[:, cols] + exact3(moved, [a[:first_hub, cols] for a in adj])
        for a, piece in zip(adj, split3(new)):
            a[first_hub:, cols] = piece

    def forward(rows, cols):
        zt = zt_ref[:, rows]
        return dot(zt, low_ref[rows, cols]) + dot(zt, mid_ref[rows, cols]) + dot(zt, hi_ref[rows, cols])

    def pack(d):
        dh, dm, dl = split3(d)
        d_two = (dh.astype(F32) + pltpu.roll(dm.astype(F32), LANES // 2, 1)).astype(BF16)
        return jnp.concatenate([d_two, dl], axis=1), d_two, dh

    def grad_out_sums(rows, cols, packed):
        a = dot(hi_ref[rows, cols], packed[0])
        t = a[:, :LANES] + a[:, LANES:] + dot(mid_ref[rows, cols], packed[1]) + dot(low_ref[rows, cols], packed[2])
        return jnp.where(half, t + pltpu.roll(t, LANES // 2, 1), 0.0)

    own_cols, hub_cols = slice(0, own), slice(own, dsts)
    pt_ref[...] = forward(slice(0, first_hub), hub_cols)
    d_own = pack(jnp.where(plain, dy, 0.0))
    g2_ref[...] = grad_out_sums(slice(own, slots), own_cols, d_own)
    wait_all(groups, gx, rcv[2], True)
    wait_all(groups, gd, rcv[3], True)
    hub_x = gx[...].astype(F32).reshape(hubs, LANES).astype(BF16)
    zt_ref[:, first_hub:] = dot(w1_t, hub_x, 1, 1).astype(BF16)
    d_hub = pack(gd[...].reshape(hubs, LANES))
    hub_slots = slice(first_hub, slots)
    y_hub = (pt_ref[...] + forward(hub_slots, hub_cols)).T
    s1[:, :, LANES:] = rows_to_blocks(y_hub, groups)
    g2_halo = g2_ref[:halo, :] + grad_out_sums(slice(own, first_hub), hub_cols, d_hub)
    g2_hub = g2_ref[halo:, :] + grad_out_sums(hub_slots, hub_cols, d_hub)
    s1[:, :, :LANES] = rows_to_blocks(g2_halo + pltpu.roll(g2_hub, LANES // 2, 1), groups)
    send_all(groups, me, [("a", s1, r1, snd[4], rcv[4])])

    b1 = b1_ref[...]
    w2t = padded(w2t_ref, LANES, hid)
    pre = forward(slice(0, slots), own_cols).T + b1
    g2_own = grad_out_sums(slice(0, own), own_cols, d_own) + grad_out_sums(slice(0, own), hub_cols, d_hub)
    hidden = jnp.where(plain, jax.nn.relu(pre), 0.0).astype(BF16)
    live = plain & (pre > 0)
    wait_all(groups, r1, rcv[4], True)
    home = r1[...].sum(axis=0)
    pad = jnp.zeros((8 - per, LANES), F32)
    home_g = jnp.where(half, pltpu.roll(jnp.concatenate([home[:, :LANES], pad], axis=0), LANES // 2, 1), 0.0)
    home_pre = jnp.concatenate([home[:, LANES:] + b1, jnp.zeros((8 - per, hid), F32)], axis=0)
    home_dz2 = home_g.astype(BF16)
    home_dy = jnp.where(home_pre > 0, dot(home_dz2, w2t), 0.0)
    s2[...] = home_dy[:per]
    send_all(groups, me, [("b", s2, r2, snd[5], rcv[5])])

    back = jnp.where(half, r1[:, :, :LANES].reshape(halo, LANES), 0.0)
    dz2 = jnp.where(plain, g2_own + exact3(pick_t, split3(back)), 0.0).astype(BF16)
    dy1 = jnp.where(live, dot(dz2, w2t), 0.0)
    home_hidden = jax.nn.relu(home_pre).astype(BF16)
    gw2 = dot(dz2, hidden, 0, 0) + dot(home_dz2, home_hidden, 0, 0)
    s3[...] = rows_to_blocks(gw2, groups)
    s4[:, :hid] = dy1.sum(axis=0, keepdims=True) + home_dy.sum(axis=0, keepdims=True)
    s4[:, hid:] = dy.sum(axis=0, keepdims=True)
    send_all(groups, me, [("a", s3, r3, snd[6], rcv[6]), ("b", s4, r4, snd[7], rcv[7])])
    for p, piece in enumerate(split3(dy1)):
        dy_ref[p, :own, :] = piece
    chunk = 256

    def own_part(i, carry):
        rows = pl.ds(pl.multiple_of(i * chunk, chunk), chunk)
        g1_ref[rows, :] = full6([a[rows, :own] for a in adj], [dy_ref[p, :own, :] for p in range(3)])
        return carry

    lax.fori_loop(0, slots // chunk, own_part, 0)
    wait_all(groups, r2, rcv[5], True)
    for p, piece in enumerate(split3(r2[...].reshape(hubs, hid))):
        dy_ref[p, own:, :] = piece

    def hub_part(rows):
        return g1_ref[rows, :] + full6([a[rows, own:] for a in adj], [dy_ref[p, own:, :] for p in range(3)])

    s5[:, :per, :] = rows_to_blocks(hub_part(slice(own, first_hub)), groups)
    s5[:, per:, :] = rows_to_blocks(hub_part(hub_slots), groups)
    send_all(groups, me, [("a", s5, r5, snd[8], rcv[8])])

    g1_ref[:chunk, :] = hub_part(slice(0, chunk))
    g1_ref[chunk:own, :] = hub_part(slice(chunk, own))
    wait_all(groups, r3, rcv[6], True)
    wait_all(groups, r4, rcv[7], True)
    bias_ref[...] = r4[...].sum(axis=0)
    s8[:, hid:] = r3[...].sum(axis=0)
    wait_all(groups, r5, rcv[8], True)
    home_dz1 = jnp.concatenate([r5[:, per:, :].sum(axis=0), jnp.zeros((8 - per, hid), F32)], axis=0).astype(BF16)
    back = r5[:, :per, :].reshape(halo, hid)
    dz1 = g1_ref[:own, :] + exact3(pick_t, split3(back))
    dz1 = jnp.where(plain, dz1, 0.0).astype(BF16)
    gw1 = dot(xt, dz1) + dot(home_x, home_dz1, 0, 0)
    s6[...] = rows_to_blocks(gw1, groups)
    s7[...] = dot(home_dz1, w1, 1, 1)[:per]
    send_all(groups, me, [("a", s6, r6, snd[9], rcv[9]), ("b", s7, r7, snd[10], rcv[10])])

    dxt = dot(w1, dz1, 1, 1)
    wait_all(groups, r6, rcv[9], True)
    s8[:, :hid] = r6[...].sum(axis=0)
    send_all(groups, me, [("b", s8, gw_ref, snd[11], rcv[11])])

    wait_all(groups, r7, rcv[10], True)
    hub_dx = r7[...].reshape(hubs, LANES).T
    dxt_ref[...] = dxt + exact3_right(split3(hub_dx), sel_f.T.astype(BF16))
    for buf, sem in zip((rx, rd, gx, gd, r1, r2, r3, r4, r5, r6, r7, gw_ref), snd):
        wait_all(groups, buf, sem, False)
    wait_all(groups, gw_ref, rcv[11], True)


def main_call(groups, own, halo, hubs, *args):
    hid = args[6].shape[1]
    per = hubs // groups
    slots, dsts = own + halo + hubs, own + hubs
    pairs = args[0].shape[0] // CHUNK_ROWS + slots // SRC_BLOCK * (dsts // DST_BLOCK)
    vmem = pl.BlockSpec(memory_space=pltpu.VMEM)
    blocks = [
        ("a", (2 * per, LANES), BF16), ("a", (per, LANES), F32), ("b", (per, LANES), BF16), ("b", (per, LANES), F32),
        ("a", (per, LANES + hid), F32), ("b", (per, hid), F32), ("a", (1, hid), F32), ("b", (1, hid + LANES), F32),
        ("a", (2 * per, hid), F32), ("a", (1, hid), F32), ("b", (per, LANES), F32), ("b", (1, 2 * hid), F32)]
    sends = [pltpu.VMEM(((groups,) if k == "a" else ()) + b, t) for k, b, t in blocks]
    recvs = [pltpu.VMEM((groups,) + b, t) for _, b, t in blocks[:-1]]
    shape = jax.ShapeDtypeStruct
    return pl.pallas_call(
        functools.partial(main_kernel, groups, own, halo, hubs),
        out_shape=[shape((LANES, own), F32), shape((groups, 1, 2 * hid), F32), shape((1, hid + LANES), F32)],
        in_specs=[vmem] * len(args),
        out_specs=[vmem] * 3,
        scratch_shapes=sends + recvs + [
            pltpu.VMEM((8, 256), jnp.int32),
            pltpu.SMEM((8, 256), jnp.int32),
            pltpu.VMEM((pairs + 1, SRC_BLOCK, DST_BLOCK), F32),
            pltpu.VMEM((slots, dsts), BF16),
            pltpu.VMEM((slots, dsts), BF16),
            pltpu.VMEM((slots, dsts), BF16),
            pltpu.VMEM((hubs, dsts), F32),
            pltpu.VMEM((hid, hubs), F32),
            pltpu.VMEM((slots - own, LANES), F32),
            pltpu.VMEM((slots, hid), F32),
            pltpu.VMEM((3, dsts, hid), BF16),
            pltpu.VMEM((hid, slots), BF16),
        ] + [pltpu.SemaphoreType.DMA] * (1 + 2 * len(blocks)),
        compiler_params=pltpu.CompilerParams(collective_id=0, has_side_effects=True, vmem_limit_bytes=56 * 2 ** 20),
        name="main_exchange",
    )(*args)


def output_kernel(dxt_ref, gw_ref, bias_ref, dx_out, gw1_out, gw2_out, b1_out, b2_out):
    feat_in, feat_out, hid = dx_out.shape[0], gw2_out.shape[0], gw2_out.shape[1]
    dx_out[...] = dxt_ref[:feat_in, :]
    gw = gw_ref[...].reshape(gw_ref.shape[0], 2 * hid)
    gw1_out[...] = gw[:feat_in, :hid]
    gw2_out[...] = gw[:feat_out, hid:]
    b1_out[...] = bias_ref[:, :hid]
    b2_out[...] = bias_ref[:, hid:hid + feat_out]


def solution(mesh):
    groups = mesh.shape["graph"]

    def device_step(x, dst, src, w, send, hub_ids, w_first, b_first, w_second, dy):
        own, feat_in = x.shape
        feat_out = dy.shape[1]
        hid = w_first.shape[1]
        halo, hubs = send.shape[0], hub_ids.shape[0]
        slots, dsts = own + halo + hubs, own + hubs
        bucket = jnp.right_shift(src, SRC_BLOCK.bit_length() - 1) * (dsts // DST_BLOCK)
        bucket = bucket + jnp.right_shift(dst, DST_BLOCK.bit_length() - 1)
        keys = bucket * BUCKET + jnp.bitwise_and(src, SRC_BLOCK - 1) * DST_BLOCK + jnp.bitwise_and(dst, DST_BLOCK - 1)
        keys, weights = lax.sort((keys, w), num_keys=1, is_stable=False)
        keys, weights = keys.reshape(-1, LANES), weights.reshape(-1, LANES)
        raw = main_call(
            groups, own, halo, hubs, keys, weights, x.T, dy.T, send[None, :], hub_ids[None, :], b_first[None, :],
            w_first, w_second.T)
        dx, gw1, gw2, gb1, gb2 = pl.pallas_call(
            output_kernel,
            out_shape=[jax.ShapeDtypeStruct(shape, F32) for shape in (
                (feat_in, own), (feat_in, hid), (feat_out, hid), (1, hid), (1, feat_out))],
            name="outputs",
        )(*raw)
        return dx.T, gw1, gw2.T, gb1[0], gb2[0]

    rows, flat = P(("data", "graph"), None), P(("data", "graph"))
    return jax.shard_map(
        device_step,
        mesh=mesh,
        in_specs=(rows, flat, flat, flat, flat, P("data"), P(), P(), P(), rows),
        out_specs=(rows, P("data", None), P("data", None), P("data"), P("data")),
        check_vma=False,
    )
```

```python
import functools

import jax
import jax.numpy as jnp
from jax import lax
from jax.experimental import pallas as pl
from jax.experimental.pallas import tpu as pltpu
from jax.sharding import PartitionSpec as P

BF16 = jnp.bfloat16
F32 = jnp.float32
HI = lax.Precision.HIGHEST
LANES = 128
MESH = pl.DeviceIdType.MESH


def dot(a, b, ca=1, cb=0, precision=None):
    return lax.dot_general(a, b, (((ca,), (cb,)), ((), ())), precision=precision, preferred_element_type=F32)


def split3(a):
    hi = a.astype(BF16)
    rest = a - hi.astype(F32)
    mid = rest.astype(BF16)
    return hi, mid, (rest - mid.astype(F32)).astype(BF16)


def exact3(sel, pieces, ca=1):
    return dot(sel, pieces[2], ca) + dot(sel, pieces[1], ca) + dot(sel, pieces[0], ca)


def exact3_right(pieces, sel):
    return dot(pieces[2], sel) + dot(pieces[1], sel) + dot(pieces[0], sel)


def full6(a, b):
    low = dot(a[0], b[2]) + dot(a[2], b[0]) + dot(a[1], b[1])
    return low + (dot(a[0], b[1]) + dot(a[1], b[0])) + dot(a[0], b[0])


def partner(groups, me, i):
    low = sum(2 << k for k in range(0, groups.bit_length() - 2, 2))
    t = jnp.bitwise_xor(i - 1, 2 * low + 1)
    high = jnp.bitwise_and(jnp.right_shift(t, 1), low)
    return jnp.bitwise_xor(me, jnp.bitwise_xor(t, jnp.bitwise_xor(high, low)))


def wait_all(groups, buf, sem, whole):
    part = buf if whole else buf.at[pl.ds(0, groups - 1)]
    pltpu.make_async_copy(part, part, sem).wait()


def send_all(groups, me, items):
    def send(i, carry):
        peer = partner(groups, me, i)
        for kind, src, dst, send_sem, recv_sem in items:
            pltpu.make_async_remote_copy(
                src_ref=src.at[peer] if kind == "a" else src,
                dst_ref=dst.at[me],
                send_sem=send_sem,
                recv_sem=recv_sem,
                device_id=(0, peer),
                device_id_type=MESH,
            ).start()
        return carry

    lax.fori_loop(1, groups, send, 0)
    for kind, src, dst, _, recv_sem in items:
        pltpu.make_async_copy(src.at[me] if kind == "a" else src, dst.at[me], recv_sem).start()


def greet_all(groups, me):
    barrier = pltpu.get_barrier_semaphore()

    def greet(i, carry):
        pl.semaphore_signal(barrier, inc=1, device_id=(0, partner(groups, me, i)), device_id_type=MESH)
        return carry

    lax.fori_loop(1, groups, greet, 0)
    return barrier


def padded(ref, rows, cols):
    a = ref[...]
    if cols > a.shape[1]:
        a = jnp.concatenate([a, jnp.zeros((a.shape[0], cols - a.shape[1]), a.dtype)], axis=1)
    if rows > a.shape[0]:
        a = jnp.concatenate([a, jnp.zeros((rows - a.shape[0], cols), a.dtype)], axis=0)
    return a


SRC_BLOCK, DST_BLOCK = 128, 256
BUCKET = SRC_BLOCK * DST_BLOCK
CHUNK, UNROLL = 256, 19


def bitonic(keys, weights, low, high):
    vregs = keys.shape[0]
    base = vregs.bit_length() - 1

    def bit(shape, m):
        axis, m = (len(shape) - 2, m - base) if m < base + 3 else (len(shape) - 1, m - base - 3)
        return jnp.bitwise_and(jnp.right_shift(lax.broadcasted_iota(jnp.int32, shape, axis), m), 1)

    def other(a, j):
        if j >= base + 3:
            lane = lax.broadcasted_iota(jnp.int32, (vregs * 8, LANES), 1)
            return jnp.take_along_axis(
                a.reshape(vregs * 8, LANES), jnp.bitwise_xor(lane, 1 << (j - base - 3)), axis=1).reshape(a.shape)
        step = 1 << (j - base)
        if step == 4:
            return pltpu.roll(a, 4, 1)
        return jnp.where(bit(a.shape, j) > 0, pltpu.roll(a, step, 1), pltpu.roll(a, 8 - step, 1))

    full = keys.shape
    for k in range(low, high + 1):
        for j in range(k - 1, -1, -1):
            if j < base:
                near = 1 << j
                parts = (vregs // (2 * near), 2, near, 8, LANES)
                a, b = keys.reshape(parts)[:, 0], keys.reshape(parts)[:, 1]
                wa, wb = weights.reshape(parts)[:, 0], weights.reshape(parts)[:, 1]
                swap = a > b
                if k < base:
                    block = lax.broadcasted_iota(jnp.int32, a.shape, 0)
                    swap = jnp.logical_xor(swap, jnp.bitwise_and(jnp.right_shift(block, k - j - 1), 1) > 0)
                elif k < base + 10:
                    swap = jnp.logical_xor(swap, bit(a.shape, k) > 0)
                keys = jnp.stack([jnp.where(swap, b, a), jnp.where(swap, a, b)], axis=1).reshape(full)
                weights = jnp.stack([jnp.where(swap, wb, wa), jnp.where(swap, wa, wb)], axis=1).reshape(full)
            else:
                keys2, weights2 = other(keys, j), other(weights, j)
                upper = bit(full, j)
                if k < base + 10:
                    upper = jnp.bitwise_xor(upper, bit(full, k))
                take = jnp.bitwise_xor(keys2, -upper) < jnp.bitwise_xor(keys, -upper)
                keys = jnp.where(take, keys2, keys)
                weights = jnp.where(take, weights2, weights)
    return keys, weights


def ring_sum(a, axis):
    step = a.shape[axis] // 2
    while step:
        a = a + pltpu.roll(a, step, axis)
        step //= 2
    return a


def list_pairs(buckets, key_ref, plan_ref):
    size = CHUNK
    shift = size.bit_length() - 1
    total = 1 << buckets.bit_length()

    def count(i, carry):
        bucket = jnp.right_shift(key_ref[pl.ds(pl.multiple_of(i * 8, 8), 8), :], BUCKET.bit_length() - 1)
        return tuple(c + jnp.where(bucket <= b, 1, 0) for b, c in enumerate(carry))

    counts = lax.fori_loop(0, key_ref.shape[0] // 8, count, (jnp.zeros((8, LANES), jnp.int32),) * buckets)
    counts = [ring_sum(c, 0)[:1] for c in counts]
    none = jnp.zeros((1, LANES), jnp.int32)
    counts = [none] + counts + [counts[-1]] * (total - buckets)
    low = ring_sum(jnp.concatenate(counts[:total], axis=0), 1)
    high = ring_sum(jnp.concatenate(counts[1:], axis=0), 1)
    start = jnp.right_shift(low, shift)
    pairs = jnp.where(high > low, jnp.right_shift(high + size - 1, shift) - start, 0)
    row = lax.broadcasted_iota(jnp.int32, (total, LANES), 0)
    last, step = pairs, 1
    while step < total:
        last = last + jnp.where(row >= step, pltpu.roll(last, step, 0), 0)
        step *= 2
    first = last - pairs
    for half in range(plan_ref.shape[1] // LANES):
        at = lax.broadcasted_iota(jnp.int32, (total, LANES), 1) + half * LANES
        inside = (first <= at) & (at < last)
        rows = [
            jnp.where(last <= at, 1, 0), jnp.where(inside, start + at - first, 0), jnp.where(inside & (at > first), 1, 0),
            jnp.where((row == at) & (pairs > 0), last, 0)]
        rows = [ring_sum(r, 0)[:1] for r in rows] + [none] * 4
        plan_ref[:, half * LANES:(half + 1) * LANES] = jnp.concatenate(rows, axis=0)


def add_pairs(plan_ref, key_ref, w_ref, cum_ref, low, high):
    src_ids = lax.broadcasted_iota(jnp.int32, (SRC_BLOCK, LANES), 0).astype(F32).astype(BF16)
    dst_ids = lax.broadcasted_iota(jnp.int32, (DST_BLOCK, LANES), 0).astype(F32).astype(BF16)
    one, zero = jnp.ones((), BF16), jnp.zeros((), BF16)

    def step(it, carry):
        work = []
        for u in range(UNROLL):
            b, c = plan_ref[0, it * UNROLL + u], plan_ref[1, it * UNROLL + u]
            rel_row = key_ref[pl.ds(c, 1), :] - b * BUCKET
            w_row = w_ref[pl.ds(c, 1), :]
            lhs, rhs = [], []
            for r in range(0, CHUNK, LANES):
                rel, weight = rel_row[:, r:r + LANES], w_row[:, r:r + LANES]
                src = jnp.right_shift(rel, DST_BLOCK.bit_length() - 1)
                src = jnp.where((src >= 0) & (src < SRC_BLOCK), src, 512).astype(F32).astype(BF16)
                dst = jnp.bitwise_and(rel, DST_BLOCK - 1).astype(F32).astype(BF16)
                hit = src_ids == jnp.broadcast_to(src, src_ids.shape)
                lhs.append(jnp.concatenate(
                    [jnp.where(hit, jnp.broadcast_to(p, src_ids.shape), zero) for p in split3(weight)], axis=0))
                rhs.append(jnp.where(dst_ids == jnp.broadcast_to(dst, dst_ids.shape), one, zero))
            work.append((jnp.concatenate(lhs, axis=1), jnp.concatenate(rhs, axis=1)))
        outs = [dot(lhs, rhs, 1, 1) for lhs, rhs in work]
        total = cum_ref[it * UNROLL]
        for u, out in enumerate(outs):
            same = jnp.broadcast_to(plan_ref[2, it * UNROLL + u], (1, DST_BLOCK)) > 0
            out = out[2 * SRC_BLOCK:] + out[SRC_BLOCK:2 * SRC_BLOCK] + out[:SRC_BLOCK]
            total = out + jnp.where(same, total, 0.0)
            cum_ref[it * UNROLL + u + 1] = total
        return carry

    lax.fori_loop(low, high, step, 0)


def rows_to_blocks(a, groups):
    return a.reshape(groups, a.shape[0] // groups, a.shape[1])


def main_kernel(groups, own, halo, hubs, dst_ref, src_ref, w_in_ref, xt_ref, dyt_ref, send_ref, hub_ref, b1_ref, w1_ref, w2t_ref,
                dxt_ref, gw_ref, bias_ref,
                sx, sd, hx, hd, s1, s2, s3, s4, s5, s6, s7, s8,
                rx, rd, gx, gd, r1, r2, r3, r4, r5, r6, r7,
                list_ref, plan_ref, raw_ref, sort_k, sort_w, key_ref, w_ref, cum_ref, hi_ref, mid_ref, low_ref, hubrow_ref, pt_ref, g2_ref, g1_ref, dy_ref, zt_ref, plan_sem, *sems):
    count = len(sems) // 2
    snd, rcv = sems[:count], sems[count:]
    adj = (hi_ref, mid_ref, low_ref)
    per = hubs // groups
    hid = b1_ref.shape[1]
    feat_in = xt_ref.shape[0]
    first_hub = own + halo
    slots, dsts = own + halo + hubs, own + hubs
    tops = dsts // DST_BLOCK
    me = lax.axis_index("graph")
    barrier = greet_all(groups, me)
    steps = (cum_ref.shape[0] - 1) // UNROLL
    middle = steps * 3 // 8
    cum_ref[0] = jnp.zeros((SRC_BLOCK, DST_BLOCK), F32)
    dst, src = dst_ref[...], src_ref[...]
    bucket = jnp.right_shift(src, SRC_BLOCK.bit_length() - 1) * tops + jnp.right_shift(dst, DST_BLOCK.bit_length() - 1)
    raw_ref[...] = (
        bucket * BUCKET + jnp.bitwise_and(src, SRC_BLOCK - 1) * DST_BLOCK + jnp.bitwise_and(dst, DST_BLOCK - 1))
    list_pairs(slots // SRC_BLOCK * tops, raw_ref, list_ref)
    plan = pltpu.make_async_copy(list_ref, plan_ref, plan_sem)
    plan.start()

    lane = lax.broadcasted_iota(jnp.int32, (1, LANES), 1)
    half = lane < LANES // 2
    own_row = lax.broadcasted_iota(jnp.int32, (own, 1), 0)
    pick_t = (own_row == send_ref[...]).astype(F32).astype(BF16)
    sel_f = (own_row == hub_ref[...] - me * own).astype(F32)
    sel_t = sel_f.astype(BF16)
    plain = jnp.sum(sel_f, axis=1, keepdims=True) == 0
    number = lax.broadcasted_iota(jnp.int32, (1, hubs), 1) + 1
    numbers = jnp.broadcast_to(number.astype(F32), (8, hubs)).astype(BF16)
    code_row = dot(numbers, sel_t, 1, 1)[:1]
    plain_row = code_row == 0
    xt = padded(xt_ref, LANES, own)
    feature = lax.broadcasted_iota(jnp.int32, (LANES, 1), 0)
    xt = jnp.where(feature == feat_in, code_row, xt.astype(F32)).astype(BF16)
    dyt = padded(dyt_ref, LANES, own)
    picked = dot(jnp.concatenate((xt,) + split3(dyt), axis=0), jnp.concatenate([pick_t, sel_t], axis=1))
    hub_dt = picked[3 * LANES:, halo:] + picked[2 * LANES:3 * LANES, halo:] + picked[LANES:2 * LANES, halo:]
    sx[:, :per, :] = rows_to_blocks(picked[:LANES, :halo].T, groups).astype(BF16)
    sx[:, per:, :] = rows_to_blocks(picked[:LANES, halo:].T, groups).astype(BF16)
    sd[...] = rows_to_blocks(hub_dt.T, groups)
    phases = raw_ref.size.bit_length() - 1
    sort_k[...], sort_w[...] = bitonic(
        raw_ref[...].reshape(sort_k.shape), w_in_ref[...].reshape(sort_w.shape), 1, phases - 4)
    pl.semaphore_wait(barrier, groups - 1)
    send_all(groups, me, [("a", sx, rx, snd[0], rcv[0]), ("a", sd, rd, snd[1], rcv[1])])

    w1 = padded(w1_ref, LANES, hid)
    w1_t = w1.astype(F32).T.astype(BF16)
    zt_ref[:, :own] = jnp.where(plain_row, dot(w1_t, xt), 0.0).astype(BF16)
    dy = dyt.T
    keys, weights = bitonic(sort_k[...], sort_w[...], phases - 3, phases)
    key_ref[...] = keys.reshape(raw_ref.shape).T
    w_ref[...] = weights.reshape(raw_ref.shape).T
    plan.wait()
    add_pairs(plan_ref, key_ref, w_ref, cum_ref, 0, middle)
    wait_all(groups, rx, rcv[0], True)
    wait_all(groups, rd, rcv[1], True)
    got = rx[...].astype(F32)
    home_x = got[:, per:, :].sum(axis=0)
    hx[...] = home_x.astype(BF16)
    hd[...] = rd[...].sum(axis=0)
    send_all(groups, me, [("b", hx, gx, snd[2], rcv[2]), ("b", hd, gd, snd[3], rcv[3])])

    home_x = jnp.concatenate([home_x, jnp.zeros((8 - per, LANES), F32)], axis=0).astype(BF16)
    add_pairs(plan_ref, key_ref, w_ref, cum_ref, middle, steps)

    def renamed(i):
        cell = [cum_ref[plan_ref[3, i * tops + j]] for j in range(tops)]
        mine = jnp.concatenate(cell[:own // DST_BLOCK], axis=1)
        pieces = split3(mine)
        return mine, pieces, jnp.concatenate(cell[own // DST_BLOCK:], axis=1) + exact3_right(pieces, sel_t)

    def rename(i, carry):
        _, pieces, hub = renamed(i)
        rows = pl.ds(pl.multiple_of(i * SRC_BLOCK, SRC_BLOCK), SRC_BLOCK)
        for ref, left, right in zip(adj, pieces, split3(hub)):
            ref[rows, :own] = left
            ref[rows, own:] = right
        return carry

    def rename_hub(i, carry):
        mine, _, hub = renamed(first_hub // SRC_BLOCK + i)
        rows = pl.ds(pl.multiple_of(i * SRC_BLOCK, SRC_BLOCK), SRC_BLOCK)
        hubrow_ref[rows, :own] = mine
        hubrow_ref[rows, own:] = hub
        return carry

    lax.fori_loop(0, first_hub // SRC_BLOCK, rename, 0)
    lax.fori_loop(0, hubs // SRC_BLOCK, rename_hub, 0)
    halo_x = got[:, :per, :].reshape(halo, LANES).astype(BF16)
    column = jnp.broadcast_to(jnp.where(lane == feat_in, 1.0, 0.0), (8, LANES)).astype(BF16)
    halo_row = dot(column, halo_x, 1, 1)[:1].astype(jnp.int32)
    zt_ref[:, own:first_hub] = jnp.where(halo_row == 0, dot(w1_t, halo_x, 1, 1), 0.0).astype(BF16)
    halo_sel = (lax.broadcasted_iota(jnp.int32, (hubs, 1), 0) + 1 == halo_row).astype(F32)
    moved = jnp.concatenate([sel_f.T, halo_sel], axis=1).astype(BF16)
    for j in range(tops):
        cols = slice(j * DST_BLOCK, (j + 1) * DST_BLOCK)
        new = hubrow_ref[:, cols] + exact3(moved, [a[:first_hub, cols] for a in adj])
        for a, piece in zip(adj, split3(new)):
            a[first_hub:, cols] = piece

    def forward(rows, cols):
        zt = zt_ref[:, rows]
        return dot(zt, low_ref[rows, cols]) + dot(zt, mid_ref[rows, cols]) + dot(zt, hi_ref[rows, cols])

    def pack(d):
        dh, dm, dl = split3(d)
        d_two = (dh.astype(F32) + pltpu.roll(dm.astype(F32), LANES // 2, 1)).astype(BF16)
        return jnp.concatenate([d_two, dl], axis=1), d_two, dh

    def grad_out_sums(rows, cols, packed):
        a = dot(hi_ref[rows, cols], packed[0])
        t = a[:, :LANES] + a[:, LANES:] + dot(mid_ref[rows, cols], packed[1]) + dot(low_ref[rows, cols], packed[2])
        return jnp.where(half, t + pltpu.roll(t, LANES // 2, 1), 0.0)

    own_cols, hub_cols = slice(0, own), slice(own, dsts)
    pt_ref[...] = forward(slice(0, first_hub), hub_cols)
    d_own = pack(jnp.where(plain, dy, 0.0))
    g2_ref[...] = grad_out_sums(slice(own, slots), own_cols, d_own)
    wait_all(groups, gx, rcv[2], True)
    wait_all(groups, gd, rcv[3], True)
    hub_x = gx[...].astype(F32).reshape(hubs, LANES).astype(BF16)
    zt_ref[:, first_hub:] = dot(w1_t, hub_x, 1, 1).astype(BF16)
    d_hub = pack(gd[...].reshape(hubs, LANES))
    hub_slots = slice(first_hub, slots)
    y_hub = (pt_ref[...] + forward(hub_slots, hub_cols)).T
    s1[:, :, LANES:] = rows_to_blocks(y_hub, groups)
    g2_halo = g2_ref[:halo, :] + grad_out_sums(slice(own, first_hub), hub_cols, d_hub)
    g2_hub = g2_ref[halo:, :] + grad_out_sums(hub_slots, hub_cols, d_hub)
    s1[:, :, :LANES] = rows_to_blocks(g2_halo + pltpu.roll(g2_hub, LANES // 2, 1), groups)
    send_all(groups, me, [("a", s1, r1, snd[4], rcv[4])])

    b1 = b1_ref[...]
    w2t = padded(w2t_ref, LANES, hid)
    pre = forward(slice(0, slots), own_cols).T + b1
    g2_own = grad_out_sums(slice(0, own), own_cols, d_own) + grad_out_sums(slice(0, own), hub_cols, d_hub)
    hidden = jnp.where(plain, jax.nn.relu(pre), 0.0).astype(BF16)
    live = plain & (pre > 0)
    wait_all(groups, r1, rcv[4], True)
    home = r1[...].sum(axis=0)
    pad = jnp.zeros((8 - per, LANES), F32)
    home_g = jnp.where(half, pltpu.roll(jnp.concatenate([home[:, :LANES], pad], axis=0), LANES // 2, 1), 0.0)
    home_pre = jnp.concatenate([home[:, LANES:] + b1, jnp.zeros((8 - per, hid), F32)], axis=0)
    home_dz2 = home_g.astype(BF16)
    home_dy = jnp.where(home_pre > 0, dot(home_dz2, w2t), 0.0)
    s2[...] = home_dy[:per]
    send_all(groups, me, [("b", s2, r2, snd[5], rcv[5])])

    back = jnp.where(half, r1[:, :, :LANES].reshape(halo, LANES), 0.0)
    dz2 = jnp.where(plain, g2_own + exact3(pick_t, split3(back)), 0.0).astype(BF16)
    dy1 = jnp.where(live, dot(dz2, w2t), 0.0)
    home_hidden = jax.nn.relu(home_pre).astype(BF16)
    gw2 = dot(dz2, hidden, 0, 0) + dot(home_dz2, home_hidden, 0, 0)
    s3[...] = rows_to_blocks(gw2, groups)
    s4[:, :hid] = dy1.sum(axis=0, keepdims=True) + home_dy.sum(axis=0, keepdims=True)
    s4[:, hid:] = dy.sum(axis=0, keepdims=True)
    send_all(groups, me, [("a", s3, r3, snd[6], rcv[6]), ("b", s4, r4, snd[7], rcv[7])])
    for p, piece in enumerate(split3(dy1)):
        dy_ref[p, :own, :] = piece
    chunk = 256

    def own_part(i, carry):
        rows = pl.ds(pl.multiple_of(i * chunk, chunk), chunk)
        g1_ref[rows, :] = full6([a[rows, :own] for a in adj], [dy_ref[p, :own, :] for p in range(3)])
        return carry

    lax.fori_loop(0, slots // chunk, own_part, 0)
    wait_all(groups, r2, rcv[5], True)
    for p, piece in enumerate(split3(r2[...].reshape(hubs, hid))):
        dy_ref[p, own:, :] = piece

    def hub_part(rows):
        return g1_ref[rows, :] + full6([a[rows, own:] for a in adj], [dy_ref[p, own:, :] for p in range(3)])

    s5[:, :per, :] = rows_to_blocks(hub_part(slice(own, first_hub)), groups)
    s5[:, per:, :] = rows_to_blocks(hub_part(hub_slots), groups)
    send_all(groups, me, [("a", s5, r5, snd[8], rcv[8])])

    g1_ref[:chunk, :] = hub_part(slice(0, chunk))
    g1_ref[chunk:own, :] = hub_part(slice(chunk, own))
    wait_all(groups, r3, rcv[6], True)
    wait_all(groups, r4, rcv[7], True)
    bias_ref[...] = r4[...].sum(axis=0)
    s8[:, hid:] = r3[...].sum(axis=0)
    wait_all(groups, r5, rcv[8], True)
    home_dz1 = jnp.concatenate([r5[:, per:, :].sum(axis=0), jnp.zeros((8 - per, hid), F32)], axis=0).astype(BF16)
    back = r5[:, :per, :].reshape(halo, hid)
    dz1 = g1_ref[:own, :] + exact3(pick_t, split3(back))
    dz1 = jnp.where(plain, dz1, 0.0).astype(BF16)
    gw1 = dot(xt, dz1) + dot(home_x, home_dz1, 0, 0)
    s6[...] = rows_to_blocks(gw1, groups)
    s7[...] = dot(home_dz1, w1, 1, 1)[:per]
    send_all(groups, me, [("a", s6, r6, snd[9], rcv[9]), ("b", s7, r7, snd[10], rcv[10])])

    dxt = dot(w1, dz1, 1, 1)
    wait_all(groups, r6, rcv[9], True)
    s8[:, :hid] = r6[...].sum(axis=0)
    send_all(groups, me, [("b", s8, gw_ref, snd[11], rcv[11])])

    wait_all(groups, r7, rcv[10], True)
    hub_dx = r7[...].reshape(hubs, LANES).T
    dxt_ref[...] = dxt + exact3_right(split3(hub_dx), sel_f.T.astype(BF16))
    for buf, sem in zip((rx, rd, gx, gd, r1, r2, r3, r4, r5, r6, r7, gw_ref), snd):
        wait_all(groups, buf, sem, False)
    wait_all(groups, gw_ref, rcv[11], True)


def main_call(groups, own, halo, hubs, *args):
    hid = args[7].shape[1]
    per = hubs // groups
    slots, dsts = own + halo + hubs, own + hubs
    edges = args[0].size
    pairs = edges // CHUNK + slots // SRC_BLOCK * (dsts // DST_BLOCK)
    vmem = pl.BlockSpec(memory_space=pltpu.VMEM)
    blocks = [
        ("a", (2 * per, LANES), BF16), ("a", (per, LANES), F32), ("b", (per, LANES), BF16), ("b", (per, LANES), F32),
        ("a", (per, LANES + hid), F32), ("b", (per, hid), F32), ("a", (1, hid), F32), ("b", (1, hid + LANES), F32),
        ("a", (2 * per, hid), F32), ("a", (1, hid), F32), ("b", (per, LANES), F32), ("b", (1, 2 * hid), F32)]
    sends = [pltpu.VMEM(((groups,) if k == "a" else ()) + b, t) for k, b, t in blocks]
    recvs = [pltpu.VMEM((groups,) + b, t) for _, b, t in blocks[:-1]]
    shape = jax.ShapeDtypeStruct
    return pl.pallas_call(
        functools.partial(main_kernel, groups, own, halo, hubs),
        out_shape=[shape((LANES, own), F32), shape((groups, 1, 2 * hid), F32), shape((1, hid + LANES), F32)],
        in_specs=[vmem] * len(args),
        out_specs=[vmem] * 3,
        scratch_shapes=sends + recvs + [
            pltpu.VMEM((8, 256), jnp.int32),
            pltpu.SMEM((8, 256), jnp.int32),
            pltpu.VMEM((edges // LANES, LANES), jnp.int32),
            pltpu.VMEM((edges // LANES // 8, 8, LANES), jnp.int32),
            pltpu.VMEM((edges // LANES // 8, 8, LANES), F32),
            pltpu.VMEM((edges // CHUNK, CHUNK), jnp.int32),
            pltpu.VMEM((edges // CHUNK, CHUNK), F32),
            pltpu.VMEM((pairs + 1, SRC_BLOCK, DST_BLOCK), F32),
            pltpu.VMEM((slots, dsts), BF16),
            pltpu.VMEM((slots, dsts), BF16),
            pltpu.VMEM((slots, dsts), BF16),
            pltpu.VMEM((hubs, dsts), F32),
            pltpu.VMEM((hid, hubs), F32),
            pltpu.VMEM((slots - own, LANES), F32),
            pltpu.VMEM((slots, hid), F32),
            pltpu.VMEM((3, dsts, hid), BF16),
            pltpu.VMEM((hid, slots), BF16),
        ] + [pltpu.SemaphoreType.DMA] * (1 + 2 * len(blocks)),
        compiler_params=pltpu.CompilerParams(collective_id=0, has_side_effects=True, vmem_limit_bytes=56 * 2 ** 20),
        name="main_exchange",
    )(*args)


def output_kernel(dxt_ref, gw_ref, bias_ref, dx_out, gw1_out, gw2_out, b1_out, b2_out):
    feat_in, feat_out, hid = dx_out.shape[0], gw2_out.shape[0], gw2_out.shape[1]
    dx_out[...] = dxt_ref[:feat_in, :]
    gw = gw_ref[...].reshape(gw_ref.shape[0], 2 * hid)
    gw1_out[...] = gw[:feat_in, :hid]
    gw2_out[...] = gw[:feat_out, hid:]
    b1_out[...] = bias_ref[:, :hid]
    b2_out[...] = bias_ref[:, hid:hid + feat_out]


def solution(mesh):
    groups = mesh.shape["graph"]

    def device_step(x, dst, src, w, send, hub_ids, w_first, b_first, w_second, dy):
        own, feat_in = x.shape
        feat_out = dy.shape[1]
        hid = w_first.shape[1]
        halo, hubs = send.shape[0], hub_ids.shape[0]
        edges = [v.reshape(-1, LANES) for v in (dst, src, w)]
        raw = main_call(
            groups, own, halo, hubs, *edges, x.T, dy.T, send[None, :], hub_ids[None, :], b_first[None, :],
            w_first, w_second.T)
        dx, gw1, gw2, gb1, gb2 = pl.pallas_call(
            output_kernel,
            out_shape=[jax.ShapeDtypeStruct(shape, F32) for shape in (
                (feat_in, own), (feat_in, hid), (feat_out, hid), (1, hid), (1, feat_out))],
            name="outputs",
        )(*raw)
        return dx.T, gw1, gw2.T, gb1[0], gb2[0]

    rows, flat = P(("data", "graph"), None), P(("data", "graph"))
    return jax.shard_map(
        device_step,
        mesh=mesh,
        in_specs=(rows, flat, flat, flat, flat, P("data"), P(), P(), P(), rows),
        out_specs=(rows, P("data", None), P("data", None), P("data"), P("data")),
        check_vma=False,
    )
```

```python
import functools

import jax
import jax.numpy as jnp
from jax import lax
from jax.experimental import pallas as pl
from jax.experimental.pallas import tpu as pltpu
from jax.sharding import PartitionSpec as P

BF16 = jnp.bfloat16
F32 = jnp.float32
HI = lax.Precision.HIGHEST
LANES = 128
MESH = pl.DeviceIdType.MESH


def dot(a, b, ca=1, cb=0, precision=None):
    return lax.dot_general(a, b, (((ca,), (cb,)), ((), ())), precision=precision, preferred_element_type=F32)


def split3(a):
    hi = a.astype(BF16)
    rest = a - hi.astype(F32)
    mid = rest.astype(BF16)
    return hi, mid, (rest - mid.astype(F32)).astype(BF16)


def exact3(sel, pieces, ca=1):
    return dot(sel, pieces[2], ca) + dot(sel, pieces[1], ca) + dot(sel, pieces[0], ca)


def exact3_right(pieces, sel):
    return dot(pieces[2], sel) + dot(pieces[1], sel) + dot(pieces[0], sel)


def full6(a, b):
    low = dot(a[0], b[2]) + dot(a[2], b[0]) + dot(a[1], b[1])
    return low + (dot(a[0], b[1]) + dot(a[1], b[0])) + dot(a[0], b[0])


def partner(groups, me, i):
    low = sum(2 << k for k in range(0, groups.bit_length() - 2, 2))
    t = jnp.bitwise_xor(i - 1, 2 * low + 1)
    high = jnp.bitwise_and(jnp.right_shift(t, 1), low)
    return jnp.bitwise_xor(me, jnp.bitwise_xor(t, jnp.bitwise_xor(high, low)))


def wait_all(groups, buf, sem, whole):
    part = buf if whole else buf.at[pl.ds(0, groups - 1)]
    pltpu.make_async_copy(part, part, sem).wait()


def send_all(groups, me, items):
    def send(i, carry):
        peer = partner(groups, me, i)
        for kind, src, dst, send_sem, recv_sem in items:
            pltpu.make_async_remote_copy(
                src_ref=src.at[peer] if kind == "a" else src,
                dst_ref=dst.at[me],
                send_sem=send_sem,
                recv_sem=recv_sem,
                device_id=(0, peer),
                device_id_type=MESH,
            ).start()
        return carry

    lax.fori_loop(1, groups, send, 0)
    for kind, src, dst, _, recv_sem in items:
        pltpu.make_async_copy(src.at[me] if kind == "a" else src, dst.at[me], recv_sem).start()


def greet_all(groups, me):
    barrier = pltpu.get_barrier_semaphore()

    def greet(i, carry):
        pl.semaphore_signal(barrier, inc=1, device_id=(0, partner(groups, me, i)), device_id_type=MESH)
        return carry

    lax.fori_loop(1, groups, greet, 0)
    return barrier


def padded(ref, rows, cols):
    a = ref[...]
    if cols > a.shape[1]:
        a = jnp.concatenate([a, jnp.zeros((a.shape[0], cols - a.shape[1]), a.dtype)], axis=1)
    if rows > a.shape[0]:
        a = jnp.concatenate([a, jnp.zeros((rows - a.shape[0], cols), a.dtype)], axis=0)
    return a


SRC_BLOCK, DST_BLOCK = 64, 256
BUCKET = SRC_BLOCK * DST_BLOCK
CHUNK, UNROLL = 256, 44


def bitonic(keys, weights, low, high):
    vregs = keys.shape[0]
    base = vregs.bit_length() - 1

    def bit(shape, m):
        axis, m = (len(shape) - 2, m - base) if m < base + 3 else (len(shape) - 1, m - base - 3)
        return jnp.bitwise_and(jnp.right_shift(lax.broadcasted_iota(jnp.int32, shape, axis), m), 1)

    def other(a, j):
        if j >= base + 3:
            lane = lax.broadcasted_iota(jnp.int32, (vregs * 8, LANES), 1)
            return jnp.take_along_axis(
                a.reshape(vregs * 8, LANES), jnp.bitwise_xor(lane, 1 << (j - base - 3)), axis=1).reshape(a.shape)
        step = 1 << (j - base)
        if step == 4:
            return pltpu.roll(a, 4, 1)
        return jnp.where(bit(a.shape, j) > 0, pltpu.roll(a, step, 1), pltpu.roll(a, 8 - step, 1))

    full = keys.shape
    for k in range(low, high + 1):
        for j in range(k - 1, -1, -1):
            if j < base:
                near = 1 << j
                parts = (vregs // (2 * near), 2, near, 8, LANES)
                a, b = keys.reshape(parts)[:, 0], keys.reshape(parts)[:, 1]
                wa, wb = weights.reshape(parts)[:, 0], weights.reshape(parts)[:, 1]
                swap = a > b
                if k < base:
                    block = lax.broadcasted_iota(jnp.int32, a.shape, 0)
                    swap = jnp.logical_xor(swap, jnp.bitwise_and(jnp.right_shift(block, k - j - 1), 1) > 0)
                elif k < base + 10:
                    swap = jnp.logical_xor(swap, bit(a.shape, k) > 0)
                keys = jnp.stack([jnp.where(swap, b, a), jnp.where(swap, a, b)], axis=1).reshape(full)
                weights = jnp.stack([jnp.where(swap, wb, wa), jnp.where(swap, wa, wb)], axis=1).reshape(full)
            else:
                keys2, weights2 = other(keys, j), other(weights, j)
                upper = bit(full, j)
                if k < base + 10:
                    upper = jnp.bitwise_xor(upper, bit(full, k))
                take = jnp.bitwise_xor(keys2, -upper) < jnp.bitwise_xor(keys, -upper)
                keys = jnp.where(take, keys2, keys)
                weights = jnp.where(take, weights2, weights)
    return keys, weights


def ring_sum(a, axis):
    step = a.shape[axis] // 2
    while step:
        a = a + pltpu.roll(a, step, axis)
        step //= 2
    return a


def list_pairs(buckets, key_ref, plan_ref):
    size = CHUNK
    shift = size.bit_length() - 1
    total = 1 << buckets.bit_length()

    def count(at, i, carry):
        bucket = jnp.right_shift(key_ref[pl.ds(pl.multiple_of(i * 8, 8), 8), :], BUCKET.bit_length() - 1)
        return tuple(c + jnp.where(bucket <= at + b, 1, 0) for b, c in enumerate(carry))

    counts = ()
    for at in range(0, buckets, 24):
        zeros = (jnp.zeros((8, LANES), jnp.int32),) * min(24, buckets - at)
        counts += lax.fori_loop(0, key_ref.shape[0] // 8, functools.partial(count, at), zeros)
    counts = [ring_sum(c, 0)[:1] for c in counts]
    none = jnp.zeros((1, LANES), jnp.int32)
    counts = [none] + counts + [counts[-1]] * (total - buckets)
    low = ring_sum(jnp.concatenate(counts[:total], axis=0), 1)
    high = ring_sum(jnp.concatenate(counts[1:], axis=0), 1)
    start = jnp.right_shift(low, shift)
    pairs = jnp.where(high > low, jnp.right_shift(high + size - 1, shift) - start, 0)
    row = lax.broadcasted_iota(jnp.int32, (total, LANES), 0)
    last, step = pairs, 1
    while step < total:
        last = last + jnp.where(row >= step, pltpu.roll(last, step, 0), 0)
        step *= 2
    first = last - pairs
    for half in range(plan_ref.shape[1] // LANES):
        at = lax.broadcasted_iota(jnp.int32, (total, LANES), 1) + half * LANES
        inside = (first <= at) & (at < last)
        rows = [
            jnp.where(last <= at, 1, 0), jnp.where(inside, start + at - first, 0), jnp.where(inside & (at > first), 1, 0),
            jnp.where((row == at) & (pairs > 0), last, 0)]
        rows = [ring_sum(r, 0)[:1] for r in rows] + [none] * 4
        plan_ref[:, half * LANES:(half + 1) * LANES] = jnp.concatenate(rows, axis=0)


def add_pairs(plan_ref, key_ref, w_ref, column_ref, cum_ref, low, high):
    src_ids = lax.broadcasted_iota(jnp.int32, (SRC_BLOCK, LANES), 0).astype(F32).astype(BF16)
    lane = lax.broadcasted_iota(jnp.int32, (CHUNK, LANES), 1)
    dst_ids = [(lane + at).astype(F32).astype(BF16) for at in range(0, DST_BLOCK, LANES)]
    one, zero = jnp.ones((), BF16), jnp.zeros((), BF16)

    def step(it, carry):
        work = []
        for u in range(UNROLL):
            b, c = plan_ref[0, it * UNROLL + u], plan_ref[1, it * UNROLL + u]
            src_row = jnp.right_shift(key_ref[pl.ds(c, 1), :] - b * BUCKET, DST_BLOCK.bit_length() - 1)
            src_row = jnp.where((src_row >= 0) & (src_row < SRC_BLOCK), src_row, 512).astype(F32)
            w_row = w_ref[pl.ds(c, 1), :]
            lhs = []
            for r in range(0, CHUNK, LANES):
                src, weight = src_row[:, r:r + LANES].astype(BF16), w_row[:, r:r + LANES]
                hit = src_ids == jnp.broadcast_to(src, src_ids.shape)
                lhs.append(jnp.concatenate(
                    [jnp.where(hit, jnp.broadcast_to(p, src_ids.shape), zero) for p in split3(weight)], axis=0))
            dst = jnp.take_along_axis(column_ref[...], jnp.broadcast_to(c, lane.shape), axis=1).astype(BF16)
            rhs = [jnp.where(dst == ids, one, zero) for ids in dst_ids]
            work.append((jnp.concatenate(lhs, axis=1), jnp.concatenate(rhs, axis=1)))
        outs = [dot(lhs, rhs) for lhs, rhs in work]
        total = cum_ref[it * UNROLL]
        for u, out in enumerate(outs):
            same = jnp.broadcast_to(plan_ref[2, it * UNROLL + u], (1, DST_BLOCK)) > 0
            out = out[2 * SRC_BLOCK:] + out[SRC_BLOCK:2 * SRC_BLOCK] + out[:SRC_BLOCK]
            total = out + jnp.where(same, total, 0.0)
            cum_ref[it * UNROLL + u + 1] = total
        return carry

    lax.fori_loop(low, high, step, 0)


def rows_to_blocks(a, groups):
    return a.reshape(groups, a.shape[0] // groups, a.shape[1])


def main_kernel(groups, own, halo, hubs, dst_ref, src_ref, w_in_ref, xt_ref, dyt_ref, send_ref, hub_ref, b1_ref, w1_ref, w2t_ref,
                dxt_ref, gw_ref, bias_ref,
                sx, sd, hx, hd, s1, s2, s3, s4, s5, s6, s7, s8,
                rx, rd, gx, gd, r1, r2, r3, r4, r5, r6, r7,
                list_ref, plan_ref, raw_ref, sort_k, sort_w, key_ref, w_ref, column_ref, cum_ref, hi_ref, mid_ref, low_ref, hubrow_ref, pt_ref, g2_ref, g1_ref, dy_ref, zt_ref, plan_sem, *sems):
    count = len(sems) // 2
    snd, rcv = sems[:count], sems[count:]
    adj = (hi_ref, mid_ref, low_ref)
    per = hubs // groups
    hid = b1_ref.shape[1]
    feat_in = xt_ref.shape[0]
    first_hub = own + halo
    slots, dsts = own + halo + hubs, own + hubs
    tops = dsts // DST_BLOCK
    me = lax.axis_index("graph")
    barrier = greet_all(groups, me)
    steps = (cum_ref.shape[0] - 1) // UNROLL
    middle = steps // 2
    cum_ref[0] = jnp.zeros((SRC_BLOCK, DST_BLOCK), F32)
    dst, src = dst_ref[...], src_ref[...]
    bucket = jnp.right_shift(src, SRC_BLOCK.bit_length() - 1) * tops + jnp.right_shift(dst, DST_BLOCK.bit_length() - 1)
    raw_ref[...] = (
        bucket * BUCKET + jnp.bitwise_and(src, SRC_BLOCK - 1) * DST_BLOCK + jnp.bitwise_and(dst, DST_BLOCK - 1))
    list_pairs(slots // SRC_BLOCK * tops, raw_ref, list_ref)
    plan = pltpu.make_async_copy(list_ref, plan_ref, plan_sem)
    plan.start()

    lane = lax.broadcasted_iota(jnp.int32, (1, LANES), 1)
    half = lane < LANES // 2
    own_row = lax.broadcasted_iota(jnp.int32, (own, 1), 0)
    pick_t = (own_row == send_ref[...]).astype(F32).astype(BF16)
    sel_f = (own_row == hub_ref[...] - me * own).astype(F32)
    sel_t = sel_f.astype(BF16)
    plain = jnp.sum(sel_f, axis=1, keepdims=True) == 0
    number = lax.broadcasted_iota(jnp.int32, (1, hubs), 1) + 1
    numbers = jnp.broadcast_to(number.astype(F32), (8, hubs)).astype(BF16)
    code_row = dot(numbers, sel_t, 1, 1)[:1]
    plain_row = code_row == 0
    xt = padded(xt_ref, LANES, own)
    feature = lax.broadcasted_iota(jnp.int32, (LANES, 1), 0)
    xt = jnp.where(feature == feat_in, code_row, xt.astype(F32)).astype(BF16)
    dyt = padded(dyt_ref, LANES, own)
    picked = dot(jnp.concatenate((xt,) + split3(dyt), axis=0), jnp.concatenate([pick_t, sel_t], axis=1))
    hub_dt = picked[3 * LANES:, halo:] + picked[2 * LANES:3 * LANES, halo:] + picked[LANES:2 * LANES, halo:]
    sx[:, :per, :] = rows_to_blocks(picked[:LANES, :halo].T, groups).astype(BF16)
    sx[:, per:, :] = rows_to_blocks(picked[:LANES, halo:].T, groups).astype(BF16)
    sd[...] = rows_to_blocks(hub_dt.T, groups)
    phases = raw_ref.size.bit_length() - 1
    sort_k[...], sort_w[...] = bitonic(
        raw_ref[...].reshape(sort_k.shape), w_in_ref[...].reshape(sort_w.shape), 1, phases - 4)
    pl.semaphore_wait(barrier, groups - 1)
    send_all(groups, me, [("a", sx, rx, snd[0], rcv[0]), ("a", sd, rd, snd[1], rcv[1])])

    w1 = padded(w1_ref, LANES, hid)
    w1_t = w1.astype(F32).T.astype(BF16)
    zt_ref[:, :own] = jnp.where(plain_row, dot(w1_t, xt), 0.0).astype(BF16)
    dy = dyt.T
    keys, weights = bitonic(sort_k[...], sort_w[...], phases - 3, phases)
    keys = keys.reshape(raw_ref.shape)
    column_ref[...] = jnp.bitwise_and(keys, DST_BLOCK - 1).astype(F32)
    key_ref[...] = keys.T
    w_ref[...] = weights.reshape(raw_ref.shape).T
    plan.wait()
    add_pairs(plan_ref, key_ref, w_ref, column_ref, cum_ref, 0, middle)
    wait_all(groups, rx, rcv[0], True)
    wait_all(groups, rd, rcv[1], True)
    got = rx[...].astype(F32)
    home_x = got[:, per:, :].sum(axis=0)
    hx[...] = home_x.astype(BF16)
    hd[...] = rd[...].sum(axis=0)
    send_all(groups, me, [("b", hx, gx, snd[2], rcv[2]), ("b", hd, gd, snd[3], rcv[3])])

    home_x = jnp.concatenate([home_x, jnp.zeros((8 - per, LANES), F32)], axis=0).astype(BF16)
    add_pairs(plan_ref, key_ref, w_ref, column_ref, cum_ref, middle, steps)

    group = LANES // SRC_BLOCK

    def renamed(i):
        cell = [
            jnp.concatenate([cum_ref[plan_ref[3, (i * group + g) * tops + j]] for g in range(group)], axis=0)
            for j in range(tops)]
        mine = jnp.concatenate(cell[:own // DST_BLOCK], axis=1)
        pieces = split3(mine)
        return mine, pieces, jnp.concatenate(cell[own // DST_BLOCK:], axis=1) + exact3_right(pieces, sel_t)

    def rename(i, carry):
        _, pieces, hub = renamed(i)
        rows = pl.ds(pl.multiple_of(i * LANES, LANES), LANES)
        for ref, left, right in zip(adj, pieces, split3(hub)):
            ref[rows, :own] = left
            ref[rows, own:] = right
        return carry

    def rename_hub(i, carry):
        mine, _, hub = renamed(first_hub // LANES + i)
        rows = pl.ds(pl.multiple_of(i * LANES, LANES), LANES)
        hubrow_ref[rows, :own] = mine
        hubrow_ref[rows, own:] = hub
        return carry

    lax.fori_loop(0, first_hub // LANES, rename, 0)
    lax.fori_loop(0, hubs // LANES, rename_hub, 0)
    halo_x = got[:, :per, :].reshape(halo, LANES).astype(BF16)
    column = jnp.broadcast_to(jnp.where(lane == feat_in, 1.0, 0.0), (8, LANES)).astype(BF16)
    halo_row = dot(column, halo_x, 1, 1)[:1].astype(jnp.int32)
    zt_ref[:, own:first_hub] = jnp.where(halo_row == 0, dot(w1_t, halo_x, 1, 1), 0.0).astype(BF16)
    halo_sel = (lax.broadcasted_iota(jnp.int32, (hubs, 1), 0) + 1 == halo_row).astype(F32)
    moved = jnp.concatenate([sel_f.T, halo_sel], axis=1).astype(BF16)
    for j in range(tops):
        cols = slice(j * DST_BLOCK, (j + 1) * DST_BLOCK)
        new = hubrow_ref[:, cols] + exact3(moved, [a[:first_hub, cols] for a in adj])
        for a, piece in zip(adj, split3(new)):
            a[first_hub:, cols] = piece

    def forward(rows, cols):
        zt = zt_ref[:, rows]
        return dot(zt, low_ref[rows, cols]) + dot(zt, mid_ref[rows, cols]) + dot(zt, hi_ref[rows, cols])

    def pack(d):
        dh, dm, dl = split3(d)
        d_two = (dh.astype(F32) + pltpu.roll(dm.astype(F32), LANES // 2, 1)).astype(BF16)
        return jnp.concatenate([d_two, dl], axis=1), d_two, dh

    def grad_out_sums(rows, cols, packed):
        a = dot(hi_ref[rows, cols], packed[0])
        t = a[:, :LANES] + a[:, LANES:] + dot(mid_ref[rows, cols], packed[1]) + dot(low_ref[rows, cols], packed[2])
        return jnp.where(half, t + pltpu.roll(t, LANES // 2, 1), 0.0)

    own_cols, hub_cols = slice(0, own), slice(own, dsts)
    pt_ref[...] = forward(slice(0, first_hub), hub_cols)
    d_own = pack(jnp.where(plain, dy, 0.0))
    g2_ref[...] = grad_out_sums(slice(own, slots), own_cols, d_own)
    wait_all(groups, gx, rcv[2], True)
    wait_all(groups, gd, rcv[3], True)
    hub_x = gx[...].astype(F32).reshape(hubs, LANES).astype(BF16)
    zt_ref[:, first_hub:] = dot(w1_t, hub_x, 1, 1).astype(BF16)
    d_hub = pack(gd[...].reshape(hubs, LANES))
    hub_slots = slice(first_hub, slots)
    y_hub = (pt_ref[...] + forward(hub_slots, hub_cols)).T
    s1[:, :, LANES:] = rows_to_blocks(y_hub, groups)
    g2_halo = g2_ref[:halo, :] + grad_out_sums(slice(own, first_hub), hub_cols, d_hub)
    g2_hub = g2_ref[halo:, :] + grad_out_sums(hub_slots, hub_cols, d_hub)
    s1[:, :, :LANES] = rows_to_blocks(g2_halo + pltpu.roll(g2_hub, LANES // 2, 1), groups)
    send_all(groups, me, [("a", s1, r1, snd[4], rcv[4])])

    b1 = b1_ref[...]
    w2t = padded(w2t_ref, LANES, hid)
    pre = forward(slice(0, slots), own_cols).T + b1
    g2_own = grad_out_sums(slice(0, own), own_cols, d_own) + grad_out_sums(slice(0, own), hub_cols, d_hub)
    hidden = jnp.where(plain, jax.nn.relu(pre), 0.0).astype(BF16)
    live = plain & (pre > 0)
    wait_all(groups, r1, rcv[4], True)
    home = r1[...].sum(axis=0)
    pad = jnp.zeros((8 - per, LANES), F32)
    home_g = jnp.where(half, pltpu.roll(jnp.concatenate([home[:, :LANES], pad], axis=0), LANES // 2, 1), 0.0)
    home_pre = jnp.concatenate([home[:, LANES:] + b1, jnp.zeros((8 - per, hid), F32)], axis=0)
    home_dz2 = home_g.astype(BF16)
    home_dy = jnp.where(home_pre > 0, dot(home_dz2, w2t), 0.0)
    s2[...] = home_dy[:per]
    send_all(groups, me, [("b", s2, r2, snd[5], rcv[5])])

    back = jnp.where(half, r1[:, :, :LANES].reshape(halo, LANES), 0.0)
    dz2 = jnp.where(plain, g2_own + exact3(pick_t, split3(back)), 0.0).astype(BF16)
    dy1 = jnp.where(live, dot(dz2, w2t), 0.0)
    home_hidden = jax.nn.relu(home_pre).astype(BF16)
    gw2 = dot(dz2, hidden, 0, 0) + dot(home_dz2, home_hidden, 0, 0)
    s3[...] = rows_to_blocks(gw2, groups)
    s4[:, :hid] = dy1.sum(axis=0, keepdims=True) + home_dy.sum(axis=0, keepdims=True)
    s4[:, hid:] = dy.sum(axis=0, keepdims=True)
    send_all(groups, me, [("a", s3, r3, snd[6], rcv[6]), ("b", s4, r4, snd[7], rcv[7])])
    for p, piece in enumerate(split3(dy1)):
        dy_ref[p, :own, :] = piece
    chunk = 256

    def own_part(i, carry):
        rows = pl.ds(pl.multiple_of(i * chunk, chunk), chunk)
        g1_ref[rows, :] = full6([a[rows, :own] for a in adj], [dy_ref[p, :own, :] for p in range(3)])
        return carry

    lax.fori_loop(0, slots // chunk, own_part, 0)
    wait_all(groups, r2, rcv[5], True)
    for p, piece in enumerate(split3(r2[...].reshape(hubs, hid))):
        dy_ref[p, own:, :] = piece

    def hub_part(rows):
        return g1_ref[rows, :] + full6([a[rows, own:] for a in adj], [dy_ref[p, own:, :] for p in range(3)])

    s5[:, :per, :] = rows_to_blocks(hub_part(slice(own, first_hub)), groups)
    s5[:, per:, :] = rows_to_blocks(hub_part(hub_slots), groups)
    send_all(groups, me, [("a", s5, r5, snd[8], rcv[8])])

    g1_ref[:chunk, :] = hub_part(slice(0, chunk))
    g1_ref[chunk:own, :] = hub_part(slice(chunk, own))
    wait_all(groups, r3, rcv[6], True)
    wait_all(groups, r4, rcv[7], True)
    bias_ref[...] = r4[...].sum(axis=0)
    s8[:, hid:] = r3[...].sum(axis=0)
    wait_all(groups, r5, rcv[8], True)
    home_dz1 = jnp.concatenate([r5[:, per:, :].sum(axis=0), jnp.zeros((8 - per, hid), F32)], axis=0).astype(BF16)
    back = r5[:, :per, :].reshape(halo, hid)
    dz1 = g1_ref[:own, :] + exact3(pick_t, split3(back))
    dz1 = jnp.where(plain, dz1, 0.0).astype(BF16)
    gw1 = dot(xt, dz1) + dot(home_x, home_dz1, 0, 0)
    s6[...] = rows_to_blocks(gw1, groups)
    s7[...] = dot(home_dz1, w1, 1, 1)[:per]
    send_all(groups, me, [("a", s6, r6, snd[9], rcv[9]), ("b", s7, r7, snd[10], rcv[10])])

    dxt = dot(w1, dz1, 1, 1)
    wait_all(groups, r6, rcv[9], True)
    s8[:, :hid] = r6[...].sum(axis=0)
    send_all(groups, me, [("b", s8, gw_ref, snd[11], rcv[11])])

    wait_all(groups, r7, rcv[10], True)
    hub_dx = r7[...].reshape(hubs, LANES).T
    dxt_ref[...] = dxt + exact3_right(split3(hub_dx), sel_f.T.astype(BF16))
    for buf, sem in zip((rx, rd, gx, gd, r1, r2, r3, r4, r5, r6, r7, gw_ref), snd):
        wait_all(groups, buf, sem, False)
    wait_all(groups, gw_ref, rcv[11], True)


def main_call(groups, own, halo, hubs, *args):
    hid = args[7].shape[1]
    per = hubs // groups
    slots, dsts = own + halo + hubs, own + hubs
    edges = args[0].size
    pairs = edges // CHUNK + slots // SRC_BLOCK * (dsts // DST_BLOCK)
    vmem = pl.BlockSpec(memory_space=pltpu.VMEM)
    blocks = [
        ("a", (2 * per, LANES), BF16), ("a", (per, LANES), F32), ("b", (per, LANES), BF16), ("b", (per, LANES), F32),
        ("a", (per, LANES + hid), F32), ("b", (per, hid), F32), ("a", (1, hid), F32), ("b", (1, hid + LANES), F32),
        ("a", (2 * per, hid), F32), ("a", (1, hid), F32), ("b", (per, LANES), F32), ("b", (1, 2 * hid), F32)]
    sends = [pltpu.VMEM(((groups,) if k == "a" else ()) + b, t) for k, b, t in blocks]
    recvs = [pltpu.VMEM((groups,) + b, t) for _, b, t in blocks[:-1]]
    shape = jax.ShapeDtypeStruct
    return pl.pallas_call(
        functools.partial(main_kernel, groups, own, halo, hubs),
        out_shape=[shape((LANES, own), F32), shape((groups, 1, 2 * hid), F32), shape((1, hid + LANES), F32)],
        in_specs=[vmem] * len(args),
        out_specs=[vmem] * 3,
        scratch_shapes=sends + recvs + [
            pltpu.VMEM((8, 256), jnp.int32),
            pltpu.SMEM((8, 256), jnp.int32),
            pltpu.VMEM((edges // LANES, LANES), jnp.int32),
            pltpu.VMEM((edges // LANES // 8, 8, LANES), jnp.int32),
            pltpu.VMEM((edges // LANES // 8, 8, LANES), F32),
            pltpu.VMEM((edges // CHUNK, CHUNK), jnp.int32),
            pltpu.VMEM((edges // CHUNK, CHUNK), F32),
            pltpu.VMEM((edges // LANES, LANES), F32),
            pltpu.VMEM((pairs + 1, SRC_BLOCK, DST_BLOCK), F32),
            pltpu.VMEM((slots, dsts), BF16),
            pltpu.VMEM((slots, dsts), BF16),
            pltpu.VMEM((slots, dsts), BF16),
            pltpu.VMEM((hubs, dsts), F32),
            pltpu.VMEM((hid, hubs), F32),
            pltpu.VMEM((slots - own, LANES), F32),
            pltpu.VMEM((slots, hid), F32),
            pltpu.VMEM((3, dsts, hid), BF16),
            pltpu.VMEM((hid, slots), BF16),
        ] + [pltpu.SemaphoreType.DMA] * (1 + 2 * len(blocks)),
        compiler_params=pltpu.CompilerParams(collective_id=0, has_side_effects=True, vmem_limit_bytes=56 * 2 ** 20),
        name="main_exchange",
    )(*args)


def output_kernel(dxt_ref, gw_ref, bias_ref, dx_out, gw1_out, gw2_out, b1_out, b2_out):
    feat_in, feat_out, hid = dx_out.shape[0], gw2_out.shape[0], gw2_out.shape[1]
    dx_out[...] = dxt_ref[:feat_in, :]
    gw = gw_ref[...].reshape(gw_ref.shape[0], 2 * hid)
    gw1_out[...] = gw[:feat_in, :hid]
    gw2_out[...] = gw[:feat_out, hid:]
    b1_out[...] = bias_ref[:, :hid]
    b2_out[...] = bias_ref[:, hid:hid + feat_out]


def solution(mesh):
    groups = mesh.shape["graph"]

    def device_step(x, dst, src, w, send, hub_ids, w_first, b_first, w_second, dy):
        own, feat_in = x.shape
        feat_out = dy.shape[1]
        hid = w_first.shape[1]
        halo, hubs = send.shape[0], hub_ids.shape[0]
        edges = [v.reshape(-1, LANES) for v in (dst, src, w)]
        raw = main_call(
            groups, own, halo, hubs, *edges, x.T, dy.T, send[None, :], hub_ids[None, :], b_first[None, :],
            w_first, w_second.T)
        dx, gw1, gw2, gb1, gb2 = pl.pallas_call(
            output_kernel,
            out_shape=[jax.ShapeDtypeStruct(shape, F32) for shape in (
                (feat_in, own), (feat_in, hid), (feat_out, hid), (1, hid), (1, feat_out))],
            name="outputs",
        )(*raw)
        return dx.T, gw1, gw2.T, gb1[0], gb2[0]

    rows, flat = P(("data", "graph"), None), P(("data", "graph"))
    return jax.shard_map(
        device_step,
        mesh=mesh,
        in_specs=(rows, flat, flat, flat, flat, P("data"), P(), P(), P(), rows),
        out_specs=(rows, P("data", None), P("data", None), P("data"), P("data")),
        check_vma=False,
    )
```

```python
import functools

import jax
import jax.numpy as jnp
from jax import lax
from jax.experimental import pallas as pl
from jax.experimental.pallas import tpu as pltpu
from jax.sharding import PartitionSpec as P

BF16 = jnp.bfloat16
F32 = jnp.float32
HI = lax.Precision.HIGHEST
LANES = 128
MESH = pl.DeviceIdType.MESH


def dot(a, b, ca=1, cb=0, precision=None):
    return lax.dot_general(a, b, (((ca,), (cb,)), ((), ())), precision=precision, preferred_element_type=F32)


def split3(a):
    hi = a.astype(BF16)
    rest = a - hi.astype(F32)
    mid = rest.astype(BF16)
    return hi, mid, (rest - mid.astype(F32)).astype(BF16)


def exact3(sel, pieces, ca=1):
    return dot(sel, pieces[2], ca) + dot(sel, pieces[1], ca) + dot(sel, pieces[0], ca)


def exact3_right(pieces, sel):
    return dot(pieces[2], sel) + dot(pieces[1], sel) + dot(pieces[0], sel)


def full6(a, b):
    low = dot(a[0], b[2]) + dot(a[2], b[0]) + dot(a[1], b[1])
    return low + (dot(a[0], b[1]) + dot(a[1], b[0])) + dot(a[0], b[0])


def partner(groups, me, i):
    low = sum(2 << k for k in range(0, groups.bit_length() - 2, 2))
    t = jnp.bitwise_xor(i - 1, 2 * low + 1)
    high = jnp.bitwise_and(jnp.right_shift(t, 1), low)
    return jnp.bitwise_xor(me, jnp.bitwise_xor(t, jnp.bitwise_xor(high, low)))


def wait_all(groups, buf, sem, whole):
    part = buf if whole else buf.at[pl.ds(0, groups - 1)]
    pltpu.make_async_copy(part, part, sem).wait()


def send_all(groups, me, items):
    def send(i, carry):
        peer = partner(groups, me, i)
        for kind, src, dst, send_sem, recv_sem in items:
            pltpu.make_async_remote_copy(
                src_ref=src.at[peer] if kind == "a" else src,
                dst_ref=dst.at[me],
                send_sem=send_sem,
                recv_sem=recv_sem,
                device_id=(0, peer),
                device_id_type=MESH,
            ).start()
        return carry

    lax.fori_loop(1, groups, send, 0)
    for kind, src, dst, _, recv_sem in items:
        pltpu.make_async_copy(src.at[me] if kind == "a" else src, dst.at[me], recv_sem).start()


def greet_all(groups, me):
    barrier = pltpu.get_barrier_semaphore()

    def greet(i, carry):
        pl.semaphore_signal(barrier, inc=1, device_id=(0, partner(groups, me, i)), device_id_type=MESH)
        return carry

    lax.fori_loop(1, groups, greet, 0)
    return barrier


def padded(ref, rows, cols):
    a = ref[...]
    if cols > a.shape[1]:
        a = jnp.concatenate([a, jnp.zeros((a.shape[0], cols - a.shape[1]), a.dtype)], axis=1)
    if rows > a.shape[0]:
        a = jnp.concatenate([a, jnp.zeros((rows - a.shape[0], cols), a.dtype)], axis=0)
    return a


SRC_BLOCK, DST_BLOCK = 64, 256
BUCKET = SRC_BLOCK * DST_BLOCK
CHUNK, UNROLL = 256, 44


def bitonic(keys, weights, low, high):
    vregs = keys.shape[0]
    base = vregs.bit_length() - 1

    def bit(shape, m):
        axis, m = (len(shape) - 2, m - base) if m < base + 3 else (len(shape) - 1, m - base - 3)
        return jnp.bitwise_and(jnp.right_shift(lax.broadcasted_iota(jnp.int32, shape, axis), m), 1)

    def other(a, j):
        if j >= base + 3:
            lane = lax.broadcasted_iota(jnp.int32, (vregs * 8, LANES), 1)
            return jnp.take_along_axis(
                a.reshape(vregs * 8, LANES), jnp.bitwise_xor(lane, 1 << (j - base - 3)), axis=1).reshape(a.shape)
        step = 1 << (j - base)
        if step == 4:
            return pltpu.roll(a, 4, 1)
        return jnp.where(bit(a.shape, j) > 0, pltpu.roll(a, step, 1), pltpu.roll(a, 8 - step, 1))

    full = keys.shape
    for k in range(low, high + 1):
        for j in range(k - 1, -1, -1):
            if j < base:
                near = 1 << j
                parts = (vregs // (2 * near), 2, near, 8, LANES)
                a, b = keys.reshape(parts)[:, 0], keys.reshape(parts)[:, 1]
                wa, wb = weights.reshape(parts)[:, 0], weights.reshape(parts)[:, 1]
                swap = a > b
                if k < base:
                    block = lax.broadcasted_iota(jnp.int32, a.shape, 0)
                    swap = jnp.logical_xor(swap, jnp.bitwise_and(jnp.right_shift(block, k - j - 1), 1) > 0)
                elif k < base + 10:
                    swap = jnp.logical_xor(swap, bit(a.shape, k) > 0)
                keys = jnp.stack([jnp.where(swap, b, a), jnp.where(swap, a, b)], axis=1).reshape(full)
                weights = jnp.stack([jnp.where(swap, wb, wa), jnp.where(swap, wa, wb)], axis=1).reshape(full)
            else:
                keys2, weights2 = other(keys, j), other(weights, j)
                upper = bit(full, j)
                if k < base + 10:
                    upper = jnp.bitwise_xor(upper, bit(full, k))
                take = jnp.bitwise_xor(keys2, -upper) < jnp.bitwise_xor(keys, -upper)
                keys = jnp.where(take, keys2, keys)
                weights = jnp.where(take, weights2, weights)
    return keys, weights


def ring_sum(a, axis):
    step = a.shape[axis] // 2
    while step:
        a = a + pltpu.roll(a, step, axis)
        step //= 2
    return a


def list_pairs(buckets, key_ref, plan_ref):
    size = CHUNK
    shift = size.bit_length() - 1
    total = 1 << buckets.bit_length()

    def count(at, i, carry):
        bucket = jnp.right_shift(key_ref[pl.ds(pl.multiple_of(i * 8, 8), 8), :], BUCKET.bit_length() - 1)
        return tuple(c + jnp.where(bucket <= at + b, 1, 0) for b, c in enumerate(carry))

    counts = ()
    for at in range(0, buckets, 24):
        zeros = (jnp.zeros((8, LANES), jnp.int32),) * min(24, buckets - at)
        counts += lax.fori_loop(0, key_ref.shape[0] // 8, functools.partial(count, at), zeros)
    counts = [ring_sum(c, 0)[:1] for c in counts]
    none = jnp.zeros((1, LANES), jnp.int32)
    counts = [none] + counts + [counts[-1]] * (total - buckets)
    low = ring_sum(jnp.concatenate(counts[:total], axis=0), 1)
    high = ring_sum(jnp.concatenate(counts[1:], axis=0), 1)
    start = jnp.right_shift(low, shift)
    pairs = jnp.where(high > low, jnp.right_shift(high + size - 1, shift) - start, 0)
    row = lax.broadcasted_iota(jnp.int32, (total, LANES), 0)
    last, step = pairs, 1
    while step < total:
        last = last + jnp.where(row >= step, pltpu.roll(last, step, 0), 0)
        step *= 2
    first = last - pairs
    for half in range(plan_ref.shape[1] // LANES):
        at = lax.broadcasted_iota(jnp.int32, (total, LANES), 1) + half * LANES
        inside = (first <= at) & (at < last)
        rows = [
            jnp.where(last <= at, 1, 0), jnp.where(inside, start + at - first, 0), jnp.where(inside & (at > first), 1, 0),
            jnp.where((row == at) & (pairs > 0), last, 0)]
        rows = [ring_sum(r, 0)[:1] for r in rows] + [none] * 4
        plan_ref[:, half * LANES:(half + 1) * LANES] = jnp.concatenate(rows, axis=0)


def add_pairs(plan_ref, key_ref, w_ref, column_ref, cum_ref, low, high):
    src_ids = lax.broadcasted_iota(jnp.int32, (SRC_BLOCK, LANES), 0).astype(F32).astype(BF16)
    lane = lax.broadcasted_iota(jnp.int32, (CHUNK, LANES), 1)
    dst_ids = [(lane + at).astype(F32).astype(BF16) for at in range(0, DST_BLOCK, LANES)]
    one, zero = jnp.ones((), BF16), jnp.zeros((), BF16)

    def step(it, carry):
        work = []
        for u in range(UNROLL):
            b, c = plan_ref[0, it * UNROLL + u], plan_ref[1, it * UNROLL + u]
            src_row = jnp.right_shift(key_ref[pl.ds(c, 1), :] - b * BUCKET, DST_BLOCK.bit_length() - 1)
            src_row = jnp.where((src_row >= 0) & (src_row < SRC_BLOCK), src_row, 512).astype(F32)
            w_row = w_ref[pl.ds(c, 1), :]
            lhs = []
            for r in range(0, CHUNK, LANES):
                src, weight = src_row[:, r:r + LANES].astype(BF16), w_row[:, r:r + LANES]
                hit = src_ids == jnp.broadcast_to(src, src_ids.shape)
                lhs.append(jnp.concatenate(
                    [jnp.where(hit, jnp.broadcast_to(p, src_ids.shape), zero) for p in split3(weight)], axis=0))
            dst = jnp.take_along_axis(column_ref[...], jnp.broadcast_to(c, lane.shape), axis=1).astype(BF16)
            rhs = [jnp.where(dst == ids, one, zero) for ids in dst_ids]
            work.append((jnp.concatenate(lhs, axis=1), jnp.concatenate(rhs, axis=1)))
        outs = [dot(lhs, rhs) for lhs, rhs in work]
        total = cum_ref[it * UNROLL]
        for u, out in enumerate(outs):
            same = jnp.broadcast_to(plan_ref[2, it * UNROLL + u], (1, DST_BLOCK)) > 0
            out = out[2 * SRC_BLOCK:] + out[SRC_BLOCK:2 * SRC_BLOCK] + out[:SRC_BLOCK]
            total = out + jnp.where(same, total, 0.0)
            cum_ref[it * UNROLL + u + 1] = total
        return carry

    lax.fori_loop(low, high, step, 0)


def rows_to_blocks(a, groups):
    return a.reshape(groups, a.shape[0] // groups, a.shape[1])


def main_kernel(groups, own, halo, hubs, dst_ref, src_ref, w_in_ref, xt_ref, dyt_ref, send_ref, hub_ref, b1_ref, w1_ref, w2t_ref,
                dxt_ref, gw1_ref, gw2_ref, bias_ref,
                sx, sd, hx, hd, s1, s2, s3, s4, s5, s6, s7, s8, s9,
                rx, rd, gx, gd, r1, r2, r3, r4, r5, r6, r7,
                list_ref, plan_ref, raw_ref, sort_k, sort_w, key_ref, w_ref, column_ref, cum_ref, hi_ref, mid_ref, low_ref, hubrow_ref, pt_ref, g2_ref, g1_ref, dy_ref, zt_ref, plan_sem, *sems):
    count = len(sems) // 2
    snd, rcv = sems[:count], sems[count:]
    adj = (hi_ref, mid_ref, low_ref)
    per = hubs // groups
    hid = b1_ref.shape[1]
    feat_in = xt_ref.shape[0]
    first_hub = own + halo
    slots, dsts = own + halo + hubs, own + hubs
    tops = dsts // DST_BLOCK
    me = lax.axis_index("graph")
    barrier = greet_all(groups, me)
    steps = (cum_ref.shape[0] - 1) // UNROLL
    middle = steps // 2
    cum_ref[0] = jnp.zeros((SRC_BLOCK, DST_BLOCK), F32)
    dst, src = dst_ref[...], src_ref[...]
    bucket = jnp.right_shift(src, SRC_BLOCK.bit_length() - 1) * tops + jnp.right_shift(dst, DST_BLOCK.bit_length() - 1)
    raw_ref[...] = (
        bucket * BUCKET + jnp.bitwise_and(src, SRC_BLOCK - 1) * DST_BLOCK + jnp.bitwise_and(dst, DST_BLOCK - 1))
    list_pairs(slots // SRC_BLOCK * tops, raw_ref, list_ref)
    plan = pltpu.make_async_copy(list_ref, plan_ref, plan_sem)
    plan.start()

    lane = lax.broadcasted_iota(jnp.int32, (1, LANES), 1)
    half = lane < LANES // 2
    own_row = lax.broadcasted_iota(jnp.int32, (own, 1), 0)
    pick_t = (own_row == send_ref[...]).astype(F32).astype(BF16)
    sel_f = (own_row == hub_ref[...] - me * own).astype(F32)
    sel_t = sel_f.astype(BF16)
    plain = jnp.sum(sel_f, axis=1, keepdims=True) == 0
    number = lax.broadcasted_iota(jnp.int32, (1, hubs), 1) + 1
    numbers = jnp.broadcast_to(number.astype(F32), (8, hubs)).astype(BF16)
    code_row = dot(numbers, sel_t, 1, 1)[:1]
    plain_row = code_row == 0
    xt = padded(xt_ref, LANES, own)
    feature = lax.broadcasted_iota(jnp.int32, (LANES, 1), 0)
    xt = jnp.where(feature == feat_in, code_row, xt.astype(F32)).astype(BF16)
    dyt = padded(dyt_ref, LANES, own)
    picked = dot(jnp.concatenate((xt,) + split3(dyt), axis=0), jnp.concatenate([pick_t, sel_t], axis=1))
    hub_dt = picked[3 * LANES:, halo:] + picked[2 * LANES:3 * LANES, halo:] + picked[LANES:2 * LANES, halo:]
    sx[:, :per, :] = rows_to_blocks(picked[:LANES, :halo].T, groups).astype(BF16)
    sx[:, per:, :] = rows_to_blocks(picked[:LANES, halo:].T, groups).astype(BF16)
    hub_d = rows_to_blocks(hub_dt.T, groups)
    sd[...] = hub_d[:, :1, :] + pltpu.roll(hub_d[:, 1:, :], LANES // 2, 2)
    phases = raw_ref.size.bit_length() - 1
    sort_k[...], sort_w[...] = bitonic(
        raw_ref[...].reshape(sort_k.shape), w_in_ref[...].reshape(sort_w.shape), 1, phases - 4)
    pl.semaphore_wait(barrier, groups - 1)
    send_all(groups, me, [("a", sx, rx, snd[0], rcv[0]), ("a", sd, rd, snd[1], rcv[1])])

    w1 = padded(w1_ref, LANES, hid)
    w1_t = w1.astype(F32).T.astype(BF16)
    zt_ref[:, :own] = jnp.where(plain_row, dot(w1_t, xt), 0.0).astype(BF16)
    dy = dyt.T
    keys, weights = bitonic(sort_k[...], sort_w[...], phases - 3, phases)
    keys = keys.reshape(raw_ref.shape)
    column_ref[...] = jnp.bitwise_and(keys, DST_BLOCK - 1).astype(F32)
    key_ref[...] = keys.T
    w_ref[...] = weights.reshape(raw_ref.shape).T
    plan.wait()
    add_pairs(plan_ref, key_ref, w_ref, column_ref, cum_ref, 0, middle)
    wait_all(groups, rx, rcv[0], True)
    wait_all(groups, rd, rcv[1], True)
    got = rx[...].astype(F32)
    home_x = got[:, per:, :].sum(axis=0)
    hx[...] = home_x.astype(BF16)
    hd[...] = rd[...].sum(axis=0)
    send_all(groups, me, [("b", hx, gx, snd[2], rcv[2]), ("b", hd, gd, snd[3], rcv[3])])

    home_x = jnp.concatenate([home_x, jnp.zeros((8 - per, LANES), F32)], axis=0).astype(BF16)
    add_pairs(plan_ref, key_ref, w_ref, column_ref, cum_ref, middle, steps)

    group = LANES // SRC_BLOCK

    def renamed(i):
        cell = [
            jnp.concatenate([cum_ref[plan_ref[3, (i * group + g) * tops + j]] for g in range(group)], axis=0)
            for j in range(tops)]
        mine = jnp.concatenate(cell[:own // DST_BLOCK], axis=1)
        pieces = split3(mine)
        return mine, pieces, jnp.concatenate(cell[own // DST_BLOCK:], axis=1) + exact3_right(pieces, sel_t)

    def rename(i, carry):
        _, pieces, hub = renamed(i)
        rows = pl.ds(pl.multiple_of(i * LANES, LANES), LANES)
        for ref, left, right in zip(adj, pieces, split3(hub)):
            ref[rows, :own] = left
            ref[rows, own:] = right
        return carry

    def rename_hub(i, carry):
        mine, _, hub = renamed(first_hub // LANES + i)
        rows = pl.ds(pl.multiple_of(i * LANES, LANES), LANES)
        hubrow_ref[rows, :own] = mine
        hubrow_ref[rows, own:] = hub
        return carry

    lax.fori_loop(0, first_hub // LANES, rename, 0)
    lax.fori_loop(0, hubs // LANES, rename_hub, 0)
    halo_x = got[:, :per, :].reshape(halo, LANES).astype(BF16)
    column = jnp.broadcast_to(jnp.where(lane == feat_in, 1.0, 0.0), (8, LANES)).astype(BF16)
    halo_row = dot(column, halo_x, 1, 1)[:1].astype(jnp.int32)
    zt_ref[:, own:first_hub] = jnp.where(halo_row == 0, dot(w1_t, halo_x, 1, 1), 0.0).astype(BF16)
    halo_sel = (lax.broadcasted_iota(jnp.int32, (hubs, 1), 0) + 1 == halo_row).astype(F32)
    moved = jnp.concatenate([sel_f.T, halo_sel], axis=1).astype(BF16)
    for j in range(tops):
        cols = slice(j * DST_BLOCK, (j + 1) * DST_BLOCK)
        new = hubrow_ref[:, cols] + exact3(moved, [a[:first_hub, cols] for a in adj])
        for a, piece in zip(adj, split3(new)):
            a[first_hub:, cols] = piece

    def forward(rows, cols):
        zt = zt_ref[:, rows]
        return dot(zt, low_ref[rows, cols]) + dot(zt, mid_ref[rows, cols]) + dot(zt, hi_ref[rows, cols])

    def pack(d):
        dh, dm, dl = split3(d)
        d_two = (dh.astype(F32) + pltpu.roll(dm.astype(F32), LANES // 2, 1)).astype(BF16)
        return jnp.concatenate([d_two, dl], axis=1), d_two, dh

    def grad_out_sums(rows, cols, packed):
        a = dot(hi_ref[rows, cols], packed[0])
        t = a[:, :LANES] + a[:, LANES:] + dot(mid_ref[rows, cols], packed[1]) + dot(low_ref[rows, cols], packed[2])
        return jnp.where(half, t + pltpu.roll(t, LANES // 2, 1), 0.0)

    own_cols, hub_cols = slice(0, own), slice(own, dsts)
    pt_ref[...] = forward(slice(0, first_hub), hub_cols)
    d_own = pack(jnp.where(plain, dy, 0.0))
    g2_ref[...] = grad_out_sums(slice(own, slots), own_cols, d_own)
    wait_all(groups, gx, rcv[2], True)
    wait_all(groups, gd, rcv[3], True)
    hub_x = gx[...].astype(F32).reshape(hubs, LANES).astype(BF16)
    zt_ref[:, first_hub:] = dot(w1_t, hub_x, 1, 1).astype(BF16)
    hub_d = gd[...].reshape(groups, LANES)
    hub_d = jnp.stack([jnp.where(half, hub_d, 0.0), jnp.where(half, pltpu.roll(hub_d, LANES // 2, 1), 0.0)], axis=1)
    d_hub = pack(hub_d.reshape(hubs, LANES))
    hub_slots = slice(first_hub, slots)
    y_hub = (pt_ref[...] + forward(hub_slots, hub_cols)).T
    s1[:, :, LANES:] = rows_to_blocks(y_hub, groups)
    g2_halo = g2_ref[:halo, :] + grad_out_sums(slice(own, first_hub), hub_cols, d_hub)
    g2_hub = g2_ref[halo:, :] + grad_out_sums(hub_slots, hub_cols, d_hub)
    s1[:, :, :LANES] = rows_to_blocks(g2_halo + pltpu.roll(g2_hub, LANES // 2, 1), groups)
    send_all(groups, me, [("a", s1, r1, snd[4], rcv[4])])

    b1 = b1_ref[...]
    w2t = padded(w2t_ref, LANES, hid)
    pre = forward(slice(0, slots), own_cols).T + b1
    g2_own = grad_out_sums(slice(0, own), own_cols, d_own) + grad_out_sums(slice(0, own), hub_cols, d_hub)
    hidden = jnp.where(plain, jax.nn.relu(pre), 0.0).astype(BF16)
    live = plain & (pre > 0)
    wait_all(groups, r1, rcv[4], True)
    home = r1[...].sum(axis=0)
    pad = jnp.zeros((8 - per, LANES), F32)
    home_g = jnp.where(half, pltpu.roll(jnp.concatenate([home[:, :LANES], pad], axis=0), LANES // 2, 1), 0.0)
    home_pre = jnp.concatenate([home[:, LANES:] + b1, jnp.zeros((8 - per, hid), F32)], axis=0)
    home_dz2 = home_g.astype(BF16)
    home_dy = jnp.where(home_pre > 0, dot(home_dz2, w2t), 0.0)
    s2[...] = home_dy[:per]
    send_all(groups, me, [("b", s2, r2, snd[5], rcv[5])])

    back = jnp.where(half, r1[:, :, :LANES].reshape(halo, LANES), 0.0)
    dz2 = jnp.where(plain, g2_own + exact3(pick_t, split3(back)), 0.0).astype(BF16)
    dy1 = jnp.where(live, dot(dz2, w2t), 0.0)
    home_hidden = jax.nn.relu(home_pre).astype(BF16)
    gw2 = dot(dz2, hidden, 0, 0) + dot(home_dz2, home_hidden, 0, 0)
    s3[...] = rows_to_blocks(gw2, groups)
    s4[:, :hid] = dy1.sum(axis=0, keepdims=True) + home_dy.sum(axis=0, keepdims=True)
    s4[:, hid:] = dy.sum(axis=0, keepdims=True)
    send_all(groups, me, [("a", s3, r3, snd[6], rcv[6]), ("b", s4, r4, snd[7], rcv[7])])
    for p, piece in enumerate(split3(dy1)):
        dy_ref[p, :own, :] = piece
    chunk = 256

    def own_part(i, carry):
        rows = pl.ds(pl.multiple_of(i * chunk, chunk), chunk)
        g1_ref[rows, :] = full6([a[rows, :own] for a in adj], [dy_ref[p, :own, :] for p in range(3)])
        return carry

    lax.fori_loop(0, slots // chunk, own_part, 0)
    wait_all(groups, r2, rcv[5], True)
    for p, piece in enumerate(split3(r2[...].reshape(hubs, hid))):
        dy_ref[p, own:, :] = piece

    def hub_part(rows):
        return g1_ref[rows, :] + full6([a[rows, own:] for a in adj], [dy_ref[p, own:, :] for p in range(3)])

    s5[:, :per, :] = rows_to_blocks(hub_part(slice(own, first_hub)), groups)
    s5[:, per:, :] = rows_to_blocks(hub_part(hub_slots), groups)
    send_all(groups, me, [("a", s5, r5, snd[8], rcv[8])])

    g1_ref[:chunk, :] = hub_part(slice(0, chunk))
    g1_ref[chunk:own, :] = hub_part(slice(chunk, own))
    wait_all(groups, r3, rcv[6], True)
    wait_all(groups, r4, rcv[7], True)
    bias_ref[...] = r4[...].sum(axis=0)
    s9[...] = r3[...].sum(axis=0)
    send_all(groups, me, [("b", s9, gw2_ref, snd[12], rcv[12])])
    wait_all(groups, r5, rcv[8], True)
    home_dz1 = jnp.concatenate([r5[:, per:, :].sum(axis=0), jnp.zeros((8 - per, hid), F32)], axis=0).astype(BF16)
    back = r5[:, :per, :].reshape(halo, hid)
    dz1 = g1_ref[:own, :] + exact3(pick_t, split3(back))
    dz1 = jnp.where(plain, dz1, 0.0).astype(BF16)
    gw1 = dot(xt, dz1) + dot(home_x, home_dz1, 0, 0)
    s6[...] = rows_to_blocks(gw1, groups)
    send_all(groups, me, [("a", s6, r6, snd[9], rcv[9])])

    s7[...] = dot(home_dz1, w1, 1, 1)[:per]
    send_all(groups, me, [("b", s7, r7, snd[10], rcv[10])])
    dxt = dot(w1, dz1, 1, 1)
    wait_all(groups, r6, rcv[9], True)
    s8[...] = r6[...].sum(axis=0)
    send_all(groups, me, [("b", s8, gw1_ref, snd[11], rcv[11])])

    wait_all(groups, r7, rcv[10], True)
    hub_dx = r7[...].reshape(hubs, LANES).T
    dxt_ref[...] = dxt + exact3_right(split3(hub_dx), sel_f.T.astype(BF16))
    wait_all(groups, gw2_ref, rcv[12], True)
    for buf, sem in zip((rx, rd, gx, gd, r1, r2, r3, r4, r5, r6, r7, gw1_ref, gw2_ref), snd):
        wait_all(groups, buf, sem, False)
    wait_all(groups, gw1_ref, rcv[11], True)


def main_call(groups, own, halo, hubs, *args):
    hid = args[7].shape[1]
    per = hubs // groups
    slots, dsts = own + halo + hubs, own + hubs
    edges = args[0].size
    pairs = edges // CHUNK + slots // SRC_BLOCK * (dsts // DST_BLOCK)
    vmem = pl.BlockSpec(memory_space=pltpu.VMEM)
    blocks = [
        ("a", (2 * per, LANES), BF16), ("a", (1, LANES), F32), ("b", (per, LANES), BF16), ("b", (1, LANES), F32),
        ("a", (per, LANES + hid), F32), ("b", (per, hid), F32), ("a", (1, hid), F32), ("b", (1, hid + LANES), F32),
        ("a", (2 * per, hid), F32), ("a", (1, hid), F32), ("b", (per, LANES), F32), ("b", (1, hid), F32), ("b", (1, hid), F32)]
    sends = [pltpu.VMEM(((groups,) if k == "a" else ()) + b, t) for k, b, t in blocks]
    recvs = [pltpu.VMEM((groups,) + b, t) for _, b, t in blocks[:-2]]
    shape = jax.ShapeDtypeStruct
    return pl.pallas_call(
        functools.partial(main_kernel, groups, own, halo, hubs),
        out_shape=[
            shape((LANES, own), F32), shape((groups, 1, hid), F32), shape((groups, 1, hid), F32),
            shape((1, hid + LANES), F32)],
        in_specs=[vmem] * len(args),
        out_specs=[vmem] * 4,
        scratch_shapes=sends + recvs + [
            pltpu.VMEM((8, 256), jnp.int32),
            pltpu.SMEM((8, 256), jnp.int32),
            pltpu.VMEM((edges // LANES, LANES), jnp.int32),
            pltpu.VMEM((edges // LANES // 8, 8, LANES), jnp.int32),
            pltpu.VMEM((edges // LANES // 8, 8, LANES), F32),
            pltpu.VMEM((edges // CHUNK, CHUNK), jnp.int32),
            pltpu.VMEM((edges // CHUNK, CHUNK), F32),
            pltpu.VMEM((edges // LANES, LANES), F32),
            pltpu.VMEM((pairs + 1, SRC_BLOCK, DST_BLOCK), F32),
            pltpu.VMEM((slots, dsts), BF16),
            pltpu.VMEM((slots, dsts), BF16),
            pltpu.VMEM((slots, dsts), BF16),
            pltpu.VMEM((hubs, dsts), F32),
            pltpu.VMEM((hid, hubs), F32),
            pltpu.VMEM((slots - own, LANES), F32),
            pltpu.VMEM((slots, hid), F32),
            pltpu.VMEM((3, dsts, hid), BF16),
            pltpu.VMEM((hid, slots), BF16),
        ] + [pltpu.SemaphoreType.DMA] * (1 + 2 * len(blocks)),
        compiler_params=pltpu.CompilerParams(collective_id=0, has_side_effects=True, vmem_limit_bytes=56 * 2 ** 20),
        name="main_exchange",
    )(*args)


def output_kernel(dxt_ref, gw1_ref, gw2_ref, bias_ref, dx_out, gw1_out, gw2_out, b1_out, b2_out):
    feat_in, feat_out, hid = dx_out.shape[0], gw2_out.shape[0], gw2_out.shape[1]
    dx_out[...] = dxt_ref[:feat_in, :]
    gw1_out[...] = gw1_ref[...].reshape(gw1_ref.shape[0], hid)[:feat_in, :]
    gw2_out[...] = gw2_ref[...].reshape(gw2_ref.shape[0], hid)[:feat_out, :]
    b1_out[...] = bias_ref[:, :hid]
    b2_out[...] = bias_ref[:, hid:hid + feat_out]


def solution(mesh):
    groups = mesh.shape["graph"]

    def device_step(x, dst, src, w, send, hub_ids, w_first, b_first, w_second, dy):
        own, feat_in = x.shape
        feat_out = dy.shape[1]
        hid = w_first.shape[1]
        halo, hubs = send.shape[0], hub_ids.shape[0]
        edges = [v.reshape(-1, LANES) for v in (dst, src, w)]
        raw = main_call(
            groups, own, halo, hubs, *edges, x.T, dy.T, send[None, :], hub_ids[None, :], b_first[None, :],
            w_first, w_second.T)
        dx, gw1, gw2, gb1, gb2 = pl.pallas_call(
            output_kernel,
            out_shape=[jax.ShapeDtypeStruct(shape, F32) for shape in (
                (feat_in, own), (feat_in, hid), (feat_out, hid), (1, hid), (1, feat_out))],
            name="outputs",
        )(*raw)
        return dx.T, gw1, gw2.T, gb1[0], gb2[0]

    rows, flat = P(("data", "graph"), None), P(("data", "graph"))
    return jax.shard_map(
        device_step,
        mesh=mesh,
        in_specs=(rows, flat, flat, flat, flat, P("data"), P(), P(), P(), rows),
        out_specs=(rows, P("data", None), P("data", None), P("data"), P("data")),
        check_vma=False,
    )
```

```python
import functools

import jax
import jax.numpy as jnp
from jax import lax
from jax.experimental import pallas as pl
from jax.experimental.pallas import tpu as pltpu
from jax.sharding import PartitionSpec as P

BF16 = jnp.bfloat16
F32 = jnp.float32
HI = lax.Precision.HIGHEST
LANES = 128
MESH = pl.DeviceIdType.MESH


def dot(a, b, ca=1, cb=0, precision=None):
    return lax.dot_general(a, b, (((ca,), (cb,)), ((), ())), precision=precision, preferred_element_type=F32)


def split3(a):
    hi = a.astype(BF16)
    rest = a - hi.astype(F32)
    mid = rest.astype(BF16)
    return hi, mid, (rest - mid.astype(F32)).astype(BF16)


def exact3(sel, pieces, ca=1):
    return dot(sel, pieces[2], ca) + dot(sel, pieces[1], ca) + dot(sel, pieces[0], ca)


def exact3_right(pieces, sel):
    return dot(pieces[2], sel) + dot(pieces[1], sel) + dot(pieces[0], sel)


def full6(a, b):
    low = dot(a[0], b[2]) + dot(a[2], b[0]) + dot(a[1], b[1])
    return low + (dot(a[0], b[1]) + dot(a[1], b[0])) + dot(a[0], b[0])


def partner(groups, me, i):
    low = sum(2 << k for k in range(0, groups.bit_length() - 2, 2))
    t = jnp.bitwise_xor(i - 1, 2 * low + 1)
    high = jnp.bitwise_and(jnp.right_shift(t, 1), low)
    return jnp.bitwise_xor(me, jnp.bitwise_xor(t, jnp.bitwise_xor(high, low)))


def wait_all(groups, buf, sem, whole):
    part = buf if whole else buf.at[pl.ds(0, groups - 1)]
    pltpu.make_async_copy(part, part, sem).wait()


def send_all(groups, me, items):
    def send(i, carry):
        peer = partner(groups, me, i)
        for kind, src, dst, send_sem, recv_sem in items:
            pltpu.make_async_remote_copy(
                src_ref=src.at[peer] if kind == "a" else src,
                dst_ref=dst.at[me],
                send_sem=send_sem,
                recv_sem=recv_sem,
                device_id=(0, peer),
                device_id_type=MESH,
            ).start()
        return carry

    lax.fori_loop(1, groups, send, 0)
    for kind, src, dst, _, recv_sem in items:
        pltpu.make_async_copy(src.at[me] if kind == "a" else src, dst.at[me], recv_sem).start()


def greet_all(groups, me):
    barrier = pltpu.get_barrier_semaphore()

    def greet(i, carry):
        pl.semaphore_signal(barrier, inc=1, device_id=(0, partner(groups, me, i)), device_id_type=MESH)
        return carry

    lax.fori_loop(1, groups, greet, 0)
    return barrier


def padded(ref, rows, cols):
    a = ref[...]
    if cols > a.shape[1]:
        a = jnp.concatenate([a, jnp.zeros((a.shape[0], cols - a.shape[1]), a.dtype)], axis=1)
    if rows > a.shape[0]:
        a = jnp.concatenate([a, jnp.zeros((rows - a.shape[0], cols), a.dtype)], axis=0)
    return a


SRC_BLOCK, DST_BLOCK = 64, 256
BUCKET = SRC_BLOCK * DST_BLOCK
CHUNK, UNROLL = 256, 88


def bitonic(keys, weights, low, high):
    vregs = keys.shape[0]
    base = vregs.bit_length() - 1

    def bit(shape, m):
        axis, m = (len(shape) - 2, m - base) if m < base + 3 else (len(shape) - 1, m - base - 3)
        return jnp.bitwise_and(jnp.right_shift(lax.broadcasted_iota(jnp.int32, shape, axis), m), 1)

    def other(a, j):
        if j >= base + 3:
            lane = lax.broadcasted_iota(jnp.int32, (vregs * 8, LANES), 1)
            return jnp.take_along_axis(
                a.reshape(vregs * 8, LANES), jnp.bitwise_xor(lane, 1 << (j - base - 3)), axis=1).reshape(a.shape)
        step = 1 << (j - base)
        if step == 4:
            return pltpu.roll(a, 4, 1)
        return jnp.where(bit(a.shape, j) > 0, pltpu.roll(a, step, 1), pltpu.roll(a, 8 - step, 1))

    full = keys.shape
    for k in range(low, high + 1):
        for j in range(k - 1, -1, -1):
            if j < base:
                near = 1 << j
                parts = (vregs // (2 * near), 2, near, 8, LANES)
                a, b = keys.reshape(parts)[:, 0], keys.reshape(parts)[:, 1]
                wa, wb = weights.reshape(parts)[:, 0], weights.reshape(parts)[:, 1]
                swap = a > b
                if k < base:
                    block = lax.broadcasted_iota(jnp.int32, a.shape, 0)
                    swap = jnp.logical_xor(swap, jnp.bitwise_and(jnp.right_shift(block, k - j - 1), 1) > 0)
                elif k < base + 10:
                    swap = jnp.logical_xor(swap, bit(a.shape, k) > 0)
                keys = jnp.stack([jnp.where(swap, b, a), jnp.where(swap, a, b)], axis=1).reshape(full)
                weights = jnp.stack([jnp.where(swap, wb, wa), jnp.where(swap, wa, wb)], axis=1).reshape(full)
            else:
                keys2, weights2 = other(keys, j), other(weights, j)
                upper = bit(full, j)
                if k < base + 10:
                    upper = jnp.bitwise_xor(upper, bit(full, k))
                take = jnp.bitwise_xor(keys2, -upper) < jnp.bitwise_xor(keys, -upper)
                keys = jnp.where(take, keys2, keys)
                weights = jnp.where(take, weights2, weights)
    return keys, weights


def ring_sum(a, axis):
    step = a.shape[axis] // 2
    while step:
        a = a + pltpu.roll(a, step, axis)
        step //= 2
    return a


def list_pairs(buckets, key_ref, plan_ref):
    size = CHUNK
    shift = size.bit_length() - 1
    total = 1 << buckets.bit_length()

    def count(at, i, carry):
        bucket = jnp.right_shift(key_ref[pl.ds(pl.multiple_of(i * block, block), block), :], BUCKET.bit_length() - 1)
        return tuple(
            c + jnp.sum(jnp.where(bucket <= at + b, 1, 0).reshape(block // 8, 8, LANES), axis=0)
            for b, c in enumerate(carry))

    counts, block = (), 32
    for at in range(0, buckets, 24):
        zeros = (jnp.zeros((8, LANES), jnp.int32),) * min(24, buckets - at)
        counts += lax.fori_loop(0, key_ref.shape[0] // block, functools.partial(count, at), zeros)
    counts = [ring_sum(c, 0)[:1] for c in counts]
    none = jnp.zeros((1, LANES), jnp.int32)
    counts = [none] + counts + [counts[-1]] * (total - buckets)
    low = ring_sum(jnp.concatenate(counts[:total], axis=0), 1)
    high = ring_sum(jnp.concatenate(counts[1:], axis=0), 1)
    start = jnp.right_shift(low, shift)
    pairs = jnp.where(high > low, jnp.right_shift(high + size - 1, shift) - start, 0)
    row = lax.broadcasted_iota(jnp.int32, (total, LANES), 0)
    last, step = pairs, 1
    while step < total:
        last = last + jnp.where(row >= step, pltpu.roll(last, step, 0), 0)
        step *= 2
    first = last - pairs
    for half in range(plan_ref.shape[1] // LANES):
        at = lax.broadcasted_iota(jnp.int32, (total, LANES), 1) + half * LANES
        inside = (first <= at) & (at < last)
        rows = [
            jnp.where(last <= at, 1, 0), jnp.where(inside, start + at - first, 0), jnp.where(inside & (at > first), 1, 0),
            jnp.where((row == at) & (pairs > 0), last, 0)]
        rows = [ring_sum(r, 0)[:1] for r in rows] + [none] * 4
        plan_ref[:, half * LANES:(half + 1) * LANES] = jnp.concatenate(rows, axis=0)


def add_pairs(plan_ref, key_ref, w_ref, column_ref, cum_ref, low, high):
    src_ids = lax.broadcasted_iota(jnp.int32, (SRC_BLOCK, LANES), 0).astype(F32).astype(BF16)
    lane = lax.broadcasted_iota(jnp.int32, (CHUNK, LANES), 1)
    dst_ids = [(lane + at).astype(F32).astype(BF16) for at in range(0, DST_BLOCK, LANES)]
    one, zero = jnp.ones((), BF16), jnp.zeros((), BF16)

    def step(it, carry):
        work = []
        for u in range(UNROLL):
            b, c = plan_ref[0, it * UNROLL + u], plan_ref[1, it * UNROLL + u]
            src_row = jnp.right_shift(key_ref[pl.ds(c, 1), :] - b * BUCKET, DST_BLOCK.bit_length() - 1)
            src_row = jnp.where((src_row >= 0) & (src_row < SRC_BLOCK), src_row, 512).astype(F32)
            w_row = w_ref[pl.ds(c, 1), :]
            lhs = []
            for r in range(0, CHUNK, LANES):
                src, weight = src_row[:, r:r + LANES].astype(BF16), w_row[:, r:r + LANES]
                hit = src_ids == jnp.broadcast_to(src, src_ids.shape)
                lhs.append(jnp.concatenate(
                    [jnp.where(hit, jnp.broadcast_to(p, src_ids.shape), zero) for p in split3(weight)], axis=0))
            dst = jnp.take_along_axis(column_ref[...], jnp.broadcast_to(c, lane.shape), axis=1).astype(BF16)
            rhs = [jnp.where(dst == ids, one, zero) for ids in dst_ids]
            work.append((jnp.concatenate(lhs, axis=1), jnp.concatenate(rhs, axis=1)))
        outs = [dot(lhs, rhs) for lhs, rhs in work]
        total = cum_ref[it * UNROLL]
        for u, out in enumerate(outs):
            same = jnp.broadcast_to(plan_ref[2, it * UNROLL + u], (1, DST_BLOCK)) > 0
            out = out[2 * SRC_BLOCK:] + out[SRC_BLOCK:2 * SRC_BLOCK] + out[:SRC_BLOCK]
            total = out + jnp.where(same, total, 0.0)
            cum_ref[it * UNROLL + u + 1] = total
        return carry

    lax.fori_loop(low, high, step, 0)


def rows_to_blocks(a, groups):
    return a.reshape(groups, a.shape[0] // groups, a.shape[1])


def main_kernel(groups, own, halo, hubs, dst_ref, src_ref, w_in_ref, xt_ref, dyt_ref, send_ref, hub_ref, b1_ref, w1_ref, w2t_ref,
                dxt_ref, gw1_ref, gw2_ref, bias_ref,
                sx, sd, hx, hd, s1, s2, s3, s4, s5, s6, s7, s8, s9,
                rx, rd, gx, gd, r1, r2, r3, r4, r5, r6, r7,
                list_ref, plan_ref, raw_ref, sort_k, sort_w, key_ref, w_ref, column_ref, cum_ref, hi_ref, mid_ref, low_ref, hubrow_ref, pt_ref, g2_ref, g1_ref, dy_ref, zt_ref, plan_sem, *sems):
    count = len(sems) // 2
    snd, rcv = sems[:count], sems[count:]
    adj = (hi_ref, mid_ref, low_ref)
    per = hubs // groups
    hid = b1_ref.shape[1]
    feat_in = xt_ref.shape[0]
    first_hub = own + halo
    slots, dsts = own + halo + hubs, own + hubs
    tops = dsts // DST_BLOCK
    me = lax.axis_index("graph")
    barrier = greet_all(groups, me)
    steps = (cum_ref.shape[0] - 1) // UNROLL
    middle = steps // 2
    cum_ref[0] = jnp.zeros((SRC_BLOCK, DST_BLOCK), F32)
    dst, src = dst_ref[...], src_ref[...]
    bucket = jnp.right_shift(src, SRC_BLOCK.bit_length() - 1) * tops + jnp.right_shift(dst, DST_BLOCK.bit_length() - 1)
    raw_ref[...] = (
        bucket * BUCKET + jnp.bitwise_and(src, SRC_BLOCK - 1) * DST_BLOCK + jnp.bitwise_and(dst, DST_BLOCK - 1))
    list_pairs(slots // SRC_BLOCK * tops, raw_ref, list_ref)
    plan = pltpu.make_async_copy(list_ref, plan_ref, plan_sem)
    plan.start()

    lane = lax.broadcasted_iota(jnp.int32, (1, LANES), 1)
    half = lane < LANES // 2
    own_row = lax.broadcasted_iota(jnp.int32, (own, 1), 0)
    pick_t = (own_row == send_ref[...]).astype(F32).astype(BF16)
    sel_f = (own_row == hub_ref[...] - me * own).astype(F32)
    sel_t = sel_f.astype(BF16)
    plain = jnp.sum(sel_f, axis=1, keepdims=True) == 0
    number = lax.broadcasted_iota(jnp.int32, (1, hubs), 1) + 1
    numbers = jnp.broadcast_to(number.astype(F32), (8, hubs)).astype(BF16)
    code_row = dot(numbers, sel_t, 1, 1)[:1]
    plain_row = code_row == 0
    xt = padded(xt_ref, LANES, own)
    feature = lax.broadcasted_iota(jnp.int32, (LANES, 1), 0)
    xt = jnp.where(feature == feat_in, code_row, xt.astype(F32)).astype(BF16)
    dyt = padded(dyt_ref, LANES, own)
    picked = dot(jnp.concatenate((xt,) + split3(dyt), axis=0), jnp.concatenate([pick_t, sel_t], axis=1))
    hub_dt = picked[3 * LANES:, halo:] + picked[2 * LANES:3 * LANES, halo:] + picked[LANES:2 * LANES, halo:]
    sx[:, :per, :] = rows_to_blocks(picked[:LANES, :halo].T, groups).astype(BF16)
    sx[:, per:, :] = rows_to_blocks(picked[:LANES, halo:].T, groups).astype(BF16)
    hub_d = rows_to_blocks(hub_dt.T, groups)
    sd[...] = hub_d[:, :1, :] + pltpu.roll(hub_d[:, 1:, :], LANES // 2, 2)
    phases = raw_ref.size.bit_length() - 1
    sort_k[...], sort_w[...] = bitonic(
        raw_ref[...].reshape(sort_k.shape), w_in_ref[...].reshape(sort_w.shape), 1, phases - 4)
    pl.semaphore_wait(barrier, groups - 1)
    send_all(groups, me, [("a", sx, rx, snd[0], rcv[0]), ("a", sd, rd, snd[1], rcv[1])])

    w1 = padded(w1_ref, LANES, hid)
    w1_t = w1.astype(F32).T.astype(BF16)
    zt_ref[:, :own] = jnp.where(plain_row, dot(w1_t, xt), 0.0).astype(BF16)
    dy = dyt.T
    keys, weights = bitonic(sort_k[...], sort_w[...], phases - 3, phases)
    keys = keys.reshape(raw_ref.shape)
    column_ref[...] = jnp.bitwise_and(keys, DST_BLOCK - 1).astype(F32)
    key_ref[...] = keys.T
    w_ref[...] = weights.reshape(raw_ref.shape).T
    plan.wait()
    add_pairs(plan_ref, key_ref, w_ref, column_ref, cum_ref, 0, middle)
    wait_all(groups, rx, rcv[0], True)
    wait_all(groups, rd, rcv[1], True)
    got = rx[...].astype(F32)
    home_x = got[:, per:, :].sum(axis=0)
    hx[...] = home_x.astype(BF16)
    hd[...] = rd[...].sum(axis=0)
    send_all(groups, me, [("b", hx, gx, snd[2], rcv[2]), ("b", hd, gd, snd[3], rcv[3])])

    home_x = jnp.concatenate([home_x, jnp.zeros((8 - per, LANES), F32)], axis=0).astype(BF16)
    add_pairs(plan_ref, key_ref, w_ref, column_ref, cum_ref, middle, steps)

    group = LANES // SRC_BLOCK

    def renamed(i):
        cell = [
            jnp.concatenate([cum_ref[plan_ref[3, (i * group + g) * tops + j]] for g in range(group)], axis=0)
            for j in range(tops)]
        mine = jnp.concatenate(cell[:own // DST_BLOCK], axis=1)
        pieces = split3(mine)
        return mine, pieces, jnp.concatenate(cell[own // DST_BLOCK:], axis=1) + exact3_right(pieces, sel_t)

    def rename(i, carry):
        _, pieces, hub = renamed(i)
        rows = pl.ds(pl.multiple_of(i * LANES, LANES), LANES)
        for ref, left, right in zip(adj, pieces, split3(hub)):
            ref[rows, :own] = left
            ref[rows, own:] = right
        return carry

    def rename_hub(i, carry):
        mine, _, hub = renamed(first_hub // LANES + i)
        rows = pl.ds(pl.multiple_of(i * LANES, LANES), LANES)
        hubrow_ref[rows, :own] = mine
        hubrow_ref[rows, own:] = hub
        return carry

    lax.fori_loop(0, first_hub // LANES, rename, 0)
    lax.fori_loop(0, hubs // LANES, rename_hub, 0)
    halo_x = got[:, :per, :].reshape(halo, LANES).astype(BF16)
    column = jnp.broadcast_to(jnp.where(lane == feat_in, 1.0, 0.0), (8, LANES)).astype(BF16)
    halo_row = dot(column, halo_x, 1, 1)[:1].astype(jnp.int32)
    zt_ref[:, own:first_hub] = jnp.where(halo_row == 0, dot(w1_t, halo_x, 1, 1), 0.0).astype(BF16)
    halo_sel = (lax.broadcasted_iota(jnp.int32, (hubs, 1), 0) + 1 == halo_row).astype(F32)
    moved = jnp.concatenate([sel_f.T, halo_sel], axis=1).astype(BF16)
    for j in range(tops):
        cols = slice(j * DST_BLOCK, (j + 1) * DST_BLOCK)
        new = hubrow_ref[:, cols] + exact3(moved, [a[:first_hub, cols] for a in adj])
        for a, piece in zip(adj, split3(new)):
            a[first_hub:, cols] = piece

    def forward(rows, cols):
        zt = zt_ref[:, rows]
        return dot(zt, low_ref[rows, cols]) + dot(zt, mid_ref[rows, cols]) + dot(zt, hi_ref[rows, cols])

    def pack(d):
        dh, dm, dl = split3(d)
        d_two = (dh.astype(F32) + pltpu.roll(dm.astype(F32), LANES // 2, 1)).astype(BF16)
        return jnp.concatenate([d_two, dl], axis=1), d_two, dh

    def grad_out_sums(rows, cols, packed):
        a = dot(hi_ref[rows, cols], packed[0])
        t = a[:, :LANES] + a[:, LANES:] + dot(mid_ref[rows, cols], packed[1]) + dot(low_ref[rows, cols], packed[2])
        return jnp.where(half, t + pltpu.roll(t, LANES // 2, 1), 0.0)

    own_cols, hub_cols = slice(0, own), slice(own, dsts)
    pt_ref[...] = forward(slice(0, first_hub), hub_cols)
    d_own = pack(jnp.where(plain, dy, 0.0))
    g2_ref[...] = grad_out_sums(slice(own, slots), own_cols, d_own)
    wait_all(groups, gx, rcv[2], True)
    wait_all(groups, gd, rcv[3], True)
    hub_x = gx[...].astype(F32).reshape(hubs, LANES).astype(BF16)
    zt_ref[:, first_hub:] = dot(w1_t, hub_x, 1, 1).astype(BF16)
    hub_d = gd[...].reshape(groups, LANES)
    hub_d = jnp.stack([jnp.where(half, hub_d, 0.0), jnp.where(half, pltpu.roll(hub_d, LANES // 2, 1), 0.0)], axis=1)
    d_hub = pack(hub_d.reshape(hubs, LANES))
    hub_slots = slice(first_hub, slots)
    y_hub = (pt_ref[...] + forward(hub_slots, hub_cols)).T
    s1[:, :, LANES:] = rows_to_blocks(y_hub, groups)
    g2_halo = g2_ref[:halo, :] + grad_out_sums(slice(own, first_hub), hub_cols, d_hub)
    g2_hub = g2_ref[halo:, :] + grad_out_sums(hub_slots, hub_cols, d_hub)
    s1[:, :, :LANES] = rows_to_blocks(g2_halo + pltpu.roll(g2_hub, LANES // 2, 1), groups)
    send_all(groups, me, [("a", s1, r1, snd[4], rcv[4])])

    b1 = b1_ref[...]
    w2t = padded(w2t_ref, LANES, hid)
    pre = forward(slice(0, slots), own_cols).T + b1
    g2_own = grad_out_sums(slice(0, own), own_cols, d_own) + grad_out_sums(slice(0, own), hub_cols, d_hub)
    hidden = jnp.where(plain, jax.nn.relu(pre), 0.0).astype(BF16)
    live = plain & (pre > 0)
    wait_all(groups, r1, rcv[4], True)
    home = r1[...].sum(axis=0)
    pad = jnp.zeros((8 - per, LANES), F32)
    home_g = jnp.where(half, pltpu.roll(jnp.concatenate([home[:, :LANES], pad], axis=0), LANES // 2, 1), 0.0)
    home_pre = jnp.concatenate([home[:, LANES:] + b1, jnp.zeros((8 - per, hid), F32)], axis=0)
    home_dz2 = home_g.astype(BF16)
    home_dy = jnp.where(home_pre > 0, dot(home_dz2, w2t), 0.0)
    s2[...] = home_dy[:per]
    send_all(groups, me, [("b", s2, r2, snd[5], rcv[5])])

    back = jnp.where(half, r1[:, :, :LANES].reshape(halo, LANES), 0.0)
    dz2 = jnp.where(plain, g2_own + exact3(pick_t, split3(back)), 0.0).astype(BF16)
    dy1 = jnp.where(live, dot(dz2, w2t), 0.0)
    home_hidden = jax.nn.relu(home_pre).astype(BF16)
    gw2 = dot(dz2, hidden, 0, 0) + dot(home_dz2, home_hidden, 0, 0)
    s3[...] = rows_to_blocks(gw2, groups)
    s4[:, :hid] = dy1.sum(axis=0, keepdims=True) + home_dy.sum(axis=0, keepdims=True)
    s4[:, hid:] = dy.sum(axis=0, keepdims=True)
    send_all(groups, me, [("a", s3, r3, snd[6], rcv[6]), ("b", s4, r4, snd[7], rcv[7])])
    for p, piece in enumerate(split3(dy1)):
        dy_ref[p, :own, :] = piece
    chunk = 256

    def own_part(i, carry):
        rows = pl.ds(pl.multiple_of(i * chunk, chunk), chunk)
        g1_ref[rows, :] = full6([a[rows, :own] for a in adj], [dy_ref[p, :own, :] for p in range(3)])
        return carry

    lax.fori_loop(0, slots // chunk, own_part, 0)
    wait_all(groups, r2, rcv[5], True)
    for p, piece in enumerate(split3(r2[...].reshape(hubs, hid))):
        dy_ref[p, own:, :] = piece

    def hub_part(rows):
        return g1_ref[rows, :] + full6([a[rows, own:] for a in adj], [dy_ref[p, own:, :] for p in range(3)])

    s5[:, :per, :] = rows_to_blocks(hub_part(slice(own, first_hub)), groups)
    s5[:, per:, :] = rows_to_blocks(hub_part(hub_slots), groups)
    send_all(groups, me, [("a", s5, r5, snd[8], rcv[8])])

    g1_ref[:chunk, :] = hub_part(slice(0, chunk))
    g1_ref[chunk:own, :] = hub_part(slice(chunk, own))
    wait_all(groups, r3, rcv[6], True)
    wait_all(groups, r4, rcv[7], True)
    bias_ref[...] = r4[...].sum(axis=0)
    s9[...] = r3[...].sum(axis=0)
    send_all(groups, me, [("b", s9, gw2_ref, snd[12], rcv[12])])
    wait_all(groups, r5, rcv[8], True)
    home_dz1 = jnp.concatenate([r5[:, per:, :].sum(axis=0), jnp.zeros((8 - per, hid), F32)], axis=0).astype(BF16)
    back = r5[:, :per, :].reshape(halo, hid)
    dz1 = g1_ref[:own, :] + exact3(pick_t, split3(back))
    dz1 = jnp.where(plain, dz1, 0.0).astype(BF16)
    gw1 = dot(xt, dz1) + dot(home_x, home_dz1, 0, 0)
    s6[...] = rows_to_blocks(gw1, groups)
    send_all(groups, me, [("a", s6, r6, snd[9], rcv[9])])

    s7[...] = dot(home_dz1, w1, 1, 1)[:per]
    send_all(groups, me, [("b", s7, r7, snd[10], rcv[10])])
    dxt = dot(w1, dz1, 1, 1)
    wait_all(groups, r6, rcv[9], True)
    s8[...] = r6[...].sum(axis=0)
    send_all(groups, me, [("b", s8, gw1_ref, snd[11], rcv[11])])

    wait_all(groups, r7, rcv[10], True)
    hub_dx = r7[...].reshape(hubs, LANES).T
    dxt_ref[...] = dxt + exact3_right(split3(hub_dx), sel_f.T.astype(BF16))
    wait_all(groups, gw2_ref, rcv[12], True)
    for buf, sem in zip((rx, rd, gx, gd, r1, r2, r3, r4, r5, r6, r7, gw1_ref, gw2_ref), snd):
        wait_all(groups, buf, sem, False)
    wait_all(groups, gw1_ref, rcv[11], True)


def main_call(groups, own, halo, hubs, *args):
    hid = args[7].shape[1]
    per = hubs // groups
    slots, dsts = own + halo + hubs, own + hubs
    edges = args[0].size
    pairs = edges // CHUNK + slots // SRC_BLOCK * (dsts // DST_BLOCK)
    vmem = pl.BlockSpec(memory_space=pltpu.VMEM)
    blocks = [
        ("a", (2 * per, LANES), BF16), ("a", (1, LANES), F32), ("b", (per, LANES), BF16), ("b", (1, LANES), F32),
        ("a", (per, LANES + hid), F32), ("b", (per, hid), F32), ("a", (1, hid), F32), ("b", (1, hid + LANES), F32),
        ("a", (2 * per, hid), F32), ("a", (1, hid), F32), ("b", (per, LANES), F32), ("b", (1, hid), F32), ("b", (1, hid), F32)]
    sends = [pltpu.VMEM(((groups,) if k == "a" else ()) + b, t) for k, b, t in blocks]
    recvs = [pltpu.VMEM((groups,) + b, t) for _, b, t in blocks[:-2]]
    shape = jax.ShapeDtypeStruct
    return pl.pallas_call(
        functools.partial(main_kernel, groups, own, halo, hubs),
        out_shape=[
            shape((LANES, own), F32), shape((groups, 1, hid), F32), shape((groups, 1, hid), F32),
            shape((1, hid + LANES), F32)],
        in_specs=[vmem] * len(args),
        out_specs=[vmem] * 4,
        scratch_shapes=sends + recvs + [
            pltpu.VMEM((8, 256), jnp.int32),
            pltpu.SMEM((8, 256), jnp.int32),
            pltpu.VMEM((edges // LANES, LANES), jnp.int32),
            pltpu.VMEM((edges // LANES // 8, 8, LANES), jnp.int32),
            pltpu.VMEM((edges // LANES // 8, 8, LANES), F32),
            pltpu.VMEM((edges // CHUNK, CHUNK), jnp.int32),
            pltpu.VMEM((edges // CHUNK, CHUNK), F32),
            pltpu.VMEM((edges // LANES, LANES), F32),
            pltpu.VMEM((pairs + 1, SRC_BLOCK, DST_BLOCK), F32),
            pltpu.VMEM((slots, dsts), BF16),
            pltpu.VMEM((slots, dsts), BF16),
            pltpu.VMEM((slots, dsts), BF16),
            pltpu.VMEM((hubs, dsts), F32),
            pltpu.VMEM((hid, hubs), F32),
            pltpu.VMEM((slots - own, LANES), F32),
            pltpu.VMEM((slots, hid), F32),
            pltpu.VMEM((3, dsts, hid), BF16),
            pltpu.VMEM((hid, slots), BF16),
        ] + [pltpu.SemaphoreType.DMA] * (1 + 2 * len(blocks)),
        compiler_params=pltpu.CompilerParams(collective_id=0, has_side_effects=True, vmem_limit_bytes=56 * 2 ** 20),
        name="main_exchange",
    )(*args)


def output_kernel(dxt_ref, gw1_ref, gw2_ref, bias_ref, dx_out, gw1_out, gw2_out, b1_out, b2_out):
    feat_in, feat_out, hid = dx_out.shape[0], gw2_out.shape[0], gw2_out.shape[1]
    dx_out[...] = dxt_ref[:feat_in, :]
    gw1_out[...] = gw1_ref[...].reshape(gw1_ref.shape[0], hid)[:feat_in, :]
    gw2_out[...] = gw2_ref[...].reshape(gw2_ref.shape[0], hid)[:feat_out, :]
    b1_out[...] = bias_ref[:, :hid]
    b2_out[...] = bias_ref[:, hid:hid + feat_out]


def solution(mesh):
    groups = mesh.shape["graph"]

    def device_step(x, dst, src, w, send, hub_ids, w_first, b_first, w_second, dy):
        own, feat_in = x.shape
        feat_out = dy.shape[1]
        hid = w_first.shape[1]
        halo, hubs = send.shape[0], hub_ids.shape[0]
        edges = [v.reshape(-1, LANES) for v in (dst, src, w)]
        raw = main_call(
            groups, own, halo, hubs, *edges, x.T, dy.T, send[None, :], hub_ids[None, :], b_first[None, :],
            w_first, w_second.T)
        dx, gw1, gw2, gb1, gb2 = pl.pallas_call(
            output_kernel,
            out_shape=[jax.ShapeDtypeStruct(shape, F32) for shape in (
                (feat_in, own), (feat_in, hid), (feat_out, hid), (1, hid), (1, feat_out))],
            name="outputs",
        )(*raw)
        return dx.T, gw1, gw2.T, gb1[0], gb2[0]

    rows, flat = P(("data", "graph"), None), P(("data", "graph"))
    return jax.shard_map(
        device_step,
        mesh=mesh,
        in_specs=(rows, flat, flat, flat, flat, P("data"), P(), P(), P(), rows),
        out_specs=(rows, P("data", None), P("data", None), P("data"), P("data")),
        check_vma=False,
    )
```

```python
import functools

import jax
import jax.numpy as jnp
from jax import lax
from jax.experimental import pallas as pl
from jax.experimental.pallas import tpu as pltpu
from jax.sharding import PartitionSpec as P

BF16 = jnp.bfloat16
F32 = jnp.float32
HI = lax.Precision.HIGHEST
LANES = 128
MESH = pl.DeviceIdType.MESH


def dot(a, b, ca=1, cb=0, precision=None):
    return lax.dot_general(a, b, (((ca,), (cb,)), ((), ())), precision=precision, preferred_element_type=F32)


def split3(a):
    hi = a.astype(BF16)
    rest = a - hi.astype(F32)
    mid = rest.astype(BF16)
    return hi, mid, (rest - mid.astype(F32)).astype(BF16)


def exact3(sel, pieces, ca=1):
    return dot(sel, pieces[2], ca) + dot(sel, pieces[1], ca) + dot(sel, pieces[0], ca)


def exact3_right(pieces, sel):
    return dot(pieces[2], sel) + dot(pieces[1], sel) + dot(pieces[0], sel)


def full6(a, b):
    low = dot(a[0], b[2]) + dot(a[2], b[0]) + dot(a[1], b[1])
    return low + (dot(a[0], b[1]) + dot(a[1], b[0])) + dot(a[0], b[0])


def partner(groups, me, i):
    low = sum(2 << k for k in range(0, groups.bit_length() - 2, 2))
    t = jnp.bitwise_xor(i - 1, 2 * low + 1)
    high = jnp.bitwise_and(jnp.right_shift(t, 1), low)
    return jnp.bitwise_xor(me, jnp.bitwise_xor(t, jnp.bitwise_xor(high, low)))


def wait_all(groups, buf, sem, whole):
    part = buf if whole else buf.at[pl.ds(0, groups - 1)]
    pltpu.make_async_copy(part, part, sem).wait()


def send_all(groups, me, items):
    def send(i, carry):
        peer = partner(groups, me, i)
        for kind, src, dst, send_sem, recv_sem in items:
            pltpu.make_async_remote_copy(
                src_ref=src.at[peer] if kind == "a" else src,
                dst_ref=dst.at[me],
                send_sem=send_sem,
                recv_sem=recv_sem,
                device_id=(0, peer),
                device_id_type=MESH,
            ).start()
        return carry

    lax.fori_loop(1, groups, send, 0)
    for kind, src, dst, _, recv_sem in items:
        pltpu.make_async_copy(src.at[me] if kind == "a" else src, dst.at[me], recv_sem).start()


def greet_all(groups, me):
    barrier = pltpu.get_barrier_semaphore()

    def greet(i, carry):
        pl.semaphore_signal(barrier, inc=1, device_id=(0, partner(groups, me, i)), device_id_type=MESH)
        return carry

    lax.fori_loop(1, groups, greet, 0)
    return barrier


def padded(ref, rows, cols):
    a = ref[...]
    if cols > a.shape[1]:
        a = jnp.concatenate([a, jnp.zeros((a.shape[0], cols - a.shape[1]), a.dtype)], axis=1)
    if rows > a.shape[0]:
        a = jnp.concatenate([a, jnp.zeros((rows - a.shape[0], cols), a.dtype)], axis=0)
    return a


SRC_BLOCK, DST_BLOCK = 64, 256
BUCKET = SRC_BLOCK * DST_BLOCK
CHUNK, UNROLL = 256, 44


def bitonic(keys, weights, low, high):
    vregs = keys.shape[0]
    base = vregs.bit_length() - 1

    def bit(shape, m):
        axis, m = (len(shape) - 2, m - base) if m < base + 3 else (len(shape) - 1, m - base - 3)
        return jnp.bitwise_and(jnp.right_shift(lax.broadcasted_iota(jnp.int32, shape, axis), m), 1)

    def other(a, j):
        if j >= base + 3:
            lane = lax.broadcasted_iota(jnp.int32, (vregs * 8, LANES), 1)
            return jnp.take_along_axis(
                a.reshape(vregs * 8, LANES), jnp.bitwise_xor(lane, 1 << (j - base - 3)), axis=1).reshape(a.shape)
        step = 1 << (j - base)
        if step == 4:
            return pltpu.roll(a, 4, 1)
        return jnp.where(bit(a.shape, j) > 0, pltpu.roll(a, step, 1), pltpu.roll(a, 8 - step, 1))

    full = keys.shape
    for k in range(low, high + 1):
        for j in range(k - 1, -1, -1):
            if j < base:
                near = 1 << j
                parts = (vregs // (2 * near), 2, near, 8, LANES)
                a, b = keys.reshape(parts)[:, 0], keys.reshape(parts)[:, 1]
                wa, wb = weights.reshape(parts)[:, 0], weights.reshape(parts)[:, 1]
                swap = a > b
                if k < base:
                    block = lax.broadcasted_iota(jnp.int32, a.shape, 0)
                    swap = jnp.logical_xor(swap, jnp.bitwise_and(jnp.right_shift(block, k - j - 1), 1) > 0)
                elif k < base + 10:
                    swap = jnp.logical_xor(swap, bit(a.shape, k) > 0)
                keys = jnp.stack([jnp.where(swap, b, a), jnp.where(swap, a, b)], axis=1).reshape(full)
                weights = jnp.stack([jnp.where(swap, wb, wa), jnp.where(swap, wa, wb)], axis=1).reshape(full)
            else:
                keys2, weights2 = other(keys, j), other(weights, j)
                upper = bit(full, j)
                if k < base + 10:
                    upper = jnp.bitwise_xor(upper, bit(full, k))
                take = jnp.bitwise_xor(keys2, -upper) < jnp.bitwise_xor(keys, -upper)
                keys = jnp.where(take, keys2, keys)
                weights = jnp.where(take, weights2, weights)
    return keys, weights


def ring_sum(a, axis):
    step = a.shape[axis] // 2
    while step:
        a = a + pltpu.roll(a, step, axis)
        step //= 2
    return a


def list_pairs(buckets, key_ref, plan_ref):
    size = CHUNK
    shift = size.bit_length() - 1
    total = 1 << buckets.bit_length()

    def count(at, i, carry):
        bucket = jnp.right_shift(key_ref[pl.ds(pl.multiple_of(i * block, block), block), :], BUCKET.bit_length() - 1)
        return tuple(
            c + jnp.sum(jnp.where(bucket <= at + b, 1, 0).reshape(block // 8, 8, LANES), axis=0)
            for b, c in enumerate(carry))

    counts, block = (), 32
    for at in range(0, buckets, 24):
        zeros = (jnp.zeros((8, LANES), jnp.int32),) * min(24, buckets - at)
        counts += lax.fori_loop(0, key_ref.shape[0] // block, functools.partial(count, at), zeros)
    counts = [ring_sum(c, 0)[:1] for c in counts]
    none = jnp.zeros((1, LANES), jnp.int32)
    counts = [none] + counts + [counts[-1]] * (total - buckets)
    low = ring_sum(jnp.concatenate(counts[:total], axis=0), 1)
    high = ring_sum(jnp.concatenate(counts[1:], axis=0), 1)
    start = jnp.right_shift(low, shift)
    pairs = jnp.where(high > low, jnp.right_shift(high + size - 1, shift) - start, 0)
    row = lax.broadcasted_iota(jnp.int32, (total, LANES), 0)
    last, step = pairs, 1
    while step < total:
        last = last + jnp.where(row >= step, pltpu.roll(last, step, 0), 0)
        step *= 2
    first = last - pairs
    for half in range(plan_ref.shape[1] // LANES):
        at = lax.broadcasted_iota(jnp.int32, (total, LANES), 1) + half * LANES
        inside = (first <= at) & (at < last)
        rows = [
            jnp.where(last <= at, 1, 0), jnp.where(inside, start + at - first, 0), jnp.where(inside & (at > first), 1, 0),
            jnp.where((row == at) & (pairs > 0), last, 0)]
        rows = [ring_sum(r, 0)[:1] for r in rows] + [none] * 4
        plan_ref[:, half * LANES:(half + 1) * LANES] = jnp.concatenate(rows, axis=0)


def add_pairs(plan_ref, key_ref, w_ref, column_ref, cum_ref, low, high):
    src_ids = lax.broadcasted_iota(jnp.int32, (SRC_BLOCK, LANES), 0).astype(F32).astype(BF16)
    lane = lax.broadcasted_iota(jnp.int32, (CHUNK, LANES), 1)
    dst_ids = [(lane + at).astype(F32).astype(BF16) for at in range(0, DST_BLOCK, LANES)]
    one, zero = jnp.ones((), BF16), jnp.zeros((), BF16)

    def step(it, carry):
        work = []
        for u in range(UNROLL):
            b, c = plan_ref[0, it * UNROLL + u], plan_ref[1, it * UNROLL + u]
            src_row = jnp.right_shift(key_ref[pl.ds(c, 1), :] - b * BUCKET, DST_BLOCK.bit_length() - 1)
            src_row = jnp.where((src_row >= 0) & (src_row < SRC_BLOCK), src_row, 512).astype(F32)
            w_row = w_ref[pl.ds(c, 1), :]
            lhs = []
            for r in range(0, CHUNK, LANES):
                src, weight = src_row[:, r:r + LANES].astype(BF16), w_row[:, r:r + LANES]
                hit = src_ids == jnp.broadcast_to(src, src_ids.shape)
                lhs.append(jnp.concatenate(
                    [jnp.where(hit, jnp.broadcast_to(p, src_ids.shape), zero) for p in split3(weight)], axis=0))
            dst = jnp.take_along_axis(column_ref[...], jnp.broadcast_to(c, lane.shape), axis=1).astype(BF16)
            rhs = [jnp.where(dst == ids, one, zero) for ids in dst_ids]
            work.append((jnp.concatenate(lhs, axis=1), jnp.concatenate(rhs, axis=1)))
        outs = [dot(lhs, rhs) for lhs, rhs in work]
        total = cum_ref[it * UNROLL]
        for u, out in enumerate(outs):
            same = jnp.broadcast_to(plan_ref[2, it * UNROLL + u], (1, DST_BLOCK)) > 0
            out = out[2 * SRC_BLOCK:] + out[SRC_BLOCK:2 * SRC_BLOCK] + out[:SRC_BLOCK]
            total = out + jnp.where(same, total, 0.0)
            cum_ref[it * UNROLL + u + 1] = total
        return carry

    lax.fori_loop(low, high, step, 0)


def rows_to_blocks(a, groups):
    return a.reshape(groups, a.shape[0] // groups, a.shape[1])


def main_kernel(groups, own, halo, hubs, inputs, *refs):
    given, refs = refs[:inputs], refs[inputs:]
    outs, refs = refs[:4], refs[4:]
    held, sems, refs = refs[:inputs], refs[inputs:2 * inputs], refs[2 * inputs:]
    loads = [pltpu.make_async_copy(*item) for item in zip(given, held, sems)]
    for load in loads:
        load.start()
    main_body(groups, own, halo, hubs, loads, *held, *outs, *refs)


def main_body(groups, own, halo, hubs, loads, dst_ref, src_ref, w_in_ref, xt_ref, dyt_ref, send_ref, hub_ref, b1_ref, w1_ref, w2t_ref,
                dxt_ref, gw1_ref, gw2_ref, bias_ref,
                sx, sd, hx, hd, s1, s2, s3, s4, s5, s6, s7, s8, s9,
                rx, rd, gx, gd, r1, r2, r3, r4, r5, r6, r7,
                list_ref, plan_ref, raw_ref, sort_k, sort_w, key_ref, w_ref, column_ref, cum_ref, hi_ref, mid_ref, low_ref, hubrow_ref, pt_ref, g2_ref, g1_ref, dy_ref, zt_ref, plan_sem, *sems):
    count = len(sems) // 2
    snd, rcv = sems[:count], sems[count:]
    adj = (hi_ref, mid_ref, low_ref)
    per = hubs // groups
    hid = b1_ref.shape[1]
    feat_in = xt_ref.shape[0]
    first_hub = own + halo
    slots, dsts = own + halo + hubs, own + hubs
    tops = dsts // DST_BLOCK
    me = lax.axis_index("graph")
    barrier = greet_all(groups, me)
    for load in loads:
        load.wait()
    steps = (cum_ref.shape[0] - 1) // UNROLL
    middle = steps // 2
    cum_ref[0] = jnp.zeros((SRC_BLOCK, DST_BLOCK), F32)
    dst, src = dst_ref[...], src_ref[...]
    bucket = jnp.right_shift(src, SRC_BLOCK.bit_length() - 1) * tops + jnp.right_shift(dst, DST_BLOCK.bit_length() - 1)
    raw_ref[...] = (
        bucket * BUCKET + jnp.bitwise_and(src, SRC_BLOCK - 1) * DST_BLOCK + jnp.bitwise_and(dst, DST_BLOCK - 1))
    list_pairs(slots // SRC_BLOCK * tops, raw_ref, list_ref)
    plan = pltpu.make_async_copy(list_ref, plan_ref, plan_sem)
    plan.start()

    lane = lax.broadcasted_iota(jnp.int32, (1, LANES), 1)
    half = lane < LANES // 2
    own_row = lax.broadcasted_iota(jnp.int32, (own, 1), 0)
    pick_t = (own_row == send_ref[...]).astype(F32).astype(BF16)
    sel_f = (own_row == hub_ref[...] - me * own).astype(F32)
    sel_t = sel_f.astype(BF16)
    plain = jnp.sum(sel_f, axis=1, keepdims=True) == 0
    number = lax.broadcasted_iota(jnp.int32, (1, hubs), 1) + 1
    numbers = jnp.broadcast_to(number.astype(F32), (8, hubs)).astype(BF16)
    code_row = dot(numbers, sel_t, 1, 1)[:1]
    plain_row = code_row == 0
    xt = padded(xt_ref, LANES, own)
    feature = lax.broadcasted_iota(jnp.int32, (LANES, 1), 0)
    xt = jnp.where(feature == feat_in, code_row, xt.astype(F32)).astype(BF16)
    dyt = padded(dyt_ref, LANES, own)
    picked = dot(jnp.concatenate((xt,) + split3(dyt), axis=0), jnp.concatenate([pick_t, sel_t], axis=1))
    hub_dt = picked[3 * LANES:, halo:] + picked[2 * LANES:3 * LANES, halo:] + picked[LANES:2 * LANES, halo:]
    sx[:, :per, :] = rows_to_blocks(picked[:LANES, :halo].T, groups).astype(BF16)
    sx[:, per:, :] = rows_to_blocks(picked[:LANES, halo:].T, groups).astype(BF16)
    hub_d = rows_to_blocks(hub_dt.T, groups)
    sd[...] = hub_d[:, :1, :] + pltpu.roll(hub_d[:, 1:, :], LANES // 2, 2)
    phases = raw_ref.size.bit_length() - 1
    sort_k[...], sort_w[...] = bitonic(
        raw_ref[...].reshape(sort_k.shape), w_in_ref[...].reshape(sort_w.shape), 1, phases - 4)
    pl.semaphore_wait(barrier, groups - 1)
    send_all(groups, me, [("a", sx, rx, snd[0], rcv[0]), ("a", sd, rd, snd[1], rcv[1])])

    w1 = padded(w1_ref, LANES, hid)
    w1_t = w1.astype(F32).T.astype(BF16)
    zt_ref[:, :own] = jnp.where(plain_row, dot(w1_t, xt), 0.0).astype(BF16)
    dy = dyt.T
    keys, weights = bitonic(sort_k[...], sort_w[...], phases - 3, phases)
    keys = keys.reshape(raw_ref.shape)
    column_ref[...] = jnp.bitwise_and(keys, DST_BLOCK - 1).astype(F32)
    key_ref[...] = keys.T
    w_ref[...] = weights.reshape(raw_ref.shape).T
    plan.wait()
    add_pairs(plan_ref, key_ref, w_ref, column_ref, cum_ref, 0, middle)
    wait_all(groups, rx, rcv[0], True)
    wait_all(groups, rd, rcv[1], True)
    got = rx[...].astype(F32)
    home_x = got[:, per:, :].sum(axis=0)
    hx[...] = home_x.astype(BF16)
    hd[...] = rd[...].sum(axis=0)
    send_all(groups, me, [("b", hx, gx, snd[2], rcv[2]), ("b", hd, gd, snd[3], rcv[3])])

    home_x = jnp.concatenate([home_x, jnp.zeros((8 - per, LANES), F32)], axis=0).astype(BF16)
    add_pairs(plan_ref, key_ref, w_ref, column_ref, cum_ref, middle, steps)

    group = LANES // SRC_BLOCK

    def renamed(i):
        cell = [
            jnp.concatenate([cum_ref[plan_ref[3, (i * group + g) * tops + j]] for g in range(group)], axis=0)
            for j in range(tops)]
        mine = jnp.concatenate(cell[:own // DST_BLOCK], axis=1)
        pieces = split3(mine)
        return mine, pieces, jnp.concatenate(cell[own // DST_BLOCK:], axis=1) + exact3_right(pieces, sel_t)

    def rename(i, carry):
        _, pieces, hub = renamed(i)
        rows = pl.ds(pl.multiple_of(i * LANES, LANES), LANES)
        for ref, left, right in zip(adj, pieces, split3(hub)):
            ref[rows, :own] = left
            ref[rows, own:] = right
        return carry

    def rename_hub(i, carry):
        mine, _, hub = renamed(first_hub // LANES + i)
        rows = pl.ds(pl.multiple_of(i * LANES, LANES), LANES)
        hubrow_ref[rows, :own] = mine
        hubrow_ref[rows, own:] = hub
        return carry

    lax.fori_loop(0, first_hub // LANES, rename, 0)
    lax.fori_loop(0, hubs // LANES, rename_hub, 0)
    halo_x = got[:, :per, :].reshape(halo, LANES).astype(BF16)
    column = jnp.broadcast_to(jnp.where(lane == feat_in, 1.0, 0.0), (8, LANES)).astype(BF16)
    halo_row = dot(column, halo_x, 1, 1)[:1].astype(jnp.int32)
    zt_ref[:, own:first_hub] = jnp.where(halo_row == 0, dot(w1_t, halo_x, 1, 1), 0.0).astype(BF16)
    halo_sel = (lax.broadcasted_iota(jnp.int32, (hubs, 1), 0) + 1 == halo_row).astype(F32)
    moved = jnp.concatenate([sel_f.T, halo_sel], axis=1).astype(BF16)
    for j in range(tops):
        cols = slice(j * DST_BLOCK, (j + 1) * DST_BLOCK)
        new = hubrow_ref[:, cols] + exact3(moved, [a[:first_hub, cols] for a in adj])
        for a, piece in zip(adj, split3(new)):
            a[first_hub:, cols] = piece

    def forward(rows, cols):
        zt = zt_ref[:, rows]
        return dot(zt, low_ref[rows, cols]) + dot(zt, mid_ref[rows, cols]) + dot(zt, hi_ref[rows, cols])

    def pack(d):
        dh, dm, dl = split3(d)
        d_two = (dh.astype(F32) + pltpu.roll(dm.astype(F32), LANES // 2, 1)).astype(BF16)
        return jnp.concatenate([d_two, dl], axis=1), d_two, dh

    def grad_out_sums(rows, cols, packed):
        a = dot(hi_ref[rows, cols], packed[0])
        t = a[:, :LANES] + a[:, LANES:] + dot(mid_ref[rows, cols], packed[1]) + dot(low_ref[rows, cols], packed[2])
        return jnp.where(half, t + pltpu.roll(t, LANES // 2, 1), 0.0)

    own_cols, hub_cols = slice(0, own), slice(own, dsts)
    pt_ref[...] = forward(slice(0, first_hub), hub_cols)
    d_own = pack(jnp.where(plain, dy, 0.0))
    g2_ref[...] = grad_out_sums(slice(own, slots), own_cols, d_own)
    wait_all(groups, gx, rcv[2], True)
    wait_all(groups, gd, rcv[3], True)
    hub_x = gx[...].astype(F32).reshape(hubs, LANES).astype(BF16)
    zt_ref[:, first_hub:] = dot(w1_t, hub_x, 1, 1).astype(BF16)
    hub_d = gd[...].reshape(groups, LANES)
    hub_d = jnp.stack([jnp.where(half, hub_d, 0.0), jnp.where(half, pltpu.roll(hub_d, LANES // 2, 1), 0.0)], axis=1)
    d_hub = pack(hub_d.reshape(hubs, LANES))
    hub_slots = slice(first_hub, slots)
    y_hub = (pt_ref[...] + forward(hub_slots, hub_cols)).T
    s1[:, :, LANES:] = rows_to_blocks(y_hub, groups)
    g2_halo = g2_ref[:halo, :] + grad_out_sums(slice(own, first_hub), hub_cols, d_hub)
    g2_hub = g2_ref[halo:, :] + grad_out_sums(hub_slots, hub_cols, d_hub)
    s1[:, :, :LANES] = rows_to_blocks(g2_halo + pltpu.roll(g2_hub, LANES // 2, 1), groups)
    send_all(groups, me, [("a", s1, r1, snd[4], rcv[4])])

    b1 = b1_ref[...]
    w2t = padded(w2t_ref, LANES, hid)
    pre = forward(slice(0, slots), own_cols).T + b1
    g2_own = grad_out_sums(slice(0, own), own_cols, d_own) + grad_out_sums(slice(0, own), hub_cols, d_hub)
    hidden = jnp.where(plain, jax.nn.relu(pre), 0.0).astype(BF16)
    live = plain & (pre > 0)
    wait_all(groups, r1, rcv[4], True)
    home = r1[...].sum(axis=0)
    pad = jnp.zeros((8 - per, LANES), F32)
    home_g = jnp.where(half, pltpu.roll(jnp.concatenate([home[:, :LANES], pad], axis=0), LANES // 2, 1), 0.0)
    home_pre = jnp.concatenate([home[:, LANES:] + b1, jnp.zeros((8 - per, hid), F32)], axis=0)
    home_dz2 = home_g.astype(BF16)
    home_dy = jnp.where(home_pre > 0, dot(home_dz2, w2t), 0.0)
    s2[...] = home_dy[:per]
    send_all(groups, me, [("b", s2, r2, snd[5], rcv[5])])

    back = jnp.where(half, r1[:, :, :LANES].reshape(halo, LANES), 0.0)
    dz2 = jnp.where(plain, g2_own + exact3(pick_t, split3(back)), 0.0).astype(BF16)
    dy1 = jnp.where(live, dot(dz2, w2t), 0.0)
    home_hidden = jax.nn.relu(home_pre).astype(BF16)
    gw2 = dot(dz2, hidden, 0, 0) + dot(home_dz2, home_hidden, 0, 0)
    s3[...] = rows_to_blocks(gw2, groups)
    s4[:, :hid] = dy1.sum(axis=0, keepdims=True) + home_dy.sum(axis=0, keepdims=True)
    s4[:, hid:] = dy.sum(axis=0, keepdims=True)
    send_all(groups, me, [("a", s3, r3, snd[6], rcv[6]), ("b", s4, r4, snd[7], rcv[7])])
    for p, piece in enumerate(split3(dy1)):
        dy_ref[p, :own, :] = piece
    chunk = 256

    def own_part(i, carry):
        rows = pl.ds(pl.multiple_of(i * chunk, chunk), chunk)
        g1_ref[rows, :] = full6([a[rows, :own] for a in adj], [dy_ref[p, :own, :] for p in range(3)])
        return carry

    lax.fori_loop(0, slots // chunk, own_part, 0)
    wait_all(groups, r2, rcv[5], True)
    for p, piece in enumerate(split3(r2[...].reshape(hubs, hid))):
        dy_ref[p, own:, :] = piece

    def hub_part(rows):
        return g1_ref[rows, :] + full6([a[rows, own:] for a in adj], [dy_ref[p, own:, :] for p in range(3)])

    s5[:, :per, :] = rows_to_blocks(hub_part(slice(own, first_hub)), groups)
    s5[:, per:, :] = rows_to_blocks(hub_part(hub_slots), groups)
    send_all(groups, me, [("a", s5, r5, snd[8], rcv[8])])

    g1_ref[:chunk, :] = hub_part(slice(0, chunk))
    g1_ref[chunk:own, :] = hub_part(slice(chunk, own))
    wait_all(groups, r3, rcv[6], True)
    wait_all(groups, r4, rcv[7], True)
    bias_ref[...] = r4[...].sum(axis=0)
    s9[...] = r3[...].sum(axis=0)
    send_all(groups, me, [("b", s9, gw2_ref, snd[12], rcv[12])])
    wait_all(groups, r5, rcv[8], True)
    home_dz1 = jnp.concatenate([r5[:, per:, :].sum(axis=0), jnp.zeros((8 - per, hid), F32)], axis=0).astype(BF16)
    back = r5[:, :per, :].reshape(halo, hid)
    dz1 = g1_ref[:own, :] + exact3(pick_t, split3(back))
    dz1 = jnp.where(plain, dz1, 0.0).astype(BF16)
    gw1 = dot(xt, dz1) + dot(home_x, home_dz1, 0, 0)
    s6[...] = rows_to_blocks(gw1, groups)
    send_all(groups, me, [("a", s6, r6, snd[9], rcv[9])])

    s7[...] = dot(home_dz1, w1, 1, 1)[:per]
    send_all(groups, me, [("b", s7, r7, snd[10], rcv[10])])
    dxt = dot(w1, dz1, 1, 1)
    wait_all(groups, r6, rcv[9], True)
    s8[...] = r6[...].sum(axis=0)
    send_all(groups, me, [("b", s8, gw1_ref, snd[11], rcv[11])])

    wait_all(groups, r7, rcv[10], True)
    hub_dx = r7[...].reshape(hubs, LANES).T
    dxt_ref[...] = dxt + exact3_right(split3(hub_dx), sel_f.T.astype(BF16))
    wait_all(groups, gw2_ref, rcv[12], True)
    for buf, sem in zip((rx, rd, gx, gd, r1, r2, r3, r4, r5, r6, r7, gw1_ref, gw2_ref), snd):
        wait_all(groups, buf, sem, False)
    wait_all(groups, gw1_ref, rcv[11], True)


def main_call(groups, own, halo, hubs, *args):
    hid = args[7].shape[1]
    per = hubs // groups
    slots, dsts = own + halo + hubs, own + hubs
    edges = args[0].size
    pairs = edges // CHUNK + slots // SRC_BLOCK * (dsts // DST_BLOCK)
    vmem = pl.BlockSpec(memory_space=pltpu.VMEM)
    blocks = [
        ("a", (2 * per, LANES), BF16), ("a", (1, LANES), F32), ("b", (per, LANES), BF16), ("b", (1, LANES), F32),
        ("a", (per, LANES + hid), F32), ("b", (per, hid), F32), ("a", (1, hid), F32), ("b", (1, hid + LANES), F32),
        ("a", (2 * per, hid), F32), ("a", (1, hid), F32), ("b", (per, LANES), F32), ("b", (1, hid), F32), ("b", (1, hid), F32)]
    sends = [pltpu.VMEM(((groups,) if k == "a" else ()) + b, t) for k, b, t in blocks]
    recvs = [pltpu.VMEM((groups,) + b, t) for _, b, t in blocks[:-2]]
    shape = jax.ShapeDtypeStruct
    return pl.pallas_call(
        functools.partial(main_kernel, groups, own, halo, hubs, len(args)),
        out_shape=[
            shape((LANES, own), F32), shape((groups, 1, hid), F32), shape((groups, 1, hid), F32),
            shape((1, hid + LANES), F32)],
        in_specs=[pl.BlockSpec(memory_space=pl.ANY)] * len(args),
        out_specs=[vmem] * 4,
        scratch_shapes=[pltpu.VMEM(a.shape, a.dtype) for a in args] + [pltpu.SemaphoreType.DMA] * len(args) + sends + recvs + [
            pltpu.VMEM((8, 256), jnp.int32),
            pltpu.SMEM((8, 256), jnp.int32),
            pltpu.VMEM((edges // LANES, LANES), jnp.int32),
            pltpu.VMEM((edges // LANES // 8, 8, LANES), jnp.int32),
            pltpu.VMEM((edges // LANES // 8, 8, LANES), F32),
            pltpu.VMEM((edges // CHUNK, CHUNK), jnp.int32),
            pltpu.VMEM((edges // CHUNK, CHUNK), F32),
            pltpu.VMEM((edges // LANES, LANES), F32),
            pltpu.VMEM((pairs + 1, SRC_BLOCK, DST_BLOCK), F32),
            pltpu.VMEM((slots, dsts), BF16),
            pltpu.VMEM((slots, dsts), BF16),
            pltpu.VMEM((slots, dsts), BF16),
            pltpu.VMEM((hubs, dsts), F32),
            pltpu.VMEM((hid, hubs), F32),
            pltpu.VMEM((slots - own, LANES), F32),
            pltpu.VMEM((slots, hid), F32),
            pltpu.VMEM((3, dsts, hid), BF16),
            pltpu.VMEM((hid, slots), BF16),
        ] + [pltpu.SemaphoreType.DMA] * (1 + 2 * len(blocks)),
        compiler_params=pltpu.CompilerParams(collective_id=0, has_side_effects=True, vmem_limit_bytes=56 * 2 ** 20),
        name="main_exchange",
    )(*args)


def output_kernel(dxt_ref, gw1_ref, gw2_ref, bias_ref, dx_out, gw1_out, gw2_out, b1_out, b2_out):
    feat_in, feat_out, hid = dx_out.shape[0], gw2_out.shape[0], gw2_out.shape[1]
    dx_out[...] = dxt_ref[:feat_in, :]
    gw1_out[...] = gw1_ref[...].reshape(gw1_ref.shape[0], hid)[:feat_in, :]
    gw2_out[...] = gw2_ref[...].reshape(gw2_ref.shape[0], hid)[:feat_out, :]
    b1_out[...] = bias_ref[:, :hid]
    b2_out[...] = bias_ref[:, hid:hid + feat_out]


def solution(mesh):
    groups = mesh.shape["graph"]

    def device_step(x, dst, src, w, send, hub_ids, w_first, b_first, w_second, dy):
        own, feat_in = x.shape
        feat_out = dy.shape[1]
        hid = w_first.shape[1]
        halo, hubs = send.shape[0], hub_ids.shape[0]
        edges = [v.reshape(-1, LANES) for v in (dst, src, w)]
        raw = main_call(
            groups, own, halo, hubs, *edges, x.T, dy.T, send[None, :], hub_ids[None, :], b_first[None, :],
            w_first, w_second.T)
        dx, gw1, gw2, gb1, gb2 = pl.pallas_call(
            output_kernel,
            out_shape=[jax.ShapeDtypeStruct(shape, F32) for shape in (
                (feat_in, own), (feat_in, hid), (feat_out, hid), (1, hid), (1, feat_out))],
            name="outputs",
        )(*raw)
        return dx.T, gw1, gw2.T, gb1[0], gb2[0]

    rows, flat = P(("data", "graph"), None), P(("data", "graph"))
    return jax.shard_map(
        device_step,
        mesh=mesh,
        in_specs=(rows, flat, flat, flat, flat, P("data"), P(), P(), P(), rows),
        out_specs=(rows, P("data", None), P("data", None), P("data"), P("data")),
        check_vma=False,
    )
```
